256 devices in a mesh: gx: 8 (over z), gy: 4 (over y), gz: 8 (over x, core).
Axes of the slice: x: 4, y: 4, z: 8, core: 2. Of those that a mesh axis runs over, the one named last changes fastest.
Arguments:
- right_side: float32 [4, 192, 96, 192], P(None, 'gx', 'gy', 'gz'), may hold values from -6 to 6
- iterate: float32 [4, 192, 96, 192], P(None, 'gx', 'gy', 'gz'), may hold values from -6 to 6
- coefficient: float32 [192, 96, 192], P('gx', 'gy', 'gz'), may hold values from 0.1 to 2
- ordering: int32 [8, 4, 8, 216], P('gx', 'gy', 'gz'), may hold values from 0 to 215, as said below
- leaf_inverse: float32 [8, 4, 8, 125, 125], P('gx', 'gy', 'gz'), may hold values from -2 to 3
- leaf_first: float32 [8, 4, 8, 125, 50], P('gx', 'gy', 'gz'), may hold values from -0.5 to 0.5
- leaf_second: float32 [8, 4, 8, 125, 60], P('gx', 'gy', 'gz'), may hold values from -0.5 to 0.5
- leaf_top: float32 [8, 4, 8, 125, 72], P('gx', 'gy', 'gz'), may hold values from -0.5 to 0.5
- first_inverse: float32 [8, 4, 200, 200], P('gx', 'gy', 'gz'), may hold values from -2 to 3
- first_second: float32 [8, 4, 8, 25, 60], P('gx', 'gy', 'gz'), may hold values from -1.25 to 1.25
- first_top: float32 [8, 4, 8, 25, 72], P('gx', 'gy', 'gz'), may hold values from -1.25 to 1.25
- second_inverse: float32 [8, 960, 960], P('gx', ('gy', 'gz')), may hold values from -2 to 3
- second_top: float32 [8, 4, 8, 30, 72], P('gx', 'gy', 'gz'), may hold values from -1 to 1
- top_inverse: float32 [9216, 9216], P(('gx', 'gy', 'gz')), may hold values from -2 to 3
Outputs:
- correction: float32 [4, 192, 96, 192], P(None, 'gx', 'gy', 'gz')
The draws below stay inside these ranges and needn't reach their ends.
Inputs may be any that keep to these rules, and one draw needn't show every extreme that they name: `ordering`: each device's row names each of its 216 coarse cells once (cell x 6^2 + y * 6 + z): first the 125 cells with x, y and z all below 5, then the 25 cells with z = 5 and x, y below it, then the 30 cells with y = 5 and x below it, then the 36 cells with x = 5, each group in any order.
All inputs are finite; a program needn't handle non-finite values.
Results may differ from the reference program's by a relative error of at most 0.0003.
Values sent between devices are 32-bit elements; how exact they have to be, the bound alone decides.
A program may use at most 64 MiB of HBM per device.

```python
import math
import jax
import jax.numpy as jnp
from jax import lax

NRHS = 4
SIDE = 6
COARSE_DEV = 216
FIRST_DEV = 25
SECOND_DEV = 30
TOP_DEV = 36
LEAF = 125
FIRST_SEP = 200
SECOND_SEP = 960
TOP_SEP = 9216
NX = 192
NY = 96
NZ = 192
N_GX = 8
N_GY = 4
N_GZ = 8


def inverse_block(key, leading, extent):
    full_shape = tuple(leading) + (extent, extent)
    jitter = jnp.clip(jax.random.normal(key, full_shape, jnp.float32), -4.0, 4.0) * 0.5
    return jnp.eye(extent, dtype=jnp.float32) + jitter / extent ** 0.5


def draw_leaf_inverse(key, part):
    return inverse_block(jax.random.fold_in(key, 11), (N_GX, N_GY, N_GZ), LEAF)


def draw_first_inverse(key, part):
    return inverse_block(jax.random.fold_in(key, 23), (N_GX, N_GY), FIRST_SEP)


def draw_second_inverse(key, part):
    return inverse_block(jax.random.fold_in(key, 37), (N_GX,), SECOND_SEP)


def draw_top_inverse(key, part):
    return inverse_block(jax.random.fold_in(key, 41), (), TOP_SEP)


def draw_ordering(key, part):
    cells = jnp.arange(COARSE_DEV, dtype=jnp.int32)
    first_coord = cells // (SIDE * SIDE)
    second_coord = cells // SIDE % SIDE
    third_coord = cells % SIDE
    edge = SIDE - 1
    classes = jnp.where(first_coord == edge, 3, jnp.where(second_coord == edge, 2, jnp.where(third_coord == edge, 1, 0))).astype(jnp.int32)
    subkeys = jax.random.split(jax.random.fold_in(key, 53), N_GX * N_GY * N_GZ)

    def one_row(subkey):
        shuffled = jax.random.permutation(subkey, COARSE_DEV).astype(jnp.int32)
        rank = jnp.argsort(classes[shuffled], stable=True)
        return shuffled[rank].astype(jnp.int32)
    return jax.vmap(one_row)(subkeys).reshape(N_GX, N_GY, N_GZ, COARSE_DEV)


def levels(own_key, dims, shards, low, top_value):
    factor_of = 1.0
    for axis_at, blocks in shards:
        draws = jax.random.uniform(jax.random.fold_in(jax.random.fold_in(own_key, 6), axis_at), (blocks,), jnp.float32, low / len(shards), top_value / len(shards))
        factor_of = factor_of * jnp.repeat(jnp.exp(draws), dims[axis_at] // blocks).reshape((-1,) + (1,) * (len(dims) - 1 - axis_at))
    return factor_of


def normal_values(stream_key, dims, scale, most, cuts=(), kind=jnp.bfloat16):
    gain = levels(stream_key, dims, cuts, -0.22, 0.18) if cuts else 1.0
    drawn = jax.random.normal(stream_key, dims, jnp.float32) * scale * gain
    return jnp.minimum(jnp.maximum(drawn, -most), most).astype(kind)


def setup_inputs(seed: int = 0) -> dict:
    keys = jax.random.split(jax.random.key(seed), 15)
    return {
        "right_side": normal_values(keys[0], (NRHS, NX, NY, NZ), 1.0, 6.0, ((1, 8), (2, 4), (3, 8)), jnp.float32),
        "iterate": normal_values(keys[1], (NRHS, NX, NY, NZ), 1.0, 6.0, ((1, 8), (2, 4), (3, 8)), jnp.float32),
        "coefficient": jnp.clip(jnp.exp(math.log(2.0) - 2.9957323 * jax.random.uniform(keys[2], (NX, NY, NZ), jnp.float32) ** levels(keys[2], (NX, NY, NZ), ((0, 8), (1, 4), (2, 8)), -0.2, 0.2)), 0.1, 2.0),
        "ordering": draw_ordering(jax.random.fold_in(keys[14], 71), 0),
        "leaf_inverse": draw_leaf_inverse(jax.random.fold_in(keys[14], 71), 0),
        "leaf_first": normal_values(keys[5], (N_GX, N_GY, N_GZ, LEAF, 2 * FIRST_DEV), LEAF ** -0.5, 0.5, ((0, 8), (1, 4), (2, 8)), jnp.float32),
        "leaf_second": normal_values(keys[6], (N_GX, N_GY, N_GZ, LEAF, 2 * SECOND_DEV), LEAF ** -0.5, 0.5, ((0, 8), (1, 4), (2, 8)), jnp.float32),
        "leaf_top": normal_values(keys[7], (N_GX, N_GY, N_GZ, LEAF, 2 * TOP_DEV), LEAF ** -0.5, 0.5, ((0, 8), (1, 4), (2, 8)), jnp.float32),
        "first_inverse": draw_first_inverse(jax.random.fold_in(keys[14], 71), 0),
        "first_second": normal_values(keys[9], (N_GX, N_GY, N_GZ, FIRST_DEV, 2 * SECOND_DEV), FIRST_DEV ** -0.5, 1.25, ((0, 8), (1, 4), (2, 8)), jnp.float32),
        "first_top": normal_values(keys[10], (N_GX, N_GY, N_GZ, FIRST_DEV, 2 * TOP_DEV), FIRST_DEV ** -0.5, 1.25, ((0, 8), (1, 4), (2, 8)), jnp.float32),
        "second_inverse": draw_second_inverse(jax.random.fold_in(keys[14], 71), 0),
        "second_top": normal_values(keys[12], (N_GX, N_GY, N_GZ, SECOND_DEV, 2 * TOP_DEV), SECOND_DEV ** -0.5, 1.0, ((0, 8), (1, 4), (2, 8)), jnp.float32),
        "top_inverse": draw_top_inverse(jax.random.fold_in(keys[14], 71), 0),
    }


precise = lax.Precision.HIGHEST


def contract(pattern, operand, matrix):
    return jnp.einsum(pattern, operand, matrix, precision=precise, preferred_element_type=jnp.float32)


def weigh(extended, dimension):
    length = extended.shape[dimension] - 1
    previous = lax.slice_in_dim(extended, 0, length, 2, dimension)
    centre = lax.slice_in_dim(extended, 1, length + 1, 2, dimension)
    following = lax.slice_in_dim(extended, 2, length + 1, 2, dimension)
    return 0.25 * previous + 0.5 * centre + 0.25 * following


def spread(extended, dimension):
    length = extended.shape[dimension] - 1
    current = lax.slice_in_dim(extended, 0, length, 1, dimension)
    following = lax.slice_in_dim(extended, 1, length + 1, 1, dimension)
    paired = jnp.stack([current, 0.5 * (current + following)], axis=dimension + 1)
    new_shape = list(current.shape)
    new_shape[dimension] = 2 * length
    return paired.reshape(new_shape)


def restrict(values):
    extended = jnp.pad(values, ((0, 0), (1, 0), (1, 0), (1, 0)))
    for dimension in (1, 2, 3):
        extended = weigh(extended, dimension)
    return extended


def prolong(values):
    extended = jnp.pad(values, ((0, 0), (0, 1), (0, 1), (0, 1)))
    for dimension in (1, 2, 3):
        extended = spread(extended, dimension)
    return extended


def residual_of(right_side, iterate, coefficient):
    padded = jnp.pad(iterate, ((0, 0), (1, 1), (1, 1), (1, 1)))
    beside = padded[:, 2:, 1:-1, 1:-1] + padded[:, :-2, 1:-1, 1:-1]
    beside = beside + padded[:, 1:-1, 2:, 1:-1] + padded[:, 1:-1, :-2, 1:-1]
    beside = beside + padded[:, 1:-1, 1:-1, 2:] + padded[:, 1:-1, 1:-1, :-2]
    return right_side - ((6.0 + coefficient) * iterate - beside)


def from_above(values, axis):
    length = values.shape[axis]
    kept = lax.slice_in_dim(values, 1, length, 1, axis)
    widths = [(0, 0)] * values.ndim
    widths[axis] = (0, 1)
    return jnp.pad(kept, widths)


def from_below(values, axis):
    length = values.shape[axis]
    kept = lax.slice_in_dim(values, 0, length - 1, 1, axis)
    widths = [(0, 0)] * values.ndim
    widths[axis] = (1, 0)
    return jnp.pad(kept, widths)


def reference(right_side, iterate, coefficient, ordering, leaf_inverse, leaf_first, leaf_second, leaf_top, first_inverse, first_second, first_top, second_inverse, second_top, top_inverse):
    coarse = restrict(restrict(residual_of(right_side, iterate, coefficient)))
    blocks = coarse.reshape(NRHS, N_GX, SIDE, N_GY, SIDE, N_GZ, SIDE)
    blocks = blocks.transpose(0, 1, 3, 5, 2, 4, 6).reshape(NRHS, N_GX, N_GY, N_GZ, COARSE_DEV)
    chosen = jnp.take_along_axis(blocks, jnp.broadcast_to(ordering[None], blocks.shape), axis=4)
    first_end = LEAF + FIRST_DEV
    second_end = first_end + SECOND_DEV
    leaf_rhs = chosen[..., :LEAF]
    first_rhs = chosen[..., LEAF:first_end]
    second_rhs = chosen[..., first_end:second_end]
    top_rhs = chosen[..., second_end:]

    leaf_solved = contract('rabcl,abclk->rabck', leaf_rhs, leaf_inverse)
    toward = contract('rabcl,abclk->rabck', leaf_solved, leaf_first)
    first_target = first_rhs - toward[..., :FIRST_DEV] - from_above(toward[..., FIRST_DEV:], 3)
    first_target = first_target.reshape(NRHS, N_GX, N_GY, FIRST_SEP)
    first_solved = contract('rabi,abik->rabk', first_target, first_inverse).reshape(NRHS, N_GX, N_GY, N_GZ, FIRST_DEV)

    toward = contract('rabcl,abclk->rabck', leaf_solved, leaf_second) + contract('rabcl,abclk->rabck', first_solved, first_second)
    second_target = second_rhs - toward[..., :SECOND_DEV] - from_above(toward[..., SECOND_DEV:], 2)
    second_target = second_target.reshape(NRHS, N_GX, SECOND_SEP)
    second_solved = contract('rai,aik->rak', second_target, second_inverse).reshape(NRHS, N_GX, N_GY, N_GZ, SECOND_DEV)

    toward = contract('rabcl,abclk->rabck', leaf_solved, leaf_top) + contract('rabcl,abclk->rabck', first_solved, first_top)
    toward = toward + contract('rabcl,abclk->rabck', second_solved, second_top)
    top_target = top_rhs - toward[..., :TOP_DEV] - from_above(toward[..., TOP_DEV:], 1)
    top_target = top_target.reshape(NRHS, TOP_SEP)
    top_solved = contract('ri,ik->rk', top_target, top_inverse)

    top_back = contract('rk,ik->ri', top_solved, top_inverse).reshape(NRHS, N_GX, N_GY, N_GZ, TOP_DEV)
    top_pair = jnp.concatenate([top_back, from_below(top_back, 1)], axis=4)
    second_gap = second_solved - contract('rabck,abcik->rabci', top_pair, second_top)
    second_gap = second_gap.reshape(NRHS, N_GX, SECOND_SEP)
    second_back = contract('rak,aik->rai', second_gap, second_inverse).reshape(NRHS, N_GX, N_GY, N_GZ, SECOND_DEV)
    second_pair = jnp.concatenate([second_back, from_below(second_back, 2)], axis=4)
    first_gap = first_solved - contract('rabck,abcik->rabci', second_pair, first_second)
    first_gap = first_gap - contract('rabck,abcik->rabci', top_pair, first_top)
    first_gap = first_gap.reshape(NRHS, N_GX, N_GY, FIRST_SEP)
    first_back = contract('rabk,abik->rabi', first_gap, first_inverse).reshape(NRHS, N_GX, N_GY, N_GZ, FIRST_DEV)
    first_pair = jnp.concatenate([first_back, from_below(first_back, 3)], axis=4)
    leaf_gap = leaf_solved - contract('rabck,abcik->rabci', first_pair, leaf_first)
    leaf_gap = leaf_gap - contract('rabck,abcik->rabci', second_pair, leaf_second)
    leaf_gap = leaf_gap - contract('rabck,abcik->rabci', top_pair, leaf_top)
    leaf_back = contract('rabck,abclk->rabcl', leaf_gap, leaf_inverse)

    ordered = jnp.concatenate([leaf_back, first_back, second_back, top_back], axis=4)
    inverse_order = jnp.argsort(ordering, axis=-1).astype(jnp.int32)
    listed = jnp.take_along_axis(ordered, jnp.broadcast_to(inverse_order[None], ordered.shape), axis=4)
    listed = listed.reshape(NRHS, N_GX, N_GY, N_GZ, SIDE, SIDE, SIDE)
    coarse_grid = listed.transpose(0, 1, 4, 2, 5, 3, 6).reshape(NRHS, N_GX * SIDE, N_GY * SIDE, N_GZ * SIDE)
    return prolong(prolong(coarse_grid))
```

```python
import functools

import jax
import jax.numpy as jnp
from jax import lax
from jax.experimental import pallas as pl
from jax.experimental.pallas import tpu as pltpu
from jax.sharding import PartitionSpec as P

MESH = pl.DeviceIdType.MESH
F32 = jnp.float32
BF16 = jnp.bfloat16
AXES = ("gx", "gy", "gz")

FLAT = ((1, 0), (-1, 0), (0, 1), (0, -1), (1, 1), (1, -1), (-1, 1))
ABOVE = ((0, 0),) + FLAT
BELOW = ((0, 0), (1, 0), (0, 1), (1, 1))
HALO = [(x, y, 0) for x, y in FLAT] + [(x, y, 1) for x, y in ABOVE] + [(x, y, -1) for x, y in BELOW]
RIM = [(1, 0, 0), (0, 1, 0), (1, 1, 0), (0, 0, 1), (1, 0, 1), (0, 1, 1), (1, 1, 1)]


def split(value):
    high = value.astype(BF16)
    return high, (value - high.astype(F32)).astype(BF16)


def dot(left, right, dims=((1,), (0,))):
    return lax.dot_general(left, right, (dims, ((), ())), preferred_element_type=F32)


def times(value, factor, dims=((1,), (0,))):
    high, low = split(value)
    f_high, f_low = factor
    return dot(high, f_high, dims) + dot(low, f_high, dims) + dot(high, f_low, dims)


BACK = ((1,), (1,))


def iota(shape, dim):
    return lax.broadcasted_iota(jnp.int32, shape, dim)


def floats(shape, dim):
    return iota(shape, dim).astype(F32)


def whole_part(value, by):
    return jnp.floor((value + 0.5) * (1.0 / by))


def tent(coarse, fine):
    return jnp.maximum(4.0 - jnp.abs(fine - 4.0 * coarse), 0.0)


def inner(coarse, fine, first):
    below = 1.0 - first * jnp.maximum(1.0 - fine, 0.0)
    return (tent(coarse, fine + 1.0) + tent(coarse, fine - 1.0) * below) * 0.0625


def outer(coarse, fine):
    return tent(coarse, fine) * 0.0625


def kernel(cfg, *refs):
    ngx, ngy, ngz, rhs, fine, side, leaf, n1, n2, n3, ntop = cfg
    plane = ngy * ngz
    cells = side**3
    (rs_h, it_h, cf_h, or_h, li_h, lf_h, ls_h, lt_h, fi_h, fs_h, ft_h, si_h, st_h, ti_h) = refs[:14]
    out_h = refs[14]
    (
        rs, it, cf, od, li, lf, ls, lt, fi, fs, ft, si, st, ti, out_v,
        a21, bmat, e_h, e_l, fsx, fs_hi, fs_lo, stx, st_hi, st_lo,
        w1, w1_h, w1_l, w2, w2_h, w2_l, fi_low, si_low,
        flat, got_flat, got_thin, send1, got1, send2, got2, up_send, up_got,
        part, got5, s6, got6, yall, down_send, down_got, gap2, gap1, corr, got_corr,
        local_sem, out_sem, send_sem, recv_sem,
    ) = refs[15:]

    a, b, c = (lax.axis_index(n) for n in AXES)
    me = b * ngz + c
    used = [0]
    pending = []

    def at(dx, dy, dz):
        return (
            lax.rem(a + (dx + ngx), ngx) if dx else a,
            lax.rem(b + (dy + ngy), ngy) if dy else b,
            lax.rem(c + (dz + ngz), ngz) if dz else c,
        )

    def send(src, dst, device):
        i = used[0]
        used[0] += 1
        copy = pltpu.make_async_remote_copy(
            src_ref=src,
            dst_ref=dst,
            send_sem=send_sem.at[i],
            recv_sem=recv_sem.at[i],
            device_id=device,
            device_id_type=MESH,
        )
        copy.start()
        pending.append(copy)
        return copy

    def arrive(copies):
        for copy in copies:
            copy.wait_recv()

    pairs = [
        (it_h, it), (rs_h, rs), (cf_h, cf), (or_h, od), (li_h, li), (lf_h, lf), (ls_h, ls), (lt_h, lt),
        (fi_h, fi), (si_h, si), (fs_h, fs), (ft_h, ft), (st_h, st), (ti_h, ti),
    ]
    loads = [pltpu.make_async_copy(s, d, local_sem.at[i]) for i, (s, d) in enumerate(pairs)]
    for load in loads:
        load.start()

    partners = set()
    for dy in range(ngy):
        for dz in range(ngz):
            partners.add((0, dy, dz))
    for dx in range(ngx):
        partners.add((dx, 0, 0))
    for d in HALO + RIM:
        for s in (1, -1):
            partners.add((s * d[0] % ngx, s * d[1] % ngy, s * d[2] % ngz))
    partners.discard((0, 0, 0))
    barrier = pltpu.get_barrier_semaphore()
    for d in sorted(partners):
        pl.semaphore_signal(barrier, inc=1, device_id=at(*d), device_id_type=MESH)

    first_x = jnp.where(a == 0, 1.0, 0.0).astype(F32)
    first_y = jnp.where(b == 0, 1.0, 0.0).astype(F32)
    first_z = jnp.where(c == 0, 1.0, 0.0).astype(F32)

    shape = (64, fine * fine)
    row, col = floats(shape, 0), floats(shape, 1)
    cx = whole_part(row, 8)
    cy = row - 8.0 * cx - 1.0
    cx = cx - 1.0
    fx = whole_part(col, fine)
    fy = col - fine * fx
    ox, oy = outer(cx, fx), outer(cy, fy)
    a21[0:64, :] = (inner(cx, fx, first_x) * oy + ox * inner(cy, fy, first_y)).astype(BF16)
    a21[64:128, :] = (ox * oy).astype(BF16)

    zshape = (8 * rhs, 2 * rhs * fine)
    row, col = floats(zshape, 0), floats(zshape, 1)
    cz = whole_part(row, rhs)
    cr = row - rhs * cz
    cz = cz - 1.0
    kind = whole_part(col, rhs * fine)
    rest = col - rhs * fine * kind
    fr = whole_part(rest, fine)
    fz = rest - fine * fr
    same = jnp.maximum(1.0 - jnp.abs(cr - fr), 0.0)
    wvz = ((1.0 - kind) * outer(cz, fz) + kind * inner(cz, fz, first_z)) * same
    wvz = wvz.astype(BF16)

    for load in loads[:3]:
        load.wait()
    g1, g2 = [], []
    own = a21[64:128, :]
    both = a21[...]
    for r in range(rhs):
        now = it[r]
        q = rs[r] - (6.0 + cf[...]) * now
        q_h, q_l = split(q.reshape(fine * fine, fine))
        i_h, i_l = split(now.reshape(fine * fine, fine))
        from_it = dot(both, i_h) + dot(both, i_l)
        g1.append(from_it[0:64] + dot(own, q_h) + dot(own, q_l))
        g2.append(from_it[64:128])
    g_h, g_l = split(jnp.concatenate(g1 + g2, axis=1))
    ct = dot(wvz, g_h, BACK) + dot(wvz, g_l, BACK)
    for j in range(4):
        lo = ct[2 * rhs * j : 2 * rhs * j + rhs]
        hi = ct[2 * rhs * j + rhs : 2 * rhs * j + 2 * rhs]
        flat[j] = jnp.concatenate([lo, hi], axis=1)

    pl.semaphore_wait(barrier, len(partners))

    halo_copies = []
    for i, (dx, dy, dz) in enumerate(HALO):
        if dz == 0:
            src, dst = flat, got_flat.at[i]
        else:
            src, dst = flat.at[3 if dz == 1 else 0], got_thin.at[i - len(FLAT)]
        halo_copies.append(send(src, dst, at(dx, dy, dz)))
    for load in loads[3:]:
        load.wait()
    fi_copy = send(fi, fi_low, at(0, 0, 1))
    si_copy = send(si, si_low, at(0, 1, 0))

    shape = (cells, 512)
    m, k = iota(shape, 0), iota(shape, 1)
    e1, e2 = leaf + n1, leaf + n1 + n2
    want = jnp.where(m < e1, m + (128 - leaf), jnp.where(m < e2, m + (256 - e1), m + (384 - e2)))
    bmat[...] = jnp.where((m >= leaf) & (k == want), 1.0, 0.0).astype(F32)
    li_v = li[...]
    li_pair = split(li_v)
    bmat[0:leaf, 0:leaf] = li_v
    bmat[0:leaf, 128 : 128 + 2 * n1] = -times(li_v, split(lf[...]))
    bmat[0:leaf, 256 : 256 + 2 * n2] = -times(li_v, split(ls[...]))
    bmat[0:leaf, 384 : 384 + 2 * n3] = -times(li_v, split(lt[...]))
    bh, bl = split(bmat[...])
    shape = (512, cells)
    k = iota(shape, 0)
    z, x, y = k >> 6, (k >> 3) & 7, k & 7
    inside = (z >= 1) & (z <= side) & (x >= 1) & (x <= side) & (y >= 1) & (y <= side)
    cell = jnp.where(inside, ((x - 1) * side + (y - 1)) * side + (z - 1), -1)
    chosen = jnp.where(cell == od[...], 1.0, 0.0).astype(BF16)
    e_h[...] = dot(chosen, bh).astype(BF16)
    e_l[...] = dot(chosen, bl).astype(BF16)

    fsx[...] = jnp.zeros(fsx.shape, F32)
    fsx[0:n1, 0 : 2 * n2] = -fs[...]
    fsx[0:n1, 128 : 128 + 2 * n3] = -ft[...]
    stx[...] = jnp.zeros(stx.shape, F32)
    stx[0:n2, 0 : 2 * n3] = -st[...]
    place1 = n1 * lax.rem(c, 4)
    place2 = n2 * lax.rem(me, 4)
    shift = (128, 32)
    put1 = jnp.where(iota(shift, 0) == iota(shift, 1) + place1, 1.0, 0.0).astype(BF16)
    put2 = jnp.where(iota(shift, 0) == iota(shift, 1) + place2, 1.0, 0.0).astype(BF16)
    hi, lo = split(fsx[...])
    fs_hi[...] = dot(put1, hi).astype(BF16)
    fs_lo[...] = dot(put1, lo).astype(BF16)
    hi, lo = split(stx[...])
    st_hi[...] = dot(put2, hi).astype(BF16)
    st_lo[...] = dot(put2, lo).astype(BF16)

    groups1 = (ngz + 3) // 4
    groups2 = (plane + 3) // 4

    def grouped(w, high, low, mine, lower, size, groups, members, keep):
        w[...] = jnp.zeros(w.shape, F32)
        mine_v = mine[...]
        lower_v = jnp.where(keep, lower[...], 0.0)
        for g in range(groups):
            wide = min(4, members - 4 * g) * size
            s = slice(4 * g * size, 4 * g * size + wide)
            w[0:size, 128 * g : 128 * g + wide] = mine_v[:, s]
            w[size : 2 * size, 128 * g : 128 * g + wide] = lower_v[:, s]
        hi, lo = split(w[...])
        high[...] = hi
        low[...] = lo

    fi_copy.wait_recv()
    grouped(w1, w1_h, w1_l, fi, fi_low, n1, groups1, ngz, c > 0)

    arrive(halo_copies)
    lane = iota((rhs, 128), 1)
    at_z, at_x, at_y = lane >> 6, (lane >> 3) & 7, lane & 7

    def along(at_, d):
        if d == 0:
            return (at_ >= 1) & (at_ <= side)
        return at_ == (1 if d == 1 else side)

    def exists(i, d, n):
        return (i - d >= 0) & (i - d < n) if d else True

    total = [flat[j] for j in range(4)]
    for i, (dx, dy, dz) in enumerate(HALO):
        turn = (-(side * 8) * dx - side * dy) % 128
        keep = along(at_x, dx) & along(at_y, dy)
        there = exists(a, dx, ngx) & exists(b, dy, ngy) & exists(c, dz, ngz)
        keep = keep & there
        if dz == 0:
            for j in range(4):
                v = got_flat[i, j]
                v = pltpu.roll(v, turn, 1) if turn else v
                total[j] += jnp.where(keep, v, 0.0)
        else:
            v = got_thin[i - len(FLAT)]
            v = pltpu.roll(v, turn, 1) if turn else v
            keep = keep & (at_z == (1 if dz == 1 else 0))
            j = 0 if dz == 1 else 3
            total[j] += jnp.where(keep, v, 0.0)

    e_pair = (e_h[...], e_l[...])
    s = times(jnp.concatenate(total, axis=1), e_pair)
    s_leaf, s1, s23 = s[:, 0:128], s[:, 128:256], s[:, 256:512]

    w1_pair = (w1_h[...], w1_l[...])
    partial = times(s1, w1_pair)
    for g in range(groups1):
        send1[g] = partial[:, 128 * g : 128 * g + 128]
    copies = []
    for k in range(1, ngz):
        there = at(0, 0, k)
        copies.append(send(send1.at[there[2] // 4], got1.at[k], there))
    own1 = send1[c // 4]

    si_copy.wait_recv()
    grouped(w2, w2_h, w2_l, si, si_low, n2, groups2, plane, b > 0)

    arrive(copies)
    for k in range(1, ngz):
        own1 += got1[k]
    own1 = jnp.where((lane >= place1) & (lane < place1 + n1), own1, 0.0)
    fs_pair = (fs_hi[...], fs_lo[...])
    s23 = s23 + times(own1, fs_pair)
    s2, s3 = s23[:, 0:128], s23[:, 128:256]

    w2_pair = (w2_h[...], w2_l[...])
    partial = times(s2, w2_pair)
    for g in range(groups2):
        send2[g] = partial[:, 128 * g : 128 * g + 128]
    others = []
    for k in range(1, plane):
        d = lax.rem(me + k, plane)
        others.append((d, (a, lax.div(d, ngz), lax.rem(d, ngz))))
    copies = [send(send2.at[d // 4], got2.at[k], there) for k, (d, there) in enumerate(others, 1)]
    own2 = send2[me // 4]
    arrive(copies)
    for k in range(1, plane):
        own2 += got2[k]
    own2 = jnp.where((lane >= place2) & (lane < place2 + n2), own2, 0.0)
    st_pair = (st_hi[...], st_lo[...])
    s3 = s3 + times(own2, st_pair)

    up_send[...] = s3
    copies = [send(up_send, up_got, at(-1, 0, 0))]
    arrive(copies)
    target = s3 + jnp.where(a < ngx - 1, pltpu.roll(up_got[...], 128 - n3, 1), 0.0)
    columns = jnp.transpose(jnp.concatenate([target, jnp.zeros((8 - rhs, 128), F32)], axis=0))
    spread = [jnp.broadcast_to(columns[0:n3, r : r + 1], (n3, 128)) for r in range(rhs)]

    width = ntop // ngz
    step = 128 if width % 128 == 0 else width
    copies = []
    for j in list(range(1, ngz)) + [0]:
        group = at(0, 0, j)[2]
        for p in range(0, width, step):
            start = group * width + p
            if step == 128:
                start = pl.multiple_of(start, 128)
            block = ti[:, pl.ds(start, step)]
            for r in range(rhs):
                scale = spread[r] if step == 128 else jnp.broadcast_to(spread[r][:, 0:1], (n3, step))
                part[r, group, :, p : p + step] = jnp.sum(scale * block, axis=0, keepdims=True)
        for i in list(range(1, ngy)) + [0]:
            if i or j:
                there = at(0, i, j)
                copies.append(send(part.at[there[1], there[2]], got5.at[i * ngz + j], there))
    term = part[b, c]
    arrive(copies)
    for k in range(1, plane):
        term += got5[k]
    s6[...] = term
    copies = [send(s6, got6.at[k], at(k, 0, 0)) for k in range(1, ngx)]
    arrive(copies)
    for k in range(1, ngx):
        term += got6[k]
    yall[b, c] = term
    copies = [send(yall.at[b, c], yall.at[b, c], there) for _, there in others]
    arrive(copies)

    total = [jnp.zeros((n3, step), F32) for _ in range(rhs)]
    for g in range(ngz):
        for p in range(0, width, step):
            block = ti[:, g * width + p : g * width + p + step]
            for r in range(rhs):
                total[r] += block * yall[r, g, :, p : p + step]
    ones = jnp.ones((8, step), BF16)
    back = jnp.zeros((rhs, n3), F32)
    which = iota((rhs, n3), 0)
    for r in range(rhs):
        hi, lo = split(total[r])
        both_sums = dot(ones, hi, BACK) + dot(ones, lo, BACK)
        back += jnp.where(which == r, both_sums[0:rhs], 0.0)
    down_send[...] = jnp.zeros((rhs, 128), F32)
    down_send[:, 0:n3] = back
    copies = [send(down_send, down_got, at(1, 0, 0))]
    arrive(copies)
    z3 = down_send[...] + jnp.where(a > 0, pltpu.roll(down_got[...], n3, 1), 0.0)

    gap2[me] = own2 + times(z3, st_pair, BACK)
    copies = [send(gap2.at[me], gap2.at[me], there) for _, there in others]
    gap_first = own1 + times(z3, (fs_pair[0][:, 128:256], fs_pair[1][:, 128:256]), BACK)
    arrive(copies)

    def gathered(ref, members):
        blocks = []
        for g in range((members + 3) // 4):
            block = ref[4 * g]
            for i in range(4 * g + 1, min(4 * g + 4, members)):
                block += ref[i]
            blocks.append(block)
        return jnp.concatenate(blocks, axis=1)

    z2 = times(gathered(gap2, plane), w2_pair, BACK)

    gap1[c] = gap_first + times(z2, (fs_pair[0][:, 0:128], fs_pair[1][:, 0:128]), BACK)
    copies = [send(gap1.at[c], gap1.at[c], at(0, 0, k)) for k in range(1, ngz)]
    arrive(copies)
    z1 = times(gathered(gap1, ngz), w1_pair, BACK)

    result = times(jnp.concatenate([s_leaf, z1, z2, z3], axis=1), e_pair, BACK)
    for j in range(4):
        corr[j] = result[:, 128 * j : 128 * j + 128]
    copies = []
    for i, (dx, dy, dz) in enumerate(RIM):
        there = at(-dx, -dy, -dz)
        if dz == 0:
            copies.append(send(corr, got_corr.at[i], there))
        else:
            copies.append(send(corr.at[0], got_corr.at[i, 0], there))

    shape = (fine * fine, 128)
    row, col = floats(shape, 0), floats(shape, 1)
    fx = whole_part(row, fine)
    fy = row - fine * fx
    half = whole_part(col, 64)
    rest = col - 64.0 * half
    cx = whole_part(rest, 8)
    cy = rest - 8.0 * cx - 1.0
    spread_xy = (tent(cx - 1.0, fx) * tent(cy, fy) * 0.0625).astype(BF16)
    shape = (rhs * fine, 8 * rhs)
    row, col = floats(shape, 0), floats(shape, 1)
    fr = whole_part(row, fine)
    fz = row - fine * fr
    cz = whole_part(col, rhs)
    cr = col - rhs * cz
    same = jnp.maximum(1.0 - jnp.abs(cr - fr), 0.0)
    spread_z = (tent(cz - 1.0, fz) * same * 0.25).astype(BF16)

    arrive(copies)
    total = [corr[j] for j in range(4)]
    for i, (dx, dy, dz) in enumerate(RIM):
        turn = side * 8 * dx + side * dy
        keep = (at_x == side + 1) if dx else (at_x <= side)
        keep = keep & ((at_y == side + 1) if dy else (at_y <= side))
        if dx:
            keep = keep & (a < ngx - 1)
        if dy:
            keep = keep & (b < ngy - 1)
        if dz:
            keep = keep & (c < ngz - 1) & (at_z == 1)
        for j in range(4) if dz == 0 else (0,):
            v = got_corr[i, j]
            v = pltpu.roll(v, turn, 1) if turn else v
            total[j if dz == 0 else 3] += jnp.where(keep, v, 0.0)
    rows = []
    for j in range(4):
        rows += [total[j][:, 0:64], total[j][:, 64:128]]
    ct_h, ct_l = split(jnp.concatenate(rows, axis=0))
    ht = dot(spread_z, ct_h) + dot(spread_z, ct_l)
    ht_h = ht.astype(BF16).astype(F32)
    ht = jnp.concatenate([ht_h, ht - ht_h], axis=1)
    stores = []
    for r in range(rhs):
        part_r = ht[r * fine : (r + 1) * fine].astype(BF16)
        out_v[r] = dot(spread_xy, part_r, BACK).reshape(fine, fine, fine)
        store = pltpu.make_async_copy(out_v.at[r], out_h.at[r], out_sem.at[r])
        store.start()
        stores.append(store)
    for copy in pending:
        copy.wait_send()
    for store in stores:
        store.wait()


def per_device(mesh_sizes, *args):
    (rs, it, cf, od, li, lf, ls, lt, fi, fs, ft, si, st, ti) = args
    ngx, ngy, ngz = mesh_sizes
    od = od.reshape(1, -1)
    li, lf, ls, lt, fs, ft, st = (v[0, 0, 0] for v in (li, lf, ls, lt, fs, ft, st))
    fi, si = fi[0, 0], si[0]
    rhs, fine = rs.shape[0], rs.shape[1]
    side = fine // 4
    leaf, n1, n2, n3, ntop = li.shape[0], fs.shape[0], st.shape[0], ti.shape[0], ti.shape[1]
    cfg = (ngx, ngy, ngz, rhs, fine, side, leaf, n1, n2, n3, ntop)
    plane = ngy * ngz
    groups1, groups2 = (ngz + 3) // 4, (plane + 3) // 4
    cells = side**3
    inputs = [rs, it, cf, od, li, lf, ls, lt, fi, fs, ft, si, st, ti]
    v = pltpu.VMEM
    width = ntop // ngz
    copies = len(HALO) + 2 + 3 * (ngz - 1) + 4 * (plane - 1) + 2 + (ngx - 1) + len(RIM)
    scratch = [v(x.shape, x.dtype) for x in inputs]
    scratch += [
        v(rs.shape, F32),
        v((128, fine * fine), BF16),
        v((cells, 512), F32), v((512, 512), BF16), v((512, 512), BF16),
        v((32, 256), F32), v((128, 256), BF16), v((128, 256), BF16),
        v((32, 128), F32), v((128, 128), BF16), v((128, 128), BF16),
        v((128, 128 * groups1), F32), v((128, 128 * groups1), BF16), v((128, 128 * groups1), BF16),
        v((128, 128 * groups2), F32), v((128, 128 * groups2), BF16), v((128, 128 * groups2), BF16),
        v(fi.shape, F32), v(si.shape, F32),
        v((4, rhs, 128), F32), v((len(FLAT), 4, rhs, 128), F32), v((len(HALO) - len(FLAT), rhs, 128), F32),
        v((groups1, rhs, 128), F32), v((ngz, rhs, 128), F32),
        v((groups2, rhs, 128), F32), v((plane, rhs, 128), F32),
        v((rhs, 128), F32), v((rhs, 128), F32),
        v((rhs, ngz, 1, width), F32), v((plane, 1, width), F32),
        v((1, width), F32), v((ngx, 1, width), F32),
        v((rhs, ngz, 1, width), F32),
        v((rhs, 128), F32), v((rhs, 128), F32),
        v((plane, rhs, 128), F32), v((ngz, rhs, 128), F32),
        v((4, rhs, 128), F32), v((len(RIM), 4, rhs, 128), F32),
        pltpu.SemaphoreType.DMA((len(inputs),)), pltpu.SemaphoreType.DMA((rhs,)),
        pltpu.SemaphoreType.DMA((copies,)), pltpu.SemaphoreType.DMA((copies,)),
    ]
    return pl.pallas_call(
        functools.partial(kernel, cfg),
        out_shape=jax.ShapeDtypeStruct(rs.shape, F32),
        in_specs=[pl.BlockSpec(memory_space=pl.ANY)] * len(inputs),
        out_specs=pl.BlockSpec(memory_space=pl.ANY),
        scratch_shapes=scratch,
        compiler_params=pltpu.CompilerParams(
            collective_id=0, has_side_effects=True, vmem_limit_bytes=48 * 1024 * 1024
        ),
        name="coarse_correction",
    )(*inputs)


def solution(mesh):
    sizes = tuple(mesh.shape[n] for n in AXES)
    cells = P("gx", "gy", "gz")
    lines = P("gx", "gy", "gz", None)
    blocks = P("gx", "gy", "gz", None, None)
    field = P(None, "gx", "gy", "gz")
    return jax.shard_map(
        functools.partial(per_device, sizes),
        mesh=mesh,
        in_specs=(
            field, field, cells, lines, blocks, blocks, blocks, blocks, lines, blocks, blocks,
            P("gx", ("gy", "gz"), None), blocks, P(("gx", "gy", "gz"), None),
        ),
        out_specs=field,
        check_vma=False,
    )
```

```python
import contextlib
import functools

import jax
import jax.numpy as jnp
from jax import lax
from jax.experimental import pallas as pl
from jax.experimental.pallas import tpu as pltpu
from jax.sharding import PartitionSpec as P

MESH = pl.DeviceIdType.MESH
F32 = jnp.float32
BF16 = jnp.bfloat16
AXES = ("gx", "gy", "gz")

FLAT = ((1, 0), (-1, 0), (0, 1), (0, -1), (1, 1), (1, -1), (-1, 1))
ABOVE = ((0, 0),) + FLAT
BELOW = ((0, 0), (1, 0), (0, 1), (1, 1))
HALO = [(x, y, 0) for x, y in FLAT] + [(x, y, 1) for x, y in ABOVE] + [(x, y, -1) for x, y in BELOW]
RIM = [(1, 0, 0), (0, 1, 0), (1, 1, 0), (0, 0, 1), (1, 0, 1), (0, 1, 1), (1, 1, 1)]


def split(value):
    high = value.astype(BF16)
    return high, (value - high.astype(F32)).astype(BF16)


def dot(left, right, dims=((1,), (0,))):
    return lax.dot_general(left, right, (dims, ((), ())), preferred_element_type=F32)


def times(value, factor, dims=((1,), (0,))):
    high, low = split(value)
    f_high, f_low = factor
    return dot(high, f_high, dims) + dot(low, f_high, dims) + dot(high, f_low, dims)


BACK = ((1,), (1,))


def iota(shape, dim):
    return lax.broadcasted_iota(jnp.int32, shape, dim)


def floats(shape, dim):
    return iota(shape, dim).astype(F32)


def whole_part(value, by):
    return jnp.floor((value + 0.5) * (1.0 / by))


def tent(coarse, fine):
    return jnp.maximum(4.0 - jnp.abs(fine - 4.0 * coarse), 0.0)


def inner(coarse, fine, first):
    below = 1.0 - first * jnp.maximum(1.0 - fine, 0.0)
    return (tent(coarse, fine + 1.0) + tent(coarse, fine - 1.0) * below) * 0.0625


def outer(coarse, fine):
    return tent(coarse, fine) * 0.0625


def kernel(cfg, *refs):
    ngx, ngy, ngz, rhs, fine, side, leaf, n1, n2, n3, ntop = cfg
    plane = ngy * ngz
    cells = side**3
    (rs_h, it_h, cf_h, or_h, li_h, lf_h, ls_h, lt_h, fi_h, fs_h, ft_h, si_h, st_h, ti_h) = refs[:14]
    out_h = refs[14]
    (
        rs, it, cf, od, li, lf, ls, lt, fi, fs, ft, si, st, ti,
        a21, bmat, e_h, e_l, fsx, fs_hi, fs_lo, stx, st_hi, st_lo,
        w1, w1_h, w1_l, w2, w2_h, w2_l, fi_low, si_low, rall, total_ref,
        flat, got_flat, got_thin, send1, got1, send2, got2, up_send, up_got,
        part, got5, s6, got6, yall, down_send, down_got, gap2, gap1, corr, got_corr,
        local_sem, send_sem, recv_sem,
    ) = refs[15:]

    a, b, c = (lax.axis_index(n) for n in AXES)
    me = b * ngz + c
    used = [0]
    pending = []
    stack = contextlib.ExitStack()

    def phase(name):
        stack.close()
        stack.enter_context(jax.named_scope(name))


    def at(dx, dy, dz):
        return (
            lax.rem(a + (dx + ngx), ngx) if dx else a,
            lax.rem(b + (dy + ngy), ngy) if dy else b,
            lax.rem(c + (dz + ngz), ngz) if dz else c,
        )

    def send(src, dst, device):
        i = used[0]
        used[0] += 1
        copy = pltpu.make_async_remote_copy(
            src_ref=src,
            dst_ref=dst,
            send_sem=send_sem.at[i],
            recv_sem=recv_sem.at[i],
            device_id=device,
            device_id_type=MESH,
        )
        copy.start()
        pending.append(copy)
        return copy

    def arrive(copies):
        for copy in copies:
            copy.wait_recv()

    phase("p00_loads")
    pairs = [
        (it_h, it), (rs_h, rs), (cf_h, cf), (or_h, od), (li_h, li), (lf_h, lf), (ls_h, ls), (lt_h, lt),
        (fi_h, fi), (si_h, si), (fs_h, fs), (ft_h, ft), (st_h, st), (ti_h, ti),
    ]
    pairs = [(s.at[:, 0, :] if len(s.shape) > len(d.shape) else s, d) for s, d in pairs]
    loads = [pltpu.make_async_copy(s, d, local_sem.at[i]) for i, (s, d) in enumerate(pairs)]
    for load in loads:
        load.start()

    phase("p01_signal")
    partners = set()
    for dy in range(ngy):
        for dz in range(ngz):
            partners.add((0, dy, dz))
    for dx in range(ngx):
        partners.add((dx, 0, 0))
    for d in HALO + RIM:
        for s in (1, -1):
            partners.add((s * d[0] % ngx, s * d[1] % ngy, s * d[2] % ngz))
    partners.discard((0, 0, 0))
    barrier = pltpu.get_barrier_semaphore()
    for d in sorted(partners):
        pl.semaphore_signal(barrier, inc=1, device_id=at(*d), device_id_type=MESH)

    first_x = jnp.where(a == 0, 1.0, 0.0).astype(F32)
    first_y = jnp.where(b == 0, 1.0, 0.0).astype(F32)
    first_z = jnp.where(c == 0, 1.0, 0.0).astype(F32)

    phase("p02_weights")
    shape = (64, fine * fine)
    row, col = floats(shape, 0), floats(shape, 1)
    cx = whole_part(row, 8)
    cy = row - 8.0 * cx - 1.0
    cx = cx - 1.0
    fx = whole_part(col, fine)
    fy = col - fine * fx
    ox, oy = outer(cx, fx), outer(cy, fy)
    a21[0:64, :] = (inner(cx, fx, first_x) * oy + ox * inner(cy, fy, first_y)).astype(BF16)
    a21[64:128, :] = (ox * oy).astype(BF16)

    zshape = (8 * rhs, 2 * rhs * fine)
    row, col = floats(zshape, 0), floats(zshape, 1)
    cz = whole_part(row, rhs)
    cr = row - rhs * cz
    cz = cz - 1.0
    kind = whole_part(col, rhs * fine)
    rest = col - rhs * fine * kind
    fr = whole_part(rest, fine)
    fz = rest - fine * fr
    same = jnp.maximum(1.0 - jnp.abs(cr - fr), 0.0)
    wvz = ((1.0 - kind) * outer(cz, fz) + kind * inner(cz, fz, first_z)) * same
    wvz = wvz.astype(BF16)

    phase("p03_wait_residual")
    for load in loads[:3]:
        load.wait()
    g1, g2 = [], []
    own = a21[64:128, :]
    both = a21[...]
    for r in range(rhs):
        now = it[r]
        q = rs[r] - (6.0 + cf[...]) * now
        q_h, q_l = split(q.reshape(fine * fine, fine))
        i_h, i_l = split(now.reshape(fine * fine, fine))
        from_it = dot(both, i_h) + dot(both, i_l)
        g1.append(from_it[0:64] + dot(own, q_h) + dot(own, q_l))
        g2.append(from_it[64:128])
    g_h, g_l = split(jnp.concatenate(g1 + g2, axis=1))
    ct = dot(wvz, g_h, BACK) + dot(wvz, g_l, BACK)
    for j in range(4):
        lo = ct[2 * rhs * j : 2 * rhs * j + rhs]
        hi = ct[2 * rhs * j + rhs : 2 * rhs * j + 2 * rhs]
        flat[j] = jnp.concatenate([lo, hi], axis=1)

    phase("p05_barrier")
    pl.semaphore_wait(barrier, len(partners))

    halo_copies = []
    for i, (dx, dy, dz) in enumerate(HALO):
        if dz == 0:
            src, dst = flat, got_flat.at[i]
        else:
            src, dst = flat.at[3 if dz == 1 else 0], got_thin.at[i - len(FLAT)]
        halo_copies.append(send(src, dst, at(dx, dy, dz)))
    for load in loads[3:]:
        load.wait()
    fi_copy = send(fi, fi_low, at(0, 0, 1))
    si_copy = send(si, si_low, at(0, 1, 0))

    phase("p07_factor")
    shape = (cells, 384)
    m, k = iota(shape, 0), iota(shape, 1)
    e1, e2 = leaf + n1, leaf + n1 + n2
    want = jnp.where(m < e1, m + (192 - leaf), jnp.where(m < e2, m + (128 - e1), m + (256 - e2)))
    bmat[...] = jnp.where((m >= leaf) & (k == want), 1.0, 0.0).astype(F32)
    li_v = li[...]
    li_pair = split(li_v)
    bmat[0:leaf, 0:leaf] = li_v
    bmat[0:leaf, 192 : 192 + 2 * n1] = -times(li_v, split(lf[...]), BACK)
    bmat[0:leaf, 128 : 128 + 2 * n2] = -times(li_v, split(ls[...]), BACK)
    bmat[0:leaf, 256 : 256 + 2 * n3] = -times(li_v, split(lt[...]), BACK)
    bh, bl = split(bmat[...])
    shape = (512, cells)
    k = iota(shape, 0)
    z, x, y = k >> 6, (k >> 3) & 7, k & 7
    inside = (z >= 1) & (z <= side) & (x >= 1) & (x <= side) & (y >= 1) & (y <= side)
    cell = jnp.where(inside, ((x - 1) * side + (y - 1)) * side + (z - 1), -1)
    chosen = jnp.where(cell == od[...], 1.0, 0.0).astype(BF16)
    e_h[...] = dot(chosen, bh).astype(BF16)
    e_l[...] = dot(chosen, bl).astype(BF16)

    phase("p08_place")
    fsx[...] = jnp.zeros(fsx.shape, F32)
    fsx[0:n1, 0 : 2 * n2] = -fs[...]
    fsx[0:n1, 128 : 128 + 2 * n3] = -ft[...]
    stx[...] = jnp.zeros(stx.shape, F32)
    stx[0:n2, 0 : 2 * n3] = -st[...]
    place1 = 32 * lax.rem(c, 4)
    place2 = n2 * lax.rem(me, 4)
    shift = (128, 32)
    put1 = jnp.where(iota(shift, 0) == iota(shift, 1) + place1, 1.0, 0.0).astype(BF16)
    put2 = jnp.where(iota(shift, 0) == iota(shift, 1) + place2, 1.0, 0.0).astype(BF16)
    hi, lo = split(fsx[...])
    fs_hi[...] = dot(put1, hi).astype(BF16)
    fs_lo[...] = dot(put1, lo).astype(BF16)
    hi, lo = split(stx[...])
    st_hi[...] = dot(put2, hi).astype(BF16)
    st_lo[...] = dot(put2, lo).astype(BF16)

    groups1 = (ngz + 3) // 4
    groups2 = (plane + 3) // 4

    phase("p09_w1")
    fi_copy.wait_recv()
    w1[...] = jnp.zeros(w1.shape, F32)
    mine = fi[:, 0, :]
    lower = jnp.where(c > 0, fi_low[:, 0, :], 0.0)
    for m in range(ngz):
        w1[64 : 64 + n1, 32 * m : 32 * m + n1] = mine[:, n1 * m : n1 * m + n1]
        w1[64 + n1 : 64 + 2 * n1, 32 * m : 32 * m + n1] = lower[:, n1 * m : n1 * m + n1]
    hi, lo = split(w1[...])
    w1_h[...] = hi
    w1_l[...] = lo

    phase("p10_wait_halo")
    arrive(halo_copies)
    phase("p11_add_halo")
    lane = iota((rhs, 128), 1)
    at_z, at_x, at_y = lane >> 6, (lane >> 3) & 7, lane & 7

    def along(at_, d):
        if d == 0:
            return (at_ >= 1) & (at_ <= side)
        return at_ == (1 if d == 1 else side)

    def exists(i, d, n):
        return (i - d >= 0) & (i - d < n) if d else True

    total = [flat[j] for j in range(4)]
    for i, (dx, dy, dz) in enumerate(HALO):
        turn = (-(side * 8) * dx - side * dy) % 128
        keep = along(at_x, dx) & along(at_y, dy)
        there = exists(a, dx, ngx) & exists(b, dy, ngy) & exists(c, dz, ngz)
        keep = keep & there
        if dz == 0:
            for j in range(4):
                v = got_flat[i, j]
                v = pltpu.roll(v, turn, 1) if turn else v
                total[j] += jnp.where(keep, v, 0.0)
        else:
            v = got_thin[i - len(FLAT)]
            v = pltpu.roll(v, turn, 1) if turn else v
            keep = keep & (at_z == (1 if dz == 1 else 0))
            j = 0 if dz == 1 else 3
            total[j] += jnp.where(keep, v, 0.0)

    phase("p12_leaf")
    e_pair = (e_h[...], e_l[...])
    s = times(jnp.concatenate(total, axis=1), e_pair)
    s_leaf, s12, s3 = s[:, 0:128], s[:, 128:256], s[:, 256:384]

    phase("p13_first_product")
    w1_pair = (w1_h[...], w1_l[...])
    partial = times(s12, w1_pair)
    for g in range(groups1):
        send1[g] = partial[:, 128 * g : 128 * g + 128]
    copies = []
    for k in range(1, ngz):
        there = at(0, 0, k)
        copies.append(send(send1.at[there[2] // 4], got1.at[k], there))
    own1 = send1[c // 4]

    phase("p15_w2")
    si_copy.wait_recv()
    w2[...] = jnp.zeros(w2.shape, F32)
    mine = si[:, 0, :]
    lower = jnp.where(b > 0, si_low[:, 0, :], 0.0)
    for g in range(groups2):
        wide = min(4, plane - 4 * g) * n2
        cut = slice(4 * g * n2, 4 * g * n2 + wide)
        w2[0:n2, 128 * g : 128 * g + wide] = mine[:, cut]
        w2[n2 : 2 * n2, 128 * g : 128 * g + wide] = lower[:, cut]
    hi, lo = split(w2[...])
    w2_h[0:64, :] = hi
    w2_l[0:64, :] = lo
    back_rows = times(fsx[:, 0:64], (hi, lo))
    rall[c] = back_rows

    phase("p16_wait_first")
    for k, copy in enumerate(copies, 1):
        copy.wait_recv()
        own1 += got1[k]
    phase("p17_second_product")
    own1 = jnp.where((lane >= place1) & (lane < place1 + n1), own1, 0.0)
    fs_pair = (fs_hi[...], fs_lo[...])
    more = times(own1, fs_pair)
    s2, s3 = s12[:, 0:64] + more[:, 0:64], s3 + more[:, 128:256]

    partial = times(s2, (w2_h[0:64, :], w2_l[0:64, :]))
    for g in range(groups2):
        send2[g] = partial[:, 128 * g : 128 * g + 128]
    others = []
    for k in range(1, plane):
        d = lax.rem(me + k, plane)
        others.append((d, (a, lax.div(d, ngz), lax.rem(d, ngz))))
    copies = [send(send2.at[d // 4], got2.at[k], there) for k, (d, there) in enumerate(others, 1)]
    phase("p18_wait_second")
    own2 = send2[me // 4]
    chips = ngz // 2
    other = (a, b, c + 1 - 2 * lax.rem(c, 2))
    beside = [send(rall.at[c], rall.at[c], other)]
    if chips > 1:
        after, before = at(0, 0, 2), at(0, 0, -2)
        beside.append(send(rall.at[c], rall.at[c], after))
        beside.append(send(rall.at[c], rall.at[c], before))
    for k, copy in enumerate(copies, 1):
        copy.wait_recv()
        own2 += got2[k]
    phase("p19_second_done")
    own2 = jnp.where((lane >= place2) & (lane < place2 + n2), own2, 0.0)
    st_pair = (st_hi[...], st_lo[...])
    s3 = s3 + times(own2, st_pair)

    phase("p20_up")
    up_send[...] = s3
    copies = [send(up_send, up_got, at(-1, 0, 0))]
    arrive(copies)
    phase("p21_target")
    target = s3 + jnp.where(a < ngx - 1, pltpu.roll(up_got[...], 128 - n3, 1), 0.0)
    columns = jnp.transpose(jnp.concatenate([target, jnp.zeros((8 - rhs, 128), F32)], axis=0))
    spread = [jnp.broadcast_to(columns[0:n3, r : r + 1], (n3, 128)) for r in range(rhs)]

    phase("p22_top_product")
    width = ntop // ngz
    step = 128 if width % 128 == 0 else width
    copies, slots = [], []
    for j in list(range(1, ngz)) + [0]:
        group = at(0, 0, j)[2]
        for p in range(0, width, step):
            start = group * width + p
            if step == 128:
                start = pl.multiple_of(start, 128)
            block = ti[:, pl.ds(start, step)]
            for r in range(rhs):
                scale = spread[r] if step == 128 else jnp.broadcast_to(spread[r][:, 0:1], (n3, step))
                part[r, group, :, p : p + step] = jnp.sum(scale * block, axis=0, keepdims=True)
        for i in list(range(1, ngy)) + [0]:
            if i or j:
                there = at(0, i, j)
                slots.append(i * ngz + j)
                copies.append(send(part.at[there[1], there[2]], got5.at[i * ngz + j], there))
    phase("p23_wait_top1")
    term = part[b, c]
    for copy, slot in zip(copies, slots):
        copy.wait_recv()
        term += got5[slot]
    phase("p24_top2")
    s6[...] = term
    copies = [send(s6, got6.at[k], at(k, 0, 0)) for k in range(1, ngx)]
    arrive(beside)
    if chips > 1:
        across = [
            send(rall.at[before[2], 0:16], rall.at[before[2], 0:16], after),
            send(rall.at[after[2], 16:32], rall.at[after[2], 16:32], before),
        ]
        beside = [send(rall.at[d[2]], rall.at[d[2]], other) for d in (after, before)]
    for k, copy in enumerate(copies, 1):
        copy.wait_recv()
        term += got6[k]
    phase("p25_top3")
    yall[b, c] = term
    copies = [send(yall.at[b, c], yall.at[b, c], there) for _, there in others]
    if chips > 1:
        far = lax.rem(c + 4, ngz)
        arrive(across)
        beside.append(send(rall.at[far], rall.at[far], other))

    phase("p26_top_back")
    total_ref[...] = jnp.zeros(total_ref.shape, F32)
    for k in range(plane):
        d = lax.rem(me + (plane - k), plane) if k else me
        r, group = lax.div(d, ngz), lax.rem(d, ngz)
        if k:
            copies[k - 1].wait_recv()
        add = total_ref[r]
        for p in range(0, width, step):
            start = group * width + p
            if step == 128:
                start = pl.multiple_of(start, 128)
            add += ti[:, pl.ds(start, step)] * yall[r, group, :, p : p + step]
        total_ref[r] = add
    total = [total_ref[r] for r in range(rhs)]
    ones = jnp.ones((8, step), BF16)
    back = jnp.zeros((rhs, n3), F32)
    which = iota((rhs, n3), 0)
    for r in range(rhs):
        hi, lo = split(total[r])
        both_sums = dot(ones, hi, BACK) + dot(ones, lo, BACK)
        back += jnp.where(which == r, both_sums[0:rhs], 0.0)
    phase("p27_down")
    down_send[...] = jnp.zeros((rhs, 128), F32)
    down_send[:, 0:n3] = back
    copies = [send(down_send, down_got, at(1, 0, 0))]
    arrive(copies)
    phase("p28_gap2")
    z3 = down_send[...] + jnp.where(a > 0, pltpu.roll(down_got[...], n3, 1), 0.0)

    gap2[me] = own2 + times(z3, st_pair, BACK)
    copies = [send(gap2.at[me], gap2.at[me], there) for _, there in others]
    gap1[c] = own1 + times(z3, (fs_pair[0][:, 128:256], fs_pair[1][:, 128:256]), BACK)
    line = [send(gap1.at[c], gap1.at[c], at(0, 0, k)) for k in range(1, ngz)]

    phase("p29_rows")
    arrive(beside[1:] if chips == 1 else beside)
    hi, lo = split(rall[...].reshape(32 * ngz, 128 * groups2))
    rows = dot(w1_h[64:128, 0 : 32 * ngz], hi) + dot(w1_l[64:128, 0 : 32 * ngz], hi) + dot(w1_h[64:128, 0 : 32 * ngz], lo)
    hi, lo = split(rows)
    w2_h[64:128, :] = hi
    w2_l[64:128, :] = lo

    def gathered(ref, members):
        blocks = []
        for g in range((members + 3) // 4):
            block = ref[4 * g]
            for i in range(4 * g + 1, min(4 * g + 4, members)):
                block += ref[i]
            blocks.append(block)
        return jnp.concatenate(blocks, axis=1)

    phase("p30_wait_gap")
    arrive(line)
    z12 = times(gathered(gap1, ngz), w1_pair, BACK)
    arrive(copies)
    phase("p31_z_leaf")
    z12 = z12 + times(gathered(gap2, plane), (w2_h[...], w2_l[...]), BACK)

    result = times(jnp.concatenate([s_leaf, z12, z3], axis=1), e_pair, BACK)
    for j in range(4):
        corr[j] = result[:, 128 * j : 128 * j + 128]
    phase("p32_rim")
    copies = []
    for i, (dx, dy, dz) in enumerate(RIM):
        there = at(-dx, -dy, -dz)
        if dz == 0:
            copies.append(send(corr, got_corr.at[i], there))
        else:
            copies.append(send(corr.at[0], got_corr.at[i, 0], there))

    arrive(copies)
    phase("p33_prolong")
    total = [corr[j] for j in range(4)]
    for i, (dx, dy, dz) in enumerate(RIM):
        turn = side * 8 * dx + side * dy
        keep = (at_x == side + 1) if dx else (at_x <= side)
        keep = keep & ((at_y == side + 1) if dy else (at_y <= side))
        if dx:
            keep = keep & (a < ngx - 1)
        if dy:
            keep = keep & (b < ngy - 1)
        if dz:
            keep = keep & (c < ngz - 1) & (at_z == 1)
        for j in range(4) if dz == 0 else (0,):
            v = got_corr[i, j]
            v = pltpu.roll(v, turn, 1) if turn else v
            total[j if dz == 0 else 3] += jnp.where(keep, v, 0.0)
    rows = []
    for j in range(4):
        rows += [total[j][:, 0:64], total[j][:, 64:128]]
    out_h[...] = jnp.concatenate(rows, axis=0)
    phase("p34_finish")
    for copy in pending:
        copy.wait_send()
    stack.close()


def prolong(cfg, ct, out_h, out_v, out_sem):
    rhs, fine = cfg[3], cfg[4]
    shape = (fine * fine, 128)
    row, col = floats(shape, 0), floats(shape, 1)
    fx = whole_part(row, fine)
    fy = row - fine * fx
    half = whole_part(col, 64)
    rest = col - 64.0 * half
    cx = whole_part(rest, 8)
    cy = rest - 8.0 * cx - 1.0
    spread_xy = (tent(cx - 1.0, fx) * tent(cy, fy) * 0.0625).astype(BF16)
    shape = (rhs * fine, 8 * rhs)
    row, col = floats(shape, 0), floats(shape, 1)
    fr = whole_part(row, fine)
    fz = row - fine * fr
    cz = whole_part(col, rhs)
    cr = col - rhs * cz
    same = jnp.maximum(1.0 - jnp.abs(cr - fr), 0.0)
    spread_z = (tent(cz - 1.0, fz) * same * 0.25).astype(BF16)

    ct_h, ct_l = split(ct[...])
    ht = dot(spread_z, ct_h) + dot(spread_z, ct_l)
    ht_h = ht.astype(BF16).astype(F32)
    ht = jnp.concatenate([ht_h, ht - ht_h], axis=1)
    stores = []
    for r in range(rhs):
        part_r = ht[r * fine : (r + 1) * fine].astype(BF16)
        out_v[r] = dot(spread_xy, part_r, BACK).reshape(fine, fine, fine)
        store = pltpu.make_async_copy(out_v.at[r], out_h.at[r], out_sem.at[r])
        store.start()
        stores.append(store)
    for store in stores:
        store.wait()


def per_device(mesh_sizes, *args):
    (rs, it, cf, od, li, lf, ls, lt, fi, fs, ft, si, st, ti) = args
    ngx, ngy, ngz = mesh_sizes
    od = od.reshape(1, -1)
    rhs, fine = rs.shape[0], rs.shape[1]
    side = fine // 4
    leaf, n1, n2, n3, ntop = li.shape[3], fs.shape[3], st.shape[3], ti.shape[0], ti.shape[1]
    li, fs, ft, st = (jnp.transpose(v, (0, 1, 3, 2, 4))[0, 0] for v in (li, fs, ft, st))
    fi, si = jnp.transpose(fi, (0, 2, 1, 3))[0], jnp.transpose(si, (1, 0, 2))
    lf, ls = (jnp.transpose(v, (0, 1, 4, 2, 3))[0, 0] for v in (lf, ls))
    lt = jnp.transpose(lt, (0, 1, 2, 4, 3))[0, 0, 0]
    cfg = (ngx, ngy, ngz, rhs, fine, side, leaf, n1, n2, n3, ntop)
    plane = ngy * ngz
    groups1, groups2 = (ngz + 3) // 4, (plane + 3) // 4
    cells = side**3
    inputs = [rs, it, cf, od, li, lf, ls, lt, fi, fs, ft, si, st, ti]
    v = pltpu.VMEM
    width = ntop // ngz
    step = 128 if width % 128 == 0 else width
    copies = len(HALO) + 2 + 8 + 2 * (ngz - 1) + 4 * (plane - 1) + 2 + (ngx - 1) + len(RIM)
    narrow = [x.reshape(x.shape[0], -1) if any(x is y for y in (li, lf, ls, fs, ft, st)) else x for x in inputs]
    scratch = [v(x.shape, x.dtype) for x in narrow]
    scratch += [
        v((128, fine * fine), BF16),
        v((cells, 384), F32), v((512, 384), BF16), v((512, 384), BF16),
        v((32, 256), F32), v((128, 256), BF16), v((128, 256), BF16),
        v((32, 128), F32), v((128, 128), BF16), v((128, 128), BF16),
        v((128, 128 * groups1), F32), v((128, 128 * groups1), BF16), v((128, 128 * groups1), BF16),
        v((64, 128 * groups2), F32), v((128, 128 * groups2), BF16), v((128, 128 * groups2), BF16),
        v(fi.shape, F32), v(si.shape, F32), v((ngz, 32, 128 * groups2), F32), v((rhs, n3, step), F32),
        v((4, rhs, 128), F32), v((len(FLAT), 4, rhs, 128), F32), v((len(HALO) - len(FLAT), rhs, 128), F32),
        v((groups1, rhs, 128), F32), v((ngz, rhs, 128), F32),
        v((groups2, rhs, 128), F32), v((plane, rhs, 128), F32),
        v((rhs, 128), F32), v((rhs, 128), F32),
        v((rhs, ngz, 1, width), F32), v((plane, 1, width), F32),
        v((1, width), F32), v((ngx, 1, width), F32),
        v((rhs, ngz, 1, width), F32),
        v((rhs, 128), F32), v((rhs, 128), F32),
        v((plane, rhs, 128), F32), v((ngz, rhs, 128), F32),
        v((4, rhs, 128), F32), v((len(RIM), 4, rhs, 128), F32),
        pltpu.SemaphoreType.DMA((len(inputs),)),
        pltpu.SemaphoreType.DMA((copies,)), pltpu.SemaphoreType.DMA((copies,)),
    ]
    coarse = pl.pallas_call(
        functools.partial(kernel, cfg),
        out_shape=jax.ShapeDtypeStruct((8 * rhs, 64), F32),
        in_specs=[pl.BlockSpec(memory_space=pl.ANY)] * len(inputs),
        out_specs=pl.BlockSpec(memory_space=pltpu.VMEM),
        scratch_shapes=scratch,
        compiler_params=pltpu.CompilerParams(
            collective_id=0, has_side_effects=True, vmem_limit_bytes=67043328
        ),
        name="coarse_correction",
    )(*inputs)
    return pl.pallas_call(
        functools.partial(prolong, cfg),
        out_shape=jax.ShapeDtypeStruct(rs.shape, F32),
        in_specs=[pl.BlockSpec(memory_space=pltpu.VMEM)],
        out_specs=pl.BlockSpec(memory_space=pl.ANY),
        scratch_shapes=[v(rs.shape, F32), pltpu.SemaphoreType.DMA((rhs,))],
        compiler_params=pltpu.CompilerParams(vmem_limit_bytes=67043328),
        name="prolong",
    )(coarse)


def solution(mesh):
    sizes = tuple(mesh.shape[n] for n in AXES)
    cells = P("gx", "gy", "gz")
    lines = P("gx", "gy", "gz", None)
    blocks = P("gx", "gy", "gz", None, None)
    field = P(None, "gx", "gy", "gz")
    return jax.shard_map(
        functools.partial(per_device, sizes),
        mesh=mesh,
        in_specs=(
            field, field, cells, lines, blocks, blocks, blocks, blocks, lines, blocks, blocks,
            P("gx", ("gy", "gz"), None), blocks, P(("gx", "gy", "gz"), None),
        ),
        out_specs=field,
        check_vma=False,
    )
```

```python
import contextlib
import functools

import jax
import jax.numpy as jnp
from jax import lax
from jax.experimental import pallas as pl
from jax.experimental.pallas import tpu as pltpu
from jax.sharding import PartitionSpec as P

MESH = pl.DeviceIdType.MESH
F32 = jnp.float32
BF16 = jnp.bfloat16
AXES = ("gx", "gy", "gz")

FLAT = ((1, 0), (-1, 0), (0, 1), (0, -1), (1, 1), (1, -1), (-1, 1))
ABOVE = ((0, 0),) + FLAT
BELOW = ((0, 0), (1, 0), (0, 1), (1, 1))
HALO = [(x, y, 0) for x, y in FLAT] + [(x, y, 1) for x, y in ABOVE] + [(x, y, -1) for x, y in BELOW]
RIM = [(1, 0, 0), (0, 1, 0), (1, 1, 0), (0, 0, 1), (1, 0, 1), (0, 1, 1), (1, 1, 1)]


def split(value):
    high = value.astype(BF16)
    return high, (value - high.astype(F32)).astype(BF16)


def dot(left, right, dims=((1,), (0,))):
    return lax.dot_general(left, right, (dims, ((), ())), preferred_element_type=F32)


def times(value, factor, dims=((1,), (0,))):
    f_high, f_low = factor
    n = value.shape[0]
    if n > 4:
        high, low = split(value)
        return dot(high, f_high, dims) + dot(low, f_high, dims) + dot(high, f_low, dims)
    high = value.astype(BF16).astype(F32)
    both = jnp.concatenate([high, value - high], axis=0).astype(BF16)
    out = dot(both, f_high, dims) + dot(both, f_low, dims)
    return out[0:n] + out[n : 2 * n]


BACK = ((1,), (1,))


def iota(shape, dim):
    return lax.broadcasted_iota(jnp.int32, shape, dim)


def floats(shape, dim):
    return iota(shape, dim).astype(F32)


def whole_part(value, by):
    return jnp.floor((value + 0.5) * (1.0 / by))


def tent(coarse, fine):
    return jnp.maximum(4.0 - jnp.abs(fine - 4.0 * coarse), 0.0)


def inner(coarse, fine, first):
    below = 1.0 - first * jnp.maximum(1.0 - fine, 0.0)
    return (tent(coarse, fine + 1.0) + tent(coarse, fine - 1.0) * below) * 0.0625


def outer(coarse, fine):
    return tent(coarse, fine) * 0.0625


def kernel(cfg, *refs):
    ngx, ngy, ngz, rhs, fine, side, leaf, n1, n2, n3, ntop = cfg
    plane = ngy * ngz
    cells = side**3
    (rs_h, it_h, cf_h, od_h, li_h, lf_h, ls_h, lt_h, fi_h, fs_h, ft_h, si_h, st_h, ti_h) = refs[:14]
    out_h = refs[14]
    (
        rs, it, cf, od, li, lf, ls, lt, fi, fs, ft, si, st, ti,
        a21, bmat, e_h, e_l, fsx, fs_hi, fs_lo, stx, st_hi, st_lo,
        stu, ftu, back_hi, back_lo, st_high, ft_high,
        w1, w1_h, w1_l, w2, w2_h, w2_l, fi_low, si_low, rall, total_ref, r_hi, r_lo,
        flat, got_flat, got_thin, send1, got1, send2, got2, up_send, up_got,
        part, got5, s6, got6, yall, down_send, down_got, gap2, gap1, low2, low1, corr, got_corr,
        local_sem, word1, word2, word3, send_sem, recv_sem,
    ) = refs[15:]

    a, b, c = (lax.axis_index(n) for n in AXES)
    me = b * ngz + c
    used = [0]
    pending = []
    stack = contextlib.ExitStack()

    def phase(name):
        stack.close()
        stack.enter_context(jax.named_scope(name))


    def at(dx, dy, dz):
        return (
            lax.rem(a + (dx + ngx), ngx) if dx else a,
            lax.rem(b + (dy + ngy), ngy) if dy else b,
            lax.rem(c + (dz + ngz), ngz) if dz else c,
        )

    def far_first(d):
        return -sum(min(i % n, -i % n) * w for i, n, w in zip(d, (ngx, ngy, ngz), (2, 2, 1))), d

    def send(src, dst, device):
        i = used[0]
        used[0] += 1
        copy = pltpu.make_async_remote_copy(
            src_ref=src,
            dst_ref=dst,
            send_sem=send_sem.at[i],
            recv_sem=recv_sem.at[i],
            device_id=device,
            device_id_type=MESH,
        )
        copy.start()
        pending.append(copy)
        return copy

    def arrive(copies):
        for copy in copies:
            copy.wait_recv()

    phase("p00_loads")
    first = [(cf_h, cf)]
    for r in range(rhs):
        first += [(it_h.at[r], it.at[r]), (rs_h.at[r], rs.at[r])]
    pairs = [
        (od_h, od), (li_h, li), (lf_h, lf), (ls_h, ls), (lt_h, lt),
        (fi_h, fi), (si_h, si), (fs_h, fs), (ft_h, ft), (st_h, st),
    ]
    pairs = first + [(s.at[:, 0, :] if len(s.shape) > len(d.shape) else s, d) for s, d in pairs] + [(ti_h, ti)]
    loads = [pltpu.make_async_copy(s, d, local_sem.at[i]) for i, (s, d) in enumerate(pairs)]
    for load in loads[:-1]:
        load.start()

    phase("p01_signal")
    partners = {(0, 0, dz) for dz in range(ngz)}
    for d in HALO + RIM:
        for s in (1, -1):
            partners.add((s * d[0] % ngx, s * d[1] % ngy, s * d[2] % ngz))
    partners.discard((0, 0, 0))
    barrier = pltpu.get_barrier_semaphore()
    for d in sorted(partners, key=far_first):
        pl.semaphore_signal(barrier, inc=1, device_id=at(*d), device_id_type=MESH)

    first_x = jnp.where(a == 0, 1.0, 0.0).astype(F32)
    first_y = jnp.where(b == 0, 1.0, 0.0).astype(F32)
    first_z = jnp.where(c == 0, 1.0, 0.0).astype(F32)

    phase("p02_weights")
    shape = (64, fine * fine)
    row, col = floats(shape, 0), floats(shape, 1)
    cx = whole_part(row, 8)
    cy = row - 8.0 * cx - 1.0
    cx = cx - 1.0
    fx = whole_part(col, fine)
    fy = col - fine * fx
    ox, oy = outer(cx, fx), outer(cy, fy)
    a21[0:64, :] = (inner(cx, fx, first_x) * oy + ox * inner(cy, fy, first_y)).astype(BF16)
    a21[64:128, :] = (ox * oy).astype(BF16)

    zshape = (8 * rhs, 2 * rhs * fine)
    row, col = floats(zshape, 0), floats(zshape, 1)
    cz = whole_part(row, rhs)
    cr = row - rhs * cz
    cz = cz - 1.0
    kind = whole_part(col, rhs * fine)
    rest = col - rhs * fine * kind
    fr = whole_part(rest, fine)
    fz = rest - fine * fr
    same = jnp.maximum(1.0 - jnp.abs(cr - fr), 0.0)
    wvz = ((1.0 - kind) * outer(cz, fz) + kind * inner(cz, fz, first_z)) * same
    wvz = wvz.astype(BF16)

    phase("p03_wait_residual")
    loads[0].wait()
    diagonal = 6.0 + cf[...]
    its, qs = [], []
    for r in range(rhs):
        loads[2 * r + 1].wait()
        loads[2 * r + 2].wait()
        now = it[r]
        its.append(now.reshape(fine * fine, fine))
        qs.append((rs[r] - diagonal * now).reshape(fine * fine, fine))
    i_h, i_l = split(jnp.concatenate(its, axis=1))
    q_h, q_l = split(jnp.concatenate(qs, axis=1))
    own = a21[64:128, :]
    both = a21[...]
    from_it = dot(both, i_h) + dot(both, i_l)
    g1 = from_it[0:64] + dot(own, q_h) + dot(own, q_l)
    g_h, g_l = split(jnp.concatenate([g1, from_it[64:128]], axis=1))
    ct = dot(wvz, g_h, BACK) + dot(wvz, g_l, BACK)
    for j in range(4):
        lo = ct[2 * rhs * j : 2 * rhs * j + rhs]
        hi = ct[2 * rhs * j + rhs : 2 * rhs * j + 2 * rhs]
        flat[j] = jnp.concatenate([lo, hi], axis=1)

    phase("p05_barrier")
    pl.semaphore_wait(barrier, len(partners))

    halo_copies = []
    for i, (dx, dy, dz) in enumerate(HALO):
        if dz == 0:
            src, dst = flat, got_flat.at[i]
        else:
            src, dst = flat.at[3 if dz == 1 else 0], got_thin.at[i - len(FLAT)]
        halo_copies.append(send(src, dst, at(dx, dy, dz)))
    def tell(sem):
        for dx in (1, -1):
            pl.semaphore_signal(sem, inc=1, device_id=at(dx, 0, 0), device_id_type=MESH)

    tell(word1)
    loads[-1].start()
    for load in loads[1 + 2 * rhs : -1]:
        load.wait()
    fi_copy = send(fi, fi_low, at(0, 0, 1))
    si_copy = send(si, si_low, at(0, 1, 0))
    st_copy = send(st, st_high, at(-1, 0, 0))
    ft_copy = send(ft, ft_high, at(-1, 0, 0))

    phase("p07_factor")
    shape = (cells, 384)
    m, k = iota(shape, 0), iota(shape, 1)
    e1, e2 = leaf + n1, leaf + n1 + n2
    want = jnp.where(m < e1, m + (192 - leaf), jnp.where(m < e2, m + (128 - e1), m + (256 - e2)))
    bmat[...] = jnp.where((m >= leaf) & (k == want), 1.0, 0.0).astype(F32)
    li_v = li[...]
    li_pair = split(li_v)
    bmat[0:leaf, 0:leaf] = li_v
    bmat[0:leaf, 192 : 192 + 2 * n1] = -times(li_v, split(lf[...]), BACK)
    bmat[0:leaf, 128 : 128 + 2 * n2] = -times(li_v, split(ls[...]), BACK)
    bmat[0:leaf, 256 : 256 + 2 * n3] = -times(li_v, split(lt[...]), BACK)
    bh, bl = split(bmat[...])
    shape = (512, cells)
    k = iota(shape, 0)
    z, x, y = k >> 6, (k >> 3) & 7, k & 7
    inside = (z >= 1) & (z <= side) & (x >= 1) & (x <= side) & (y >= 1) & (y <= side)
    cell = jnp.where(inside, ((x - 1) * side + (y - 1)) * side + (z - 1), -1)
    chosen = jnp.where(cell == od[...], 1.0, 0.0).astype(BF16)
    e_h[...] = dot(chosen, bh).astype(BF16)
    e_l[...] = dot(chosen, bl).astype(BF16)

    phase("p08_place")
    fsx[...] = jnp.zeros(fsx.shape, F32)
    fsx[0:n1, 0 : 2 * n2] = -fs[...]
    fsx[0:n1, 128 : 128 + 2 * n3] = -ft[...]
    stx[...] = jnp.zeros(stx.shape, F32)
    stx[0:n2, 0 : 2 * n3] = -st[...]
    place1 = 32 * lax.rem(c, 4)
    place2 = n2 * lax.rem(me, 4)
    shift = (128, 32)
    put1 = jnp.where(iota(shift, 0) == iota(shift, 1) + place1, 1.0, 0.0).astype(BF16)
    put2 = jnp.where(iota(shift, 0) == iota(shift, 1) + place2, 1.0, 0.0).astype(BF16)
    hi, lo = split(fsx[...])
    fs_hi[...] = dot(put1, hi).astype(BF16)
    fs_lo[...] = dot(put1, lo).astype(BF16)
    hi, lo = split(stx[...])
    st_hi[0:128, :] = dot(put2, hi).astype(BF16)
    st_lo[0:128, :] = dot(put2, lo).astype(BF16)

    groups1 = (ngz + 3) // 4
    groups2 = (plane + 3) // 4

    phase("p09_w1")
    fi_copy.wait_recv()
    w1[...] = jnp.zeros(w1.shape, F32)
    mine = fi[:, 0, :]
    lower = jnp.where(c > 0, fi_low[:, 0, :], 0.0)
    for m in range(ngz):
        w1[64 : 64 + n1, 32 * m : 32 * m + n1] = mine[:, n1 * m : n1 * m + n1]
        w1[64 + n1 : 64 + 2 * n1, 32 * m : 32 * m + n1] = lower[:, n1 * m : n1 * m + n1]
    hi, lo = split(w1[...])
    w1_h[...] = hi
    w1_l[...] = lo

    phase("p10_wait_halo")
    arrive(halo_copies)
    phase("p11_add_halo")
    lane = iota((rhs, 128), 1)
    at_z, at_x, at_y = lane >> 6, (lane >> 3) & 7, lane & 7

    def along(at_, d):
        if d == 0:
            return (at_ >= 1) & (at_ <= side)
        return at_ == (1 if d == 1 else side)

    def exists(i, d, n):
        return (i - d >= 0) & (i - d < n) if d else True

    total = [flat[j] for j in range(4)]
    for i, (dx, dy, dz) in enumerate(HALO):
        turn = (-(side * 8) * dx - side * dy) % 128
        keep = along(at_x, dx) & along(at_y, dy)
        there = exists(a, dx, ngx) & exists(b, dy, ngy) & exists(c, dz, ngz)
        keep = keep & there
        if dz == 0:
            for j in range(4):
                v = got_flat[i, j]
                v = pltpu.roll(v, turn, 1) if turn else v
                total[j] += jnp.where(keep, v, 0.0)
        else:
            v = got_thin[i - len(FLAT)]
            v = pltpu.roll(v, turn, 1) if turn else v
            keep = keep & (at_z == (1 if dz == 1 else 0))
            j = 0 if dz == 1 else 3
            total[j] += jnp.where(keep, v, 0.0)

    phase("p12_leaf")
    e_pair = (e_h[...], e_l[...])
    s = times(jnp.concatenate(total, axis=1), e_pair)
    s_leaf, s12, s3 = s[:, 0:128], s[:, 128:256], s[:, 256:384]

    phase("p13_first_product")
    word = pl.semaphore_wait
    word(word1, 2)
    tell(word2)

    w1_pair = (w1_h[...], w1_l[...])
    partial = times(s12, w1_pair)
    for g in range(groups1):
        send1[g] = partial[:, 128 * g : 128 * g + 128]
    steps = sorted(range(1, ngz), key=lambda k: -min(k, ngz - k))
    copies = []
    for k in steps:
        there = at(0, 0, k)
        copies.append(send(send1.at[there[2] // 4], got1.at[k], there))
    own1 = send1[c // 4]

    phase("p15_w2")
    si_copy.wait_recv()
    w2[...] = jnp.zeros(w2.shape, F32)
    mine = si[:, 0, :]
    lower = jnp.where(b > 0, si_low[:, 0, :], 0.0)
    for g in range(groups2):
        wide = min(4, plane - 4 * g) * n2
        cut = slice(4 * g * n2, 4 * g * n2 + wide)
        w2[0:n2, 128 * g : 128 * g + wide] = mine[:, cut]
        w2[n2 : 2 * n2, 128 * g : 128 * g + wide] = lower[:, cut]
    hi, lo = split(w2[...])
    w2_h[0:64, :] = hi
    w2_l[0:64, :] = lo
    back_rows = times(fsx[:, 0:64], (hi, lo))
    rall[c] = back_rows
    rows_h, rows_l = split(back_rows)
    r_hi[...] = dot(put1, rows_h).astype(BF16)
    r_lo[...] = dot(put1, rows_l).astype(BF16)
    partial = times(s12[:, 0:64], (hi, lo))

    phase("p16_wait_first")
    for k, copy in reversed(list(zip(steps, copies))):
        copy.wait_recv()
        own1 += got1[k]
    phase("p17_second_product")
    own1 = jnp.where((lane >= place1) & (lane < place1 + n1), own1, 0.0)
    partial = partial + times(own1, (r_hi[...], r_lo[...]))
    for g in range(groups2):
        send2[g] = partial[:, 128 * g : 128 * g + 128]
    offsets = [(dy, dz) for dy in range(ngy) for dz in range(ngz) if dy or dz]
    offsets = sorted(offsets, key=lambda d: far_first((0,) + d))
    copies, copies_up = [], []

    def group_of(there):
        return (there[1] * ngz + there[2]) // 4

    for dy, dz in offsets:
        there = at(-1, dy, dz)
        copies_up.append(send(send2.at[group_of(there)], got2.at[1, dy * ngz + dz], there))
    for dy, dz in offsets:
        there = at(0, dy, dz)
        copies.append(send(send2.at[group_of(there)], got2.at[0, dy * ngz + dz], there))
    copies_up.append(send(send2.at[me // 4], got2.at[1, 0], at(-1, 0, 0)))
    word(word2, 2)
    tell(word3)
    own2 = send2[me // 4]

    fs_top = (fs_hi[:, 128:256], fs_lo[:, 128:256])
    s3 = s3 + times(own1, fs_top)
    up_send[...] = s3
    up_copy = send(up_send, up_got, at(-1, 0, 0))

    phase("p18_wait_second")
    stu[...] = jnp.zeros(stu.shape, F32)
    ftu[...] = jnp.zeros(ftu.shape, F32)
    st_copy.wait_recv()
    ft_copy.wait_recv()
    stu[0:n2, 0:n3] = -st_high[:, n3 : 2 * n3]
    ftu[0:n1, 0:n3] = -ft_high[:, n3 : 2 * n3]
    for ref, put, row in ((stu, put2, 128), (ftu, put1, 384)):
        hi, lo = split(jnp.where(a < ngx - 1, ref[...], 0.0))
        back_hi[row : row + 128, :] = dot(put, hi).astype(BF16)
        back_lo[row : row + 128, :] = dot(put, lo).astype(BF16)
    column = iota((128, 128), 1)
    for got, src in ((back_hi, (st_hi[0:128, :], fs_top[0])), (back_lo, (st_lo[0:128, :], fs_top[1]))):
        for row, rows in zip((0, 256), src):
            got[row : row + 128, :] = jnp.where(column < n3, rows.astype(F32), 0.0).astype(BF16)
    st_hi[128:256, :] = back_hi[128:256, :]
    st_lo[128:256, :] = back_lo[128:256, :]
    chips = ngz // 2
    other = (a, b, c + 1 - 2 * lax.rem(c, 2))
    beside = [send(rall.at[c], rall.at[c], other)]
    if chips > 1:
        after, before = at(0, 0, 2), at(0, 0, -2)
        beside.append(send(rall.at[c], rall.at[c], after))
        beside.append(send(rall.at[c], rall.at[c], before))
    up_copy.wait_recv()
    copies_up[-1].wait_recv()
    above = got2[1, 0]
    target = s3 + jnp.where(a < ngx - 1, pltpu.roll(up_got[...], 128 - n3, 1), 0.0)
    for (dy, dz), copy, copy_up in reversed(list(zip(offsets, copies, copies_up))):
        copy.wait_recv()
        own2 += got2[0, dy * ngz + dz]
        copy_up.wait_recv()
        above += got2[1, dy * ngz + dz]
    phase("p21_target")
    mine = (lane >= place2) & (lane < place2 + n2)
    own2 = jnp.where(mine, own2, 0.0)
    above = jnp.where(mine, above, 0.0)
    target = target + times(jnp.concatenate([own2, above], axis=1), (st_hi[...], st_lo[...]))
    columns = jnp.transpose(jnp.concatenate([target, jnp.zeros((8 - rhs, 128), F32)], axis=0))
    spread = [jnp.broadcast_to(columns[0:n3, r : r + 1], (n3, 128)) for r in range(rhs)]

    phase("p22_top_product")
    width = ntop // ngz
    step = 128 if width % 128 == 0 else width
    loads[-1].wait()
    copies, slots = [], []
    for j in steps + [0]:
        group = at(0, 0, j)[2]
        for p in range(0, width, step):
            start = group * width + p
            if step == 128:
                start = pl.multiple_of(start, 128)
            block = ti[:, pl.ds(start, step)]
            for r in range(rhs):
                scale = spread[r] if step == 128 else jnp.broadcast_to(spread[r][:, 0:1], (n3, step))
                part[r, group, :, p : p + step] = jnp.sum(scale * block, axis=0, keepdims=True)
        for i in sorted(range(ngy), key=lambda i: -min(i, ngy - i)):
            if i or j:
                there = at(0, i, j)
                slots.append(i * ngz + j)
                copies.append(send(part.at[there[1], there[2]], got5.at[i * ngz + j], there))
    phase("p23_wait_top1")
    term = part[b, c]
    near = sorted(zip(slots, copies), key=lambda e: far_first((0, e[0] // ngz, e[0] % ngz)), reverse=True)
    for slot, copy in near:
        copy.wait_recv()
        term += got5[slot]
    word(word3, 2)
    phase("p24_top2")
    s6[...] = term
    along_x = sorted(range(1, ngx), key=lambda k: -min(k, ngx - k))
    copies = [send(s6, got6.at[k], at(k, 0, 0)) for k in along_x]
    arrive(beside)
    if chips > 1:
        across = [
            send(rall.at[before[2], 0:16], rall.at[before[2], 0:16], after),
            send(rall.at[after[2], 16:32], rall.at[after[2], 16:32], before),
        ]
        beside = [send(rall.at[d[2]], rall.at[d[2]], other) for d in (after, before)]
    for k, copy in reversed(list(zip(along_x, copies))):
        copy.wait_recv()
        term += got6[k]
    phase("p25_top3")
    yall[b, c] = term
    copies = [send(yall.at[b, c], yall.at[b, c], at(0, dy, dz)) for dy, dz in offsets]
    if chips > 1:
        far = lax.rem(c + 4, ngz)
        arrive(across)
        beside.append(send(rall.at[far], rall.at[far], other))

    phase("p26_top_back")
    total_ref[...] = jnp.zeros(total_ref.shape, F32)
    for (dy, dz), copy in [((0, 0), None)] + list(reversed(list(zip(offsets, copies)))):
        _, r, group = at(0, -dy, -dz)
        if copy is not None:
            copy.wait_recv()
        add = total_ref[r]
        for p in range(0, width, step):
            start = group * width + p
            if step == 128:
                start = pl.multiple_of(start, 128)
            add += ti[:, pl.ds(start, step)] * yall[r, group, :, p : p + step]
        total_ref[r] = add
    total = [total_ref[r] for r in range(rhs)]
    ones = jnp.ones((8, step), BF16)
    back = jnp.zeros((rhs, n3), F32)
    which = iota((rhs, n3), 0)
    for r in range(rhs):
        hi, lo = split(total[r])
        both_sums = dot(ones, hi, BACK) + dot(ones, lo, BACK)
        back += jnp.where(which == r, both_sums[0:rhs], 0.0)
    phase("p27_down")
    down_send[...] = jnp.zeros((rhs, 128), F32)
    down_send[:, 0:n3] = back
    right_sides = times(down_send[...], (back_hi[...], back_lo[...]), BACK)
    gap2[0, me] = own2 + right_sides[:, 0:128]
    low2[...] = right_sides[:, 128:256]
    gap1[0, c] = own1 + right_sides[:, 256:384]
    low1[...] = right_sides[:, 384:512]
    copies = [send(low2, gap2.at[1, me], at(1, dy, dz)) for dy, dz in offsets]
    copies += [send(gap2.at[0, me], gap2.at[0, me], at(0, dy, dz)) for dy, dz in offsets]
    copies.append(send(low2, gap2.at[1, me], at(1, 0, 0)))
    line = [send(low1, gap1.at[1, c], at(1, 0, k)) for k in steps + [0]]
    line += [send(gap1.at[0, c], gap1.at[0, c], at(0, 0, k)) for k in steps]
    down_copy = send(down_send, down_got, at(1, 0, 0))

    phase("p29_rows")
    arrive(beside[1:] if chips == 1 else beside)
    hi, lo = split(rall[...].reshape(32 * ngz, 128 * groups2))
    rows = dot(w1_h[64:128, 0 : 32 * ngz], hi) + dot(w1_l[64:128, 0 : 32 * ngz], hi) + dot(w1_h[64:128, 0 : 32 * ngz], lo)
    hi, lo = split(rows)
    w2_h[64:128, :] = hi
    w2_l[64:128, :] = lo

    def gathered(ref, members):
        blocks = []
        for g in range((members + 3) // 4):
            own_part, lower_part = ref[0, 4 * g], ref[1, 4 * g]
            for i in range(4 * g + 1, min(4 * g + 4, members)):
                own_part += ref[0, i]
                lower_part += ref[1, i]
            blocks.append(own_part + jnp.where(a > 0, lower_part, 0.0))
        return jnp.concatenate(blocks, axis=1)

    phase("p30_wait_gap")
    arrive([down_copy])
    z3 = down_send[...] + jnp.where(a > 0, pltpu.roll(down_got[...], n3, 1), 0.0)
    corr_part = times(jnp.concatenate([s_leaf, z3], axis=1), tuple(jnp.concatenate([e[:, 0:128], e[:, 256:384]], axis=1) for e in e_pair), BACK)
    arrive(line)
    z12 = times(gathered(gap1, ngz), w1_pair, BACK)
    arrive(copies)
    phase("p31_z_leaf")
    z12 = z12 + times(gathered(gap2, plane), (w2_h[...], w2_l[...]), BACK)

    result = corr_part + times(z12, (e_h[:, 128:256], e_l[:, 128:256]), BACK)
    for j in range(4):
        corr[j] = result[:, 128 * j : 128 * j + 128]
    phase("p32_rim")
    copies = []
    for i, (dx, dy, dz) in enumerate(RIM):
        there = at(-dx, -dy, -dz)
        if dz == 0:
            copies.append(send(corr, got_corr.at[i], there))
        else:
            copies.append(send(corr.at[0], got_corr.at[i, 0], there))

    arrive(copies)
    phase("p33_prolong")
    total = [corr[j] for j in range(4)]
    for i, (dx, dy, dz) in enumerate(RIM):
        turn = side * 8 * dx + side * dy
        keep = (at_x == side + 1) if dx else (at_x <= side)
        keep = keep & ((at_y == side + 1) if dy else (at_y <= side))
        if dx:
            keep = keep & (a < ngx - 1)
        if dy:
            keep = keep & (b < ngy - 1)
        if dz:
            keep = keep & (c < ngz - 1) & (at_z == 1)
        for j in range(4) if dz == 0 else (0,):
            v = got_corr[i, j]
            v = pltpu.roll(v, turn, 1) if turn else v
            total[j if dz == 0 else 3] += jnp.where(keep, v, 0.0)
    rows = []
    for j in range(4):
        rows += [total[j][:, 0:64], total[j][:, 64:128]]
    out_h[...] = jnp.concatenate(rows, axis=0)
    phase("p34_finish")
    for copy in pending:
        copy.wait_send()
    stack.close()


def prolong(cfg, ct, out_h, out_v, out_sem):
    rhs, fine = cfg[3], cfg[4]
    shape = (fine * fine, 128)
    row, col = floats(shape, 0), floats(shape, 1)
    fx = whole_part(row, fine)
    fy = row - fine * fx
    half = whole_part(col, 64)
    rest = col - 64.0 * half
    cx = whole_part(rest, 8)
    cy = rest - 8.0 * cx - 1.0
    spread_xy = (tent(cx - 1.0, fx) * tent(cy, fy) * 0.0625).astype(BF16)
    shape = (rhs * fine, 8 * rhs)
    row, col = floats(shape, 0), floats(shape, 1)
    fr = whole_part(row, fine)
    fz = row - fine * fr
    cz = whole_part(col, rhs)
    cr = col - rhs * cz
    same = jnp.maximum(1.0 - jnp.abs(cr - fr), 0.0)
    spread_z = (tent(cz - 1.0, fz) * same * 0.25).astype(BF16)

    ct_h, ct_l = split(ct[...])
    ht = dot(spread_z, ct_h) + dot(spread_z, ct_l)
    ht_h = ht.astype(BF16).astype(F32)
    ht = jnp.concatenate([ht_h, ht - ht_h], axis=1)
    stores = []
    for r in range(rhs):
        part_r = ht[r * fine : (r + 1) * fine].astype(BF16)
        out_v[r] = dot(spread_xy, part_r, BACK).reshape(fine, fine, fine)
        store = pltpu.make_async_copy(out_v.at[r], out_h.at[r], out_sem.at[r])
        store.start()
        stores.append(store)
    for store in stores:
        store.wait()


def per_device(mesh_sizes, *args):
    (rs, it, cf, od, li, lf, ls, lt, fi, fs, ft, si, st, ti) = args
    ngx, ngy, ngz = mesh_sizes
    od = od.reshape(1, -1)
    rhs, fine = rs.shape[0], rs.shape[1]
    side = fine // 4
    leaf, n1, n2, n3, ntop = li.shape[3], fs.shape[3], st.shape[3], ti.shape[0], ti.shape[1]
    li, fs, ft, st = (jnp.transpose(v, (0, 1, 3, 2, 4))[0, 0] for v in (li, fs, ft, st))
    fi, si = jnp.transpose(fi, (0, 2, 1, 3))[0], jnp.transpose(si, (1, 0, 2))
    lf, ls = (jnp.transpose(v, (0, 1, 4, 2, 3))[0, 0] for v in (lf, ls))
    lt = jnp.transpose(lt, (0, 1, 2, 4, 3))[0, 0, 0]
    cfg = (ngx, ngy, ngz, rhs, fine, side, leaf, n1, n2, n3, ntop)
    plane = ngy * ngz
    groups1, groups2 = (ngz + 3) // 4, (plane + 3) // 4
    cells = side**3
    inputs = [rs, it, cf, od, li, lf, ls, lt, fi, fs, ft, si, st, ti]
    v = pltpu.VMEM
    width = ntop // ngz
    step = 128 if width % 128 == 0 else width
    copies = len(HALO) + 4 + 8 + 3 * ngz - 2 + 6 * plane - 4 + 2 + (ngx - 1) + len(RIM)
    narrow = [x.reshape(x.shape[0], -1) if any(x is y for y in (li, lf, ls, fs, ft, st)) else x for x in inputs]
    scratch = [v(x.shape, x.dtype) for x in narrow]
    scratch += [
        v((128, fine * fine), BF16),
        v((cells, 384), F32), v((512, 384), BF16), v((512, 384), BF16),
        v((32, 256), F32), v((128, 256), BF16), v((128, 256), BF16),
        v((32, 128), F32), v((256, 128), BF16), v((256, 128), BF16),
        v((32, 128), F32), v((32, 128), F32), v((512, 128), BF16), v((512, 128), BF16), v(st.shape[::2], F32), v(ft.shape[::2], F32),
        v((128, 128 * groups1), F32), v((128, 128 * groups1), BF16), v((128, 128 * groups1), BF16),
        v((64, 128 * groups2), F32), v((128, 128 * groups2), BF16), v((128, 128 * groups2), BF16),
        v(fi.shape, F32), v(si.shape, F32), v((ngz, 32, 128 * groups2), F32), v((rhs, n3, step), F32),
        v((128, 128 * groups2), BF16), v((128, 128 * groups2), BF16),
        v((4, rhs, 128), F32), v((len(FLAT), 4, rhs, 128), F32), v((len(HALO) - len(FLAT), rhs, 128), F32),
        v((groups1, rhs, 128), F32), v((ngz, rhs, 128), F32),
        v((groups2, rhs, 128), F32), v((2, plane, rhs, 128), F32),
        v((rhs, 128), F32), v((rhs, 128), F32),
        v((rhs, ngz, 1, width), F32), v((plane, 1, width), F32),
        v((1, width), F32), v((ngx, 1, width), F32),
        v((rhs, ngz, 1, width), F32),
        v((rhs, 128), F32), v((rhs, 128), F32),
        v((2, plane, rhs, 128), F32), v((2, ngz, rhs, 128), F32), v((rhs, 128), F32), v((rhs, 128), F32),
        v((4, rhs, 128), F32), v((len(RIM), 4, rhs, 128), F32),
        pltpu.SemaphoreType.DMA((len(inputs) + 2 * rhs - 2,)),
        *[pltpu.SemaphoreType.REGULAR] * 3,
        pltpu.SemaphoreType.DMA((copies,)), pltpu.SemaphoreType.DMA((copies,)),
    ]
    coarse = pl.pallas_call(
        functools.partial(kernel, cfg),
        out_shape=jax.ShapeDtypeStruct((8 * rhs, 64), F32),
        in_specs=[pl.BlockSpec(memory_space=pl.ANY)] * len(inputs),
        out_specs=pl.BlockSpec(memory_space=pltpu.VMEM),
        scratch_shapes=scratch,
        compiler_params=pltpu.CompilerParams(
            collective_id=0, has_side_effects=True, vmem_limit_bytes=67043328
        ),
        name="coarse_correction",
    )(*inputs)
    return pl.pallas_call(
        functools.partial(prolong, cfg),
        out_shape=jax.ShapeDtypeStruct(rs.shape, F32),
        in_specs=[pl.BlockSpec(memory_space=pltpu.VMEM)],
        out_specs=pl.BlockSpec(memory_space=pl.ANY),
        scratch_shapes=[v(rs.shape, F32), pltpu.SemaphoreType.DMA((rhs,))],
        compiler_params=pltpu.CompilerParams(vmem_limit_bytes=67043328),
        name="prolong",
    )(coarse)


def solution(mesh):
    sizes = tuple(mesh.shape[n] for n in AXES)
    cells = P("gx", "gy", "gz")
    lines = P("gx", "gy", "gz", None)
    blocks = P("gx", "gy", "gz", None, None)
    field = P(None, "gx", "gy", "gz")
    return jax.shard_map(
        functools.partial(per_device, sizes),
        mesh=mesh,
        in_specs=(
            field, field, cells, lines, blocks, blocks, blocks, blocks, lines, blocks, blocks,
            P("gx", ("gy", "gz"), None), blocks, P(("gx", "gy", "gz"), None),
        ),
        out_specs=field,
        check_vma=False,
    )
```

```python
import contextlib
import functools

import jax
import jax.numpy as jnp
from jax import lax
from jax.experimental import pallas as pl
from jax.experimental.pallas import tpu as pltpu
from jax.sharding import PartitionSpec as P

MESH = pl.DeviceIdType.MESH
F32 = jnp.float32
BF16 = jnp.bfloat16
AXES = ("gx", "gy", "gz")

FLAT = ((1, 0), (-1, 0), (0, 1), (0, -1), (1, 1), (1, -1), (-1, 1))
ABOVE = ((0, 0),) + FLAT
BELOW = ((0, 0), (1, 0), (0, 1), (1, 1))
HALO = [(x, y, 0) for x, y in FLAT] + [(x, y, 1) for x, y in ABOVE] + [(x, y, -1) for x, y in BELOW]
RIM = [(1, 0, 0), (0, 1, 0), (1, 1, 0), (0, 0, 1), (1, 0, 1), (0, 1, 1), (1, 1, 1)]


def split(value):
    high = value.astype(BF16)
    return high, (value - high.astype(F32)).astype(BF16)


def dot(left, right, dims=((1,), (0,))):
    return lax.dot_general(left, right, (dims, ((), ())), preferred_element_type=F32)


def times(value, factor, dims=((1,), (0,))):
    f_high, f_low = factor
    n = value.shape[0]
    if n > 4:
        high, low = split(value)
        return dot(high, f_high, dims) + dot(low, f_high, dims) + dot(high, f_low, dims)
    high = value.astype(BF16).astype(F32)
    both = jnp.concatenate([high, value - high], axis=0).astype(BF16)
    out = dot(both, f_high, dims) + dot(both, f_low, dims)
    return out[0:n] + out[n : 2 * n]


BACK = ((1,), (1,))


def iota(shape, dim):
    return lax.broadcasted_iota(jnp.int32, shape, dim)


def floats(shape, dim):
    return iota(shape, dim).astype(F32)


def whole_part(value, by):
    return jnp.floor((value + 0.5) * (1.0 / by))


def tent(coarse, fine):
    return jnp.maximum(4.0 - jnp.abs(fine - 4.0 * coarse), 0.0)


def inner(coarse, fine, first):
    below = 1.0 - first * jnp.maximum(1.0 - fine, 0.0)
    return (tent(coarse, fine + 1.0) + tent(coarse, fine - 1.0) * below) * 0.0625


def outer(coarse, fine):
    return tent(coarse, fine) * 0.0625


def kernel(cfg, *refs):
    ngx, ngy, ngz, rhs, fine, side, leaf, n1, n2, n3, ntop = cfg
    plane = ngy * ngz
    cells = side**3
    (rs_h, it_h, cf_h, od_h, li_h, lf_h, ls_h, lt_h, fi_h, fs_h, ft_h, si_h, st_h, ti_h) = refs[:14]
    out_h = refs[14]
    (
        rs, it, cf, od, li, lf, ls, lt, fi, fs, ft, si, st, ti,
        pack_it, pack_q, a21, bmat, e_h, e_l, fsx, fs_hi, fs_lo, stx, st_hi, st_lo,
        stu, ftu, back_hi, back_lo, st_high, ft_high,
        w1, w1_h, w1_l, w2, w2_h, w2_l, fi_low, si_low, rall, r_hi, r_lo,
        flat, got_flat, got_thin, send1, got1, send2, got2, up_send, up_got,
        part, got5, s6, got6, yall, down_send, down_got, gap2, gap1, low2, low1, corr, got_corr,
        local_sem, word1, word2, word3, send_sem, recv_sem,
    ) = refs[15:]

    a, b, c = (lax.axis_index(n) for n in AXES)
    me = b * ngz + c
    used = [0]
    pending = []
    stack = contextlib.ExitStack()

    def phase(name):
        stack.close()
        stack.enter_context(jax.named_scope(name))


    known = {}

    def step_along(name, here, by, n):
        by %= n
        if (name, by) not in known:
            known[name, by] = lax.rem(here + by, n) if by else here
        return known[name, by]

    def at(dx, dy, dz):
        return step_along("x", a, dx, ngx), step_along("y", b, dy, ngy), step_along("z", c, dz, ngz)

    def quarter(dz):
        if ("q", dz % ngz) not in known:
            known["q", dz % ngz] = lax.div(step_along("z", c, dz, ngz), 4)
        return known["q", dz % ngz]

    def far_first(d):
        return -sum(min(i % n, -i % n) * w for i, n, w in zip(d, (ngx, ngy, ngz), (2, 2, 1))), d

    def send(src, dst, device):
        i = used[0]
        used[0] += 1
        copy = pltpu.make_async_remote_copy(
            src_ref=src,
            dst_ref=dst,
            send_sem=send_sem.at[i],
            recv_sem=recv_sem.at[i],
            device_id=device,
            device_id_type=MESH,
        )
        copy.start()
        pending.append(copy)
        return copy

    def drain():
        for copy in pending:
            copy.wait_send()
        pending.clear()

    def arrive(copies):
        for copy in copies:
            copy.wait_recv()

    phase("p00_loads")
    first = [(cf_h, cf)]
    half = fine // 2
    for r in range(rhs):
        for h in (0, half):
            first += [(x.at[r, h : h + half], y.at[r, h : h + half]) for x, y in ((it_h, it), (rs_h, rs))]
    pairs = [
        (od_h, od), (li_h, li), (lf_h, lf), (ls_h, ls), (lt_h, lt),
        (fi_h, fi), (si_h, si), (fs_h, fs), (ft_h, ft), (st_h, st),
    ]
    pairs = first + [(s.at[:, 0, :] if len(s.shape) > len(d.shape) else s, d) for s, d in pairs] + [(ti_h, ti)]
    loads = [pltpu.make_async_copy(s, d, local_sem.at[i]) for i, (s, d) in enumerate(pairs)]
    for load in loads[:-1]:
        load.start()

    phase("p01_signal")
    partners = {(0, 0, dz) for dz in range(ngz)}
    for d in HALO + RIM:
        for s in (1, -1):
            partners.add((s * d[0] % ngx, s * d[1] % ngy, s * d[2] % ngz))
    partners.discard((0, 0, 0))
    barrier = pltpu.get_barrier_semaphore()
    for d in sorted(partners, key=far_first):
        pl.semaphore_signal(barrier, inc=1, device_id=at(*d), device_id_type=MESH)

    first_x = jnp.where(a == 0, 1.0, 0.0).astype(F32)
    first_y = jnp.where(b == 0, 1.0, 0.0).astype(F32)
    first_z = jnp.where(c == 0, 1.0, 0.0).astype(F32)

    phase("p02_weights")
    shape = (64, fine * fine)
    row, col = floats(shape, 0), floats(shape, 1)
    cx = whole_part(row, 8)
    cy = row - 8.0 * cx - 1.0
    cx = cx - 1.0
    fx = whole_part(col, fine)
    fy = col - fine * fx
    ox, oy = outer(cx, fx), outer(cy, fy)
    a21[0:64, :] = (inner(cx, fx, first_x) * oy + ox * inner(cy, fy, first_y)).astype(BF16)
    a21[64:128, :] = (ox * oy).astype(BF16)

    zshape = (8 * rhs, 2 * rhs * fine)
    row, col = floats(zshape, 0), floats(zshape, 1)
    cz = whole_part(row, rhs)
    cr = row - rhs * cz
    cz = cz - 1.0
    kind = whole_part(col, rhs * fine)
    rest = col - rhs * fine * kind
    fr = whole_part(rest, fine)
    fz = rest - fine * fr
    same = jnp.maximum(1.0 - jnp.abs(cr - fr), 0.0)
    wvz = ((1.0 - kind) * outer(cz, fz) + kind * inner(cz, fz, first_z)) * same
    wvz = wvz.astype(BF16)

    phase("p03_wait_residual")
    loads[0].wait()
    diagonal = 6.0 + cf[...]
    for r in range(rhs):
        for load in loads[4 * r + 1 : 4 * r + 5]:
            load.wait()
        now = it[r]
        at_r = slice(fine * r, fine * r + fine)
        pack_it[:, at_r] = now.reshape(fine * fine, fine)
        pack_q[:, at_r] = (rs[r] - diagonal * now).reshape(fine * fine, fine)
    i_h, i_l = split(pack_it[...])
    q_h, q_l = split(pack_q[...])
    own = a21[64:128, :]
    both = a21[...]
    from_it = dot(both, i_h) + dot(both, i_l)
    g1 = from_it[0:64] + dot(own, q_h) + dot(own, q_l)
    g_h, g_l = split(jnp.concatenate([g1, from_it[64:128]], axis=1))
    ct = dot(wvz, g_h, BACK) + dot(wvz, g_l, BACK)
    for j in range(4):
        lo = ct[2 * rhs * j : 2 * rhs * j + rhs]
        hi = ct[2 * rhs * j + rhs : 2 * rhs * j + 2 * rhs]
        flat[j] = jnp.concatenate([lo, hi], axis=1)

    phase("p05_barrier")
    pl.semaphore_wait(barrier, len(partners))

    halo_copies = []
    halo = sorted(enumerate(HALO), key=lambda e: far_first(e[1]))
    for i, (dx, dy, dz) in halo:
        if dz == 0:
            src, dst = flat, got_flat.at[i]
        else:
            src, dst = flat.at[3 if dz == 1 else 0], got_thin.at[i - len(FLAT)]
        halo_copies.append(send(src, dst, at(dx, dy, dz)))
    def tell(sem):
        for dx in (1, -1):
            pl.semaphore_signal(sem, inc=1, device_id=at(dx, 0, 0), device_id_type=MESH)

    tell(word1)
    loads[-1].start()
    for load in loads[1 + 4 * rhs : -1]:
        load.wait()
    fi_copy = send(fi, fi_low, at(0, 0, 1))
    si_copy = send(si, si_low, at(0, 1, 0))
    st_copy = send(st, st_high, at(-1, 0, 0))
    ft_copy = send(ft, ft_high, at(-1, 0, 0))

    phase("p07_factor")
    shape = (cells, 384)
    m, k = iota(shape, 0), iota(shape, 1)
    e1, e2 = leaf + n1, leaf + n1 + n2
    want = jnp.where(m < e1, m + (192 - leaf), jnp.where(m < e2, m + (128 - e1), m + (256 - e2)))
    bmat[...] = jnp.where((m >= leaf) & (k == want), 1.0, 0.0).astype(F32)
    li_v = li[...]
    li_pair = split(li_v)
    bmat[0:leaf, 0:leaf] = li_v
    bmat[0:leaf, 192 : 192 + 2 * n1] = -times(li_v, split(lf[...]), BACK)
    bmat[0:leaf, 128 : 128 + 2 * n2] = -times(li_v, split(ls[...]), BACK)
    bmat[0:leaf, 256 : 256 + 2 * n3] = -times(li_v, split(lt[...]), BACK)
    bh, bl = split(bmat[...])
    shape = (512, cells)
    k = iota(shape, 0)
    z, x, y = k >> 6, (k >> 3) & 7, k & 7
    inside = (z >= 1) & (z <= side) & (x >= 1) & (x <= side) & (y >= 1) & (y <= side)
    cell = jnp.where(inside, ((x - 1) * side + (y - 1)) * side + (z - 1), -1)
    chosen = jnp.where(cell == od[...], 1.0, 0.0).astype(BF16)
    e_h[...] = dot(chosen, bh).astype(BF16)
    e_l[...] = dot(chosen, bl).astype(BF16)

    phase("p08_place")
    fsx[...] = jnp.zeros(fsx.shape, F32)
    fsx[0:n1, 0 : 2 * n2] = -fs[...]
    fsx[0:n1, 128 : 128 + 2 * n3] = -ft[...]
    stx[...] = jnp.zeros(stx.shape, F32)
    stx[0:n2, 0 : 2 * n3] = -st[...]
    place1 = 32 * lax.rem(c, 4)
    place2 = n2 * lax.rem(me, 4)
    shift = (128, 32)
    put1 = jnp.where(iota(shift, 0) == iota(shift, 1) + place1, 1.0, 0.0).astype(BF16)
    put2 = jnp.where(iota(shift, 0) == iota(shift, 1) + place2, 1.0, 0.0).astype(BF16)
    hi, lo = split(fsx[...])
    fs_hi[...] = dot(put1, hi).astype(BF16)
    fs_lo[...] = dot(put1, lo).astype(BF16)
    hi, lo = split(stx[...])
    st_hi[0:128, :] = dot(put2, hi).astype(BF16)
    st_lo[0:128, :] = dot(put2, lo).astype(BF16)

    groups1 = (ngz + 3) // 4
    groups2 = (plane + 3) // 4

    phase("p09_w1")
    fi_copy.wait_recv()
    w1[...] = jnp.zeros(w1.shape, F32)
    mine = fi[:, 0, :]
    lower = jnp.where(c > 0, fi_low[:, 0, :], 0.0)
    for m in range(ngz):
        w1[64 : 64 + n1, 32 * m : 32 * m + n1] = mine[:, n1 * m : n1 * m + n1]
        w1[64 + n1 : 64 + 2 * n1, 32 * m : 32 * m + n1] = lower[:, n1 * m : n1 * m + n1]
    hi, lo = split(w1[...])
    w1_h[...] = hi
    w1_l[...] = lo
    e_mid = (e_h[:, 128:256], e_l[:, 128:256])
    lead = dot(e_mid[0], hi) + dot(e_mid[1], hi) + dot(e_mid[0], lo)
    lead_pair = split(lead)

    phase("p10_wait_halo")
    phase("p11_add_halo")
    lane = iota((rhs, 128), 1)
    at_z, at_x, at_y = lane >> 6, (lane >> 3) & 7, lane & 7

    def along(at_, d):
        if d == 0:
            return (at_ >= 1) & (at_ <= side)
        return at_ == (1 if d == 1 else side)

    def exists(i, d, n):
        return (i - d >= 0) & (i - d < n) if d else True

    total = [flat[j] for j in range(4)]
    for (i, (dx, dy, dz)), copy in reversed(list(zip(halo, halo_copies))):
        copy.wait_recv()
        turn = (-(side * 8) * dx - side * dy) % 128
        keep = along(at_x, dx) & along(at_y, dy)
        there = exists(a, dx, ngx) & exists(b, dy, ngy) & exists(c, dz, ngz)
        keep = keep & there
        if dz == 0:
            for j in range(4):
                v = got_flat[i, j]
                v = pltpu.roll(v, turn, 1) if turn else v
                total[j] += jnp.where(keep, v, 0.0)
        else:
            v = got_thin[i - len(FLAT)]
            v = pltpu.roll(v, turn, 1) if turn else v
            keep = keep & (at_z == (1 if dz == 1 else 0))
            j = 0 if dz == 1 else 3
            total[j] += jnp.where(keep, v, 0.0)

    phase("p12_leaf")
    gathered_cells = jnp.concatenate(total, axis=1)
    partial = times(gathered_cells, lead_pair)
    for g in range(groups1):
        send1[g] = partial[:, 128 * g : 128 * g + 128]
    steps = sorted(range(1, ngz), key=lambda k: -min(k, ngz - k))
    copies = []
    for k in steps:
        there = at(0, 0, k)
        copies.append(send(send1.at[quarter(k)], got1.at[k], there))
    own1 = send1[quarter(0)]
    word = pl.semaphore_wait
    word(word1, 2)
    tell(word2)
    e_pair = (e_h[...], e_l[...])
    s = times(gathered_cells, e_pair)
    s_leaf, s12, s3 = s[:, 0:128], s[:, 128:256], s[:, 256:384]
    w1_pair = (w1_h[...], w1_l[...])

    phase("p15_w2")
    si_copy.wait_recv()
    w2[...] = jnp.zeros(w2.shape, F32)
    mine = si[:, 0, :]
    lower = jnp.where(b > 0, si_low[:, 0, :], 0.0)
    for g in range(groups2):
        wide = min(4, plane - 4 * g) * n2
        cut = slice(4 * g * n2, 4 * g * n2 + wide)
        w2[0:n2, 128 * g : 128 * g + wide] = mine[:, cut]
        w2[n2 : 2 * n2, 128 * g : 128 * g + wide] = lower[:, cut]
    hi, lo = split(w2[...])
    w2_h[0:64, :] = hi
    w2_l[0:64, :] = lo
    back_rows = times(fsx[:, 0:64], (hi, lo))
    rall[c] = back_rows
    rows_h, rows_l = split(back_rows)
    r_hi[...] = dot(put1, rows_h).astype(BF16)
    r_lo[...] = dot(put1, rows_l).astype(BF16)
    partial = times(s12[:, 0:64], (hi, lo))

    phase("p16_wait_first")
    for k, copy in reversed(list(zip(steps, copies))):
        copy.wait_recv()
        own1 += got1[k]
    phase("p17_second_product")
    own1 = jnp.where((lane >= place1) & (lane < place1 + n1), own1, 0.0)
    partial = partial + times(own1, (r_hi[...], r_lo[...]))
    for g in range(groups2):
        send2[g] = partial[:, 128 * g : 128 * g + 128]
    offsets = [(dy, dz) for dy in range(ngy) for dz in range(ngz) if dy or dz]
    offsets = sorted(offsets, key=lambda d: far_first((0,) + d))
    copies, copies_up = [], []

    def group_of(dy, dz):
        if ngz % 4:
            return lax.div(step_along("y", b, dy, ngy) * ngz + step_along("z", c, dz, ngz), 4)
        return step_along("y", b, dy, ngy) * (ngz // 4) + quarter(dz)

    for dy, dz in offsets:
        there = at(-1, dy, dz)
        copies_up.append(send(send2.at[group_of(dy, dz)], got2.at[1, dy * ngz + dz], there))
    for dy, dz in offsets:
        there = at(0, dy, dz)
        copies.append(send(send2.at[group_of(dy, dz)], got2.at[0, dy * ngz + dz], there))
    copies_up.append(send(send2.at[me // 4], got2.at[1, 0], at(-1, 0, 0)))
    word(word2, 2)
    tell(word3)
    own2 = send2[me // 4]

    fs_top = (fs_hi[:, 128:256], fs_lo[:, 128:256])
    s3 = s3 + times(own1, fs_top)
    up_send[...] = s3
    up_copy = send(up_send, up_got, at(-1, 0, 0))

    phase("p18_wait_second")
    stu[...] = jnp.zeros(stu.shape, F32)
    ftu[...] = jnp.zeros(ftu.shape, F32)
    st_copy.wait_recv()
    ft_copy.wait_recv()
    stu[0:n2, 0:n3] = -st_high[:, n3 : 2 * n3]
    ftu[0:n1, 0:n3] = -ft_high[:, n3 : 2 * n3]
    for ref, put, row in ((stu, put2, 128), (ftu, put1, 384)):
        hi, lo = split(jnp.where(a < ngx - 1, ref[...], 0.0))
        back_hi[row : row + 128, :] = dot(put, hi).astype(BF16)
        back_lo[row : row + 128, :] = dot(put, lo).astype(BF16)
    column = iota((128, 128), 1)
    for got, src in ((back_hi, (st_hi[0:128, :], fs_top[0])), (back_lo, (st_lo[0:128, :], fs_top[1]))):
        for row, rows in zip((0, 256), src):
            got[row : row + 128, :] = jnp.where(column < n3, rows.astype(F32), 0.0).astype(BF16)
    st_hi[128:256, :] = back_hi[128:256, :]
    st_lo[128:256, :] = back_lo[128:256, :]
    chips = ngz // 2
    other = (a, b, c + 1 - 2 * lax.rem(c, 2))
    beside = [send(rall.at[c], rall.at[c], other)]
    if chips > 1:
        after, before = at(0, 0, 2), at(0, 0, -2)
        beside.append(send(rall.at[c], rall.at[c], after))
        beside.append(send(rall.at[c], rall.at[c], before))
    up_copy.wait_recv()
    copies_up[-1].wait_recv()
    above = got2[1, 0]
    target = s3 + jnp.where(a < ngx - 1, pltpu.roll(up_got[...], 128 - n3, 1), 0.0)
    for (dy, dz), copy, copy_up in reversed(list(zip(offsets, copies, copies_up))):
        copy.wait_recv()
        own2 += got2[0, dy * ngz + dz]
        copy_up.wait_recv()
        above += got2[1, dy * ngz + dz]
    phase("p21_target")
    mine = (lane >= place2) & (lane < place2 + n2)
    own2 = jnp.where(mine, own2, 0.0)
    above = jnp.where(mine, above, 0.0)
    target = target + times(jnp.concatenate([own2, above], axis=1), (st_hi[...], st_lo[...]))
    columns = jnp.transpose(jnp.concatenate([target, jnp.zeros((8 - rhs, 128), F32)], axis=0))
    spread = [jnp.broadcast_to(columns[0:n3, r : r + 1], (n3, 128)) for r in range(rhs)]

    phase("p22_top_product")
    width = ntop // ngz
    step = 128 if width % 128 == 0 else width
    loads[-1].wait()
    copies, slots = [], []
    for j in steps + [0]:
        group = at(0, 0, j)[2]
        for p in range(0, width, step):
            start = group * width + p
            if step == 128:
                start = pl.multiple_of(start, 128)
            block = ti[:, pl.ds(start, step)]
            for r in range(rhs):
                scale = spread[r] if step == 128 else jnp.broadcast_to(spread[r][:, 0:1], (n3, step))
                part[r, group, :, p : p + step] = jnp.sum(scale * block, axis=0, keepdims=True)
        for i in sorted(range(ngy), key=lambda i: -min(i, ngy - i)):
            if i or j:
                there = at(0, i, j)
                slots.append(i * ngz + j)
                copies.append(send(part.at[there[1], there[2]], got5.at[i * ngz + j], there))
    phase("p23_wait_top1")
    term = part[b, c]
    near = sorted(zip(slots, copies), key=lambda e: far_first((0, e[0] // ngz, e[0] % ngz)), reverse=True)
    for slot, copy in near:
        copy.wait_recv()
        term += got5[slot]
    word(word3, 2)
    phase("p24_top2")
    s6[...] = term
    along_x = sorted(range(1, ngx), key=lambda k: -min(k, ngx - k))
    copies = [send(s6, got6.at[k], at(k, 0, 0)) for k in along_x]
    arrive(beside)
    if chips > 1:
        across = [
            send(rall.at[before[2], 0:16], rall.at[before[2], 0:16], after),
            send(rall.at[after[2], 16:32], rall.at[after[2], 16:32], before),
        ]
        beside = [send(rall.at[d[2]], rall.at[d[2]], other) for d in (after, before)]
    for k, copy in reversed(list(zip(along_x, copies))):
        copy.wait_recv()
        term += got6[k]
    phase("p25_top3")
    yall[b, c] = term
    copies = [send(yall.at[b, c], yall.at[b, c], at(0, dy, dz)) for dy, dz in offsets]
    if chips > 1:
        far = lax.rem(c + 4, ngz)
        arrive(across)
        beside.append(send(rall.at[far], rall.at[far], other))

    phase("p26_top_back")
    arrivals = dict(zip(offsets, copies))
    total = [jnp.zeros((n3, step), F32) for _ in range(rhs)]
    for dz in [0] + list(reversed(steps)):
        group = step_along("z", c, -dz, ngz)
        for dy in sorted(range(ngy), key=lambda i: min(i, ngy - i)):
            if dy or dz:
                arrivals[dy, dz].wait_recv()
        for p in range(0, width, step):
            start = group * width + p
            if step == 128:
                start = pl.multiple_of(start, 128)
            block = ti[:, pl.ds(start, step)]
            for r in range(rhs):
                total[r] += block * yall[r, group, :, p : p + step]
    ones = jnp.ones((8, step), BF16)
    back = jnp.zeros((rhs, n3), F32)
    which = iota((rhs, n3), 0)
    for r in range(rhs):
        hi, lo = split(total[r])
        both_sums = dot(ones, hi, BACK) + dot(ones, lo, BACK)
        back += jnp.where(which == r, both_sums[0:rhs], 0.0)
    phase("p27_down")
    down_send[...] = jnp.zeros((rhs, 128), F32)
    down_send[:, 0:n3] = back
    right_sides = times(down_send[...], (back_hi[...], back_lo[...]), BACK)
    gap2[0, me] = own2 + right_sides[:, 0:128]
    low2[...] = right_sides[:, 128:256]
    gap1[0, c] = own1 + right_sides[:, 256:384]
    low1[...] = right_sides[:, 384:512]
    copies = [send(low2, gap2.at[1, me], at(1, dy, dz)) for dy, dz in offsets]
    copies += [send(gap2.at[0, me], gap2.at[0, me], at(0, dy, dz)) for dy, dz in offsets]
    copies.append(send(low2, gap2.at[1, me], at(1, 0, 0)))
    line = [send(low1, gap1.at[1, c], at(1, 0, k)) for k in steps + [0]]
    line += [send(gap1.at[0, c], gap1.at[0, c], at(0, 0, k)) for k in steps]
    down_copy = send(down_send, down_got, at(1, 0, 0))

    phase("p29_rows")
    arrive(beside[1:] if chips == 1 else beside)
    hi, lo = split(rall[...].reshape(32 * ngz, 128 * groups2))
    rows = dot(w1_h[64:128, 0 : 32 * ngz], hi) + dot(w1_l[64:128, 0 : 32 * ngz], hi) + dot(w1_h[64:128, 0 : 32 * ngz], lo)
    hi, lo = split(rows)
    w2_h[64:128, :] = hi
    w2_l[64:128, :] = lo

    def gathered(ref, members):
        blocks = []
        for g in range((members + 3) // 4):
            own_part, lower_part = ref[0, 4 * g], ref[1, 4 * g]
            for i in range(4 * g + 1, min(4 * g + 4, members)):
                own_part += ref[0, i]
                lower_part += ref[1, i]
            blocks.append(own_part + jnp.where(a > 0, lower_part, 0.0))
        return jnp.concatenate(blocks, axis=1)

    drain()
    phase("p30_wait_gap")
    arrive([down_copy])
    z3 = down_send[...] + jnp.where(a > 0, pltpu.roll(down_got[...], n3, 1), 0.0)
    corr_part = times(jnp.concatenate([s_leaf, z3], axis=1), tuple(jnp.concatenate([e[:, 0:128], e[:, 256:384]], axis=1) for e in e_pair), BACK)
    arrive(line)
    z12 = times(gathered(gap1, ngz), w1_pair, BACK)
    arrive(copies)
    phase("p31_z_leaf")
    z12 = z12 + times(gathered(gap2, plane), (w2_h[...], w2_l[...]), BACK)

    result = corr_part + times(z12, (e_h[:, 128:256], e_l[:, 128:256]), BACK)
    for j in range(4):
        corr[j] = result[:, 128 * j : 128 * j + 128]
    phase("p32_rim")
    copies = []
    rim = sorted(enumerate(RIM), key=lambda e: far_first(e[1]))
    for i, (dx, dy, dz) in rim:
        there = at(-dx, -dy, -dz)
        if dz == 0:
            copies.append(send(corr, got_corr.at[i], there))
        else:
            copies.append(send(corr.at[0], got_corr.at[i, 0], there))

    total = [corr[j] for j in range(4)]
    for (i, (dx, dy, dz)), copy in reversed(list(zip(rim, copies))):
        copy.wait_recv()
        turn = side * 8 * dx + side * dy
        keep = (at_x == side + 1) if dx else (at_x <= side)
        keep = keep & ((at_y == side + 1) if dy else (at_y <= side))
        if dx:
            keep = keep & (a < ngx - 1)
        if dy:
            keep = keep & (b < ngy - 1)
        if dz:
            keep = keep & (c < ngz - 1) & (at_z == 1)
        for j in range(4) if dz == 0 else (0,):
            v = got_corr[i, j]
            v = pltpu.roll(v, turn, 1) if turn else v
            total[j if dz == 0 else 3] += jnp.where(keep, v, 0.0)
    rows = []
    for j in range(4):
        rows += [total[j][:, 0:64], total[j][:, 64:128]]
    out_h[...] = jnp.concatenate(rows, axis=0)
    phase("p34_finish")
    drain()
    stack.close()


def prolong(cfg, ct_h, out_h, ct, out_v, in_sem, out_sem):
    rhs, fine = cfg[3], cfg[4]
    load = pltpu.make_async_copy(ct_h, ct, in_sem)
    load.start()
    stack = contextlib.ExitStack()
    stack.enter_context(jax.named_scope("q0"))
    shape = (fine, 128)
    fx, col = floats(shape, 0), floats(shape, 1)
    rest = col - 64.0 * whole_part(col, 64)
    cx = whole_part(rest, 8)
    along_x = tent(cx - 1.0, fx) * 0.25
    along_y = tent(rest - 8.0 * cx - 1.0, fx) * 0.25
    spread_xy = (along_x[:, None, :] * along_y[None, :, :]).reshape(fine * fine, 128).astype(BF16)
    shape = (rhs * fine, 8 * rhs)
    row, col = floats(shape, 0), floats(shape, 1)
    fr = whole_part(row, fine)
    fz = row - fine * fr
    cz = whole_part(col, rhs)
    cr = col - rhs * cz
    same = jnp.maximum(1.0 - jnp.abs(cr - fr), 0.0)
    spread_z = (tent(cz - 1.0, fz) * same * 0.25).astype(BF16)

    stack.close()
    stack.enter_context(jax.named_scope("q1"))
    load.wait()
    stack.close()
    stack.enter_context(jax.named_scope("q2"))
    ct_h, ct_l = split(ct[...])
    ht = dot(spread_z, ct_h) + dot(spread_z, ct_l)
    ht_h = ht.astype(BF16).astype(F32)
    ht = jnp.concatenate([ht_h, ht - ht_h], axis=1)
    stack.close()
    stack.enter_context(jax.named_scope("q3"))
    stores = []
    for r in range(rhs):
        part_r = ht[r * fine : (r + 1) * fine].astype(BF16)
        out_v[r] = dot(spread_xy, part_r, BACK).reshape(fine, fine, fine)
        store = pltpu.make_async_copy(out_v.at[r], out_h.at[r], out_sem.at[r])
        store.start()
        stores.append(store)
    stack.close()
    stack.enter_context(jax.named_scope("q4"))
    for store in stores:
        store.wait()
    stack.close()


def per_device(mesh_sizes, *args):
    (rs, it, cf, od, li, lf, ls, lt, fi, fs, ft, si, st, ti) = args
    ngx, ngy, ngz = mesh_sizes
    od = od.reshape(1, -1)
    rhs, fine = rs.shape[0], rs.shape[1]
    side = fine // 4
    leaf, n1, n2, n3, ntop = li.shape[3], fs.shape[3], st.shape[3], ti.shape[0], ti.shape[1]
    li, fs, ft, st = (jnp.transpose(v, (0, 1, 3, 2, 4))[0, 0] for v in (li, fs, ft, st))
    fi, si = jnp.transpose(fi, (0, 2, 1, 3))[0], jnp.transpose(si, (1, 0, 2))
    lf, ls = (jnp.transpose(v, (0, 1, 4, 2, 3))[0, 0] for v in (lf, ls))
    lt = jnp.transpose(lt, (0, 1, 2, 4, 3))[0, 0, 0]
    cfg = (ngx, ngy, ngz, rhs, fine, side, leaf, n1, n2, n3, ntop)
    plane = ngy * ngz
    groups1, groups2 = (ngz + 3) // 4, (plane + 3) // 4
    cells = side**3
    inputs = [rs, it, cf, od, li, lf, ls, lt, fi, fs, ft, si, st, ti]
    v = pltpu.VMEM
    width = ntop // ngz
    step = 128 if width % 128 == 0 else width
    copies = len(HALO) + 4 + 8 + 3 * ngz - 2 + 6 * plane - 4 + 2 + (ngx - 1) + len(RIM)
    narrow = [x.reshape(x.shape[0], -1) if any(x is y for y in (li, lf, ls, fs, ft, st)) else x for x in inputs]
    scratch = [v(x.shape, x.dtype) for x in narrow]
    scratch += [
        v((fine * fine, rhs * fine), F32), v((fine * fine, rhs * fine), F32), v((128, fine * fine), BF16),
        v((cells, 384), F32), v((512, 384), BF16), v((512, 384), BF16),
        v((32, 256), F32), v((128, 256), BF16), v((128, 256), BF16),
        v((32, 128), F32), v((256, 128), BF16), v((256, 128), BF16),
        v((32, 128), F32), v((32, 128), F32), v((512, 128), BF16), v((512, 128), BF16), v(st.shape[::2], F32), v(ft.shape[::2], F32),
        v((128, 128 * groups1), F32), v((128, 128 * groups1), BF16), v((128, 128 * groups1), BF16),
        v((64, 128 * groups2), F32), v((128, 128 * groups2), BF16), v((128, 128 * groups2), BF16),
        v(fi.shape, F32), v(si.shape, F32), v((ngz, 32, 128 * groups2), F32),
        v((128, 128 * groups2), BF16), v((128, 128 * groups2), BF16),
        v((4, rhs, 128), F32), v((len(FLAT), 4, rhs, 128), F32), v((len(HALO) - len(FLAT), rhs, 128), F32),
        v((groups1, rhs, 128), F32), v((ngz, rhs, 128), F32),
        v((groups2, rhs, 128), F32), v((2, plane, rhs, 128), F32),
        v((rhs, 128), F32), v((rhs, 128), F32),
        v((rhs, ngz, 1, width), F32), v((plane, 1, width), F32),
        v((1, width), F32), v((ngx, 1, width), F32),
        v((rhs, ngz, 1, width), F32),
        v((rhs, 128), F32), v((rhs, 128), F32),
        v((2, plane, rhs, 128), F32), v((2, ngz, rhs, 128), F32), v((rhs, 128), F32), v((rhs, 128), F32),
        v((4, rhs, 128), F32), v((len(RIM), 4, rhs, 128), F32),
        pltpu.SemaphoreType.DMA((len(inputs) + 4 * rhs - 2,)),
        *[pltpu.SemaphoreType.REGULAR] * 3,
        pltpu.SemaphoreType.DMA((copies,)), pltpu.SemaphoreType.DMA((copies,)),
    ]
    coarse = pl.pallas_call(
        functools.partial(kernel, cfg),
        out_shape=jax.ShapeDtypeStruct((8 * rhs, 64), F32),
        in_specs=[pl.BlockSpec(memory_space=pl.ANY)] * len(inputs),
        out_specs=pl.BlockSpec(memory_space=pltpu.VMEM),
        scratch_shapes=scratch,
        compiler_params=pltpu.CompilerParams(
            collective_id=0, has_side_effects=True, vmem_limit_bytes=67043328
        ),
        name="coarse_correction",
    )(*inputs)
    return pl.pallas_call(
        functools.partial(prolong, cfg),
        out_shape=jax.ShapeDtypeStruct(rs.shape, F32),
        in_specs=[pl.BlockSpec(memory_space=pl.ANY)],
        out_specs=pl.BlockSpec(memory_space=pl.ANY),
        scratch_shapes=[v((8 * rhs, 64), F32), v(rs.shape, F32), pltpu.SemaphoreType.DMA, pltpu.SemaphoreType.DMA((rhs,))],
        compiler_params=pltpu.CompilerParams(vmem_limit_bytes=67043328),
        name="prolong",
    )(coarse)


def solution(mesh):
    sizes = tuple(mesh.shape[n] for n in AXES)
    cells = P("gx", "gy", "gz")
    lines = P("gx", "gy", "gz", None)
    blocks = P("gx", "gy", "gz", None, None)
    field = P(None, "gx", "gy", "gz")
    return jax.shard_map(
        functools.partial(per_device, sizes),
        mesh=mesh,
        in_specs=(
            field, field, cells, lines, blocks, blocks, blocks, blocks, lines, blocks, blocks,
            P("gx", ("gy", "gz"), None), blocks, P(("gx", "gy", "gz"), None),
        ),
        out_specs=field,
        check_vma=False,
    )
```

```python
import contextlib
import functools

import jax
import jax.numpy as jnp
from jax import lax
from jax.experimental import pallas as pl
from jax.experimental.pallas import tpu as pltpu
from jax.sharding import PartitionSpec as P

MESH = pl.DeviceIdType.MESH
F32 = jnp.float32
BF16 = jnp.bfloat16
AXES = ("gx", "gy", "gz")

FLAT = ((1, 0), (-1, 0), (0, 1), (0, -1), (1, 1), (1, -1), (-1, 1))
ABOVE = ((0, 0),) + FLAT
BELOW = ((0, 0), (1, 0), (0, 1), (1, 1))
HALO = [(x, y, 0) for x, y in FLAT] + [(x, y, 1) for x, y in ABOVE] + [(x, y, -1) for x, y in BELOW]
RIM = [(1, 0, 0), (0, 1, 0), (1, 1, 0), (0, 0, 1), (1, 0, 1), (0, 1, 1), (1, 1, 1)]

(
    HALO_G, FI_G, SI_G, ST_G, FT_G, FIRST_G, SECOND_G, UP_G, ROWS_G, ACROSS_G, CORE_G,
    TERM_G, LINE_G, GAP_G, FIRST_GAP_G, DOWN_G, RIM_G, SPREAD_G,
) = range(18)


def split(value):
    high = value.astype(BF16)
    return high, (value - high.astype(F32)).astype(BF16)


def dot(left, right, dims=((1,), (0,))):
    return lax.dot_general(left, right, (dims, ((), ())), preferred_element_type=F32)


def times(value, factor, dims=((1,), (0,))):
    f_high, f_low = factor
    n = value.shape[0]
    if n > 4:
        high, low = split(value)
        return dot(high, f_high, dims) + dot(low, f_high, dims) + dot(high, f_low, dims)
    high = value.astype(BF16).astype(F32)
    both = jnp.concatenate([high, value - high], axis=0).astype(BF16)
    out = dot(both, f_high, dims) + dot(both, f_low, dims)
    return out[0:n] + out[n : 2 * n]


BACK = ((1,), (1,))


def iota(shape, dim):
    return lax.broadcasted_iota(jnp.int32, shape, dim)


def floats(shape, dim):
    return iota(shape, dim).astype(F32)


def whole_part(value, by):
    return jnp.floor((value + 0.5) * (1.0 / by))


def tent(coarse, fine):
    return jnp.maximum(4.0 - jnp.abs(fine - 4.0 * coarse), 0.0)


def inner(coarse, fine, first):
    below = 1.0 - first * jnp.maximum(1.0 - fine, 0.0)
    return (tent(coarse, fine + 1.0) + tent(coarse, fine - 1.0) * below) * 0.0625


def outer(coarse, fine):
    return tent(coarse, fine) * 0.0625


def kernel(cfg, *refs):
    ngx, ngy, ngz, rhs, fine, side, leaf, n1, n2, n3, ntop = cfg
    plane = ngy * ngz
    cells = side**3
    (rs_h, it_h, cf_h, od_h, li_h, lf_h, ls_h, lt_h, fi_h, fs_h, ft_h, si_h, st_h, ti_h) = refs[:14]
    out_h = refs[14]
    (
        rs, it, cf, od, li, lf, ls, lt, fi, fs, ft, si, st, ti,
        pack_it, pack_q, a21, bmat, e_h, e_l, fsx, fs_hi, fs_lo, stx, st_hi, st_lo,
        stu, ftu, back_hi, back_lo, st_high, ft_high,
        w1, w1_h, w1_l, w2, w2_h, w2_l, fi_low, si_low, rall, r_hi, r_lo,
        flat, got_halo, send1, got1, send2, got2, up_send, up_got,
        part, got5, s6, got6, yall, down_send, down_got, gap2, gap1, low2, low1, corr, got_corr,
        local_sem, word1, word2, word3, go, send_sem, recv_sem,
    ) = refs[15:]

    a, b, c = (lax.axis_index(n) for n in AXES)
    me = b * ngz + c
    stack = contextlib.ExitStack()

    def phase(name):
        stack.close()
        stack.enter_context(jax.named_scope(name))


    known = {}

    def step_along(name, here, by, n):
        by %= n
        if (name, by) not in known:
            known[name, by] = lax.rem(here + by, n) if by else here
        return known[name, by]

    def at(dx, dy, dz):
        return step_along("x", a, dx, ngx), step_along("y", b, dy, ngy), step_along("z", c, dz, ngz)

    def quarter(dz):
        if ("q", dz % ngz) not in known:
            known["q", dz % ngz] = lax.div(step_along("z", c, dz, ngz), 4)
        return known["q", dz % ngz]

    for n, here, size in (("x", a, ngx), ("y", b, ngy), ("z", c, ngz)):
        for by in range(size):
            step_along(n, here, by, size)
    for dz in range(ngz):
        quarter(dz)
    chips = ngz // 2
    chip, core = lax.div(c, 2), lax.rem(c, 2)
    chip_at = [lax.rem(chip + j, chips) if j else chip for j in range(chips)]
    keeper = core == 1
    other = (a, b, c + 1 - 2 * core)

    def far_first(d):
        return -sum(min(i % n, -i % n) * w for i, n, w in zip(d, (ngx, ngy, ngz), (2, 2, 1))), d

    def copy_of(src, dst, device, group, into=None):
        return pltpu.make_async_remote_copy(
            src_ref=src,
            dst_ref=dst,
            send_sem=send_sem.at[group],
            recv_sem=recv_sem.at[group if into is None else into],
            device_id=device,
            device_id_type=MESH,
        )

    def send(src, dst, device, group, into=None):
        copy_of(src, dst, device, group, into).start()

    def arrived(group, ref):
        copy_of(ref, ref, other, group).wait_recv()

    def sent(group, ref):
        copy_of(ref, ref, other, group).wait_send()

    phase("p00_loads")
    first = [(cf_h, cf)]
    for r in range(rhs):
        first += [(it_h.at[r], it.at[r]), (rs_h.at[r], rs.at[r])]
    pairs = [
        (od_h, od), (li_h, li), (lf_h, lf), (ls_h, ls), (lt_h, lt),
        (fi_h, fi), (si_h, si), (fs_h, fs), (ft_h, ft), (st_h, st),
    ]
    pairs = first + [(s.at[:, 0, :] if len(s.shape) > len(d.shape) else s, d) for s, d in pairs] + [(ti_h, ti)]
    spots = [0] + [1 + i // 2 for i in range(2 * rhs)] + list(range(1 + rhs, len(pairs) - rhs))
    loads = [pltpu.make_async_copy(s, d, local_sem.at[i]) for i, (s, d) in zip(spots, pairs)]
    for load in loads[:-1]:
        load.start()

    phase("p01_signal")
    partners = {(0, 0, dz) for dz in range(ngz)}
    for d in HALO + RIM:
        for s in (1, -1):
            partners.add((s * d[0] % ngx, s * d[1] % ngy, s * d[2] % ngz))
    partners.discard((0, 0, 0))
    barrier = pltpu.get_barrier_semaphore()
    for d in sorted(partners, key=far_first):
        pl.semaphore_signal(barrier, inc=1, device_id=at(*d), device_id_type=MESH)

    first_x = jnp.where(a == 0, 1.0, 0.0).astype(F32)
    first_y = jnp.where(b == 0, 1.0, 0.0).astype(F32)
    first_z = jnp.where(c == 0, 1.0, 0.0).astype(F32)

    phase("p02_weights")
    shape = (64, fine * fine)
    row, col = floats(shape, 0), floats(shape, 1)
    cx = whole_part(row, 8)
    cy = row - 8.0 * cx - 1.0
    cx = cx - 1.0
    fx = whole_part(col, fine)
    fy = col - fine * fx
    ox, oy = outer(cx, fx), outer(cy, fy)
    a21[0:64, :] = (inner(cx, fx, first_x) * oy + ox * inner(cy, fy, first_y)).astype(BF16)
    a21[64:128, :] = (ox * oy).astype(BF16)

    zshape = (8 * rhs, 2 * rhs * fine)
    row, col = floats(zshape, 0), floats(zshape, 1)
    cz = whole_part(row, rhs)
    cr = row - rhs * cz
    cz = cz - 1.0
    kind = whole_part(col, rhs * fine)
    rest = col - rhs * fine * kind
    fr = whole_part(rest, fine)
    fz = rest - fine * fr
    same = jnp.maximum(1.0 - jnp.abs(cr - fr), 0.0)
    wvz = ((1.0 - kind) * outer(cz, fz) + kind * inner(cz, fz, first_z)) * same
    wvz = wvz.astype(BF16)

    phase("p03_wait_residual")
    loads[0].wait()
    diagonal = 6.0 + cf[...]
    for r in range(rhs):
        pltpu.make_async_copy(it_h.at[0:2], it.at[0:2], local_sem.at[1 + r]).wait()
        now = it[r]
        at_r = slice(fine * r, fine * r + fine)
        pack_it[:, at_r] = now.reshape(fine * fine, fine)
        pack_q[:, at_r] = (rs[r] - diagonal * now).reshape(fine * fine, fine)
    i_h, i_l = split(pack_it[...])
    q_h, q_l = split(pack_q[...])
    own = a21[64:128, :]
    both = a21[...]
    from_it = dot(both, i_h) + dot(both, i_l)
    g1 = from_it[0:64] + dot(own, q_h) + dot(own, q_l)
    g_h, g_l = split(jnp.concatenate([g1, from_it[64:128]], axis=1))
    ct = dot(wvz, g_h, BACK) + dot(wvz, g_l, BACK)
    for j in range(4):
        lo = ct[2 * rhs * j : 2 * rhs * j + rhs]
        hi = ct[2 * rhs * j + rhs : 2 * rhs * j + 2 * rhs]
        flat[j] = jnp.concatenate([lo, hi], axis=1)

    phase("p05_barrier")
    pl.semaphore_wait(barrier, len(partners))

    halo = sorted(enumerate(HALO), key=lambda e: far_first(e[1]))
    thin = 4 * len(FLAT)
    for i, (dx, dy, dz) in halo:
        if dz == 0:
            send(flat, got_halo.at[4 * i : 4 * i + 4], at(dx, dy, dz), HALO_G)
        else:
            src = flat.at[3 if dz == 1 else 0]
            send(src, got_halo.at[thin + i - len(FLAT)], at(dx, dy, dz), HALO_G)

    def tell(sem):
        for dx in (1, -1):
            pl.semaphore_signal(sem, inc=1, device_id=at(dx, 0, 0), device_id_type=MESH)

    tell(word1)
    loads[-1].start()
    for load in loads[1 + 2 * rhs : -1]:
        load.wait()
    send(fi, fi_low, at(0, 0, 1), FI_G)
    send(si, si_low, at(0, 1, 0), SI_G)
    send(st, st_high, at(-1, 0, 0), ST_G)
    send(ft, ft_high, at(-1, 0, 0), FT_G)

    phase("p07_factor")
    shape = (cells, 384)
    m, k = iota(shape, 0), iota(shape, 1)
    e1, e2 = leaf + n1, leaf + n1 + n2
    want = jnp.where(m < e1, m + (192 - leaf), jnp.where(m < e2, m + (128 - e1), m + (256 - e2)))
    bmat[...] = jnp.where((m >= leaf) & (k == want), 1.0, 0.0).astype(F32)
    li_v = li[...]
    li_pair = split(li_v)
    bmat[0:leaf, 0:leaf] = li_v
    bmat[0:leaf, 192 : 192 + 2 * n1] = -times(li_v, split(lf[...]), BACK)
    bmat[0:leaf, 128 : 128 + 2 * n2] = -times(li_v, split(ls[...]), BACK)
    bmat[0:leaf, 256 : 256 + 2 * n3] = -times(li_v, split(lt[...]), BACK)
    bh, bl = split(bmat[...])
    shape = (512, cells)
    k = iota(shape, 0)
    z, x, y = k >> 6, (k >> 3) & 7, k & 7
    inside = (z >= 1) & (z <= side) & (x >= 1) & (x <= side) & (y >= 1) & (y <= side)
    cell = jnp.where(inside, ((x - 1) * side + (y - 1)) * side + (z - 1), -1)
    chosen = jnp.where(cell == od[...], 1.0, 0.0).astype(BF16)
    e_h[...] = dot(chosen, bh).astype(BF16)
    e_l[...] = dot(chosen, bl).astype(BF16)

    phase("p08_place")
    fsx[...] = jnp.zeros(fsx.shape, F32)
    fsx[0:n1, 0 : 2 * n2] = -fs[...]
    fsx[0:n1, 128 : 128 + 2 * n3] = -ft[...]
    stx[...] = jnp.zeros(stx.shape, F32)
    stx[0:n2, 0 : 2 * n3] = -st[...]
    place1 = 32 * lax.rem(c, 4)
    place2 = n2 * lax.rem(me, 4)
    shift = (128, 32)
    put1 = jnp.where(iota(shift, 0) == iota(shift, 1) + place1, 1.0, 0.0).astype(BF16)
    put2 = jnp.where(iota(shift, 0) == iota(shift, 1) + place2, 1.0, 0.0).astype(BF16)
    hi, lo = split(fsx[...])
    fs_hi[...] = dot(put1, hi).astype(BF16)
    fs_lo[...] = dot(put1, lo).astype(BF16)
    hi, lo = split(stx[...])
    st_hi[0:128, :] = dot(put2, hi).astype(BF16)
    st_lo[0:128, :] = dot(put2, lo).astype(BF16)

    groups1 = (ngz + 3) // 4
    groups2 = (plane + 3) // 4

    phase("p09_w1")
    arrived(FI_G, fi_low)
    w1[...] = jnp.zeros(w1.shape, F32)
    mine = fi[:, 0, :]
    lower = jnp.where(c > 0, fi_low[:, 0, :], 0.0)
    for m in range(ngz):
        w1[64 : 64 + n1, 32 * m : 32 * m + n1] = mine[:, n1 * m : n1 * m + n1]
        w1[64 + n1 : 64 + 2 * n1, 32 * m : 32 * m + n1] = lower[:, n1 * m : n1 * m + n1]
    hi, lo = split(w1[...])
    w1_h[...] = hi
    w1_l[...] = lo
    e_mid = (e_h[:, 128:256], e_l[:, 128:256])
    lead = dot(e_mid[0], hi) + dot(e_mid[1], hi) + dot(e_mid[0], lo)
    lead_pair = split(lead)

    phase("p10_wait_halo")
    phase("p11_add_halo")
    lane = iota((rhs, 128), 1)
    at_z, at_x, at_y = lane >> 6, (lane >> 3) & 7, lane & 7

    def along(at_, d):
        if d == 0:
            return (at_ >= 1) & (at_ <= side)
        return at_ == (1 if d == 1 else side)

    def exists(i, d, n):
        return (i - d >= 0) & (i - d < n) if d else True

    total = [flat[j] for j in range(4)]
    arrived(HALO_G, got_halo)
    for i, (dx, dy, dz) in halo:
        turn = (-(side * 8) * dx - side * dy) % 128
        keep = along(at_x, dx) & along(at_y, dy)
        there = exists(a, dx, ngx) & exists(b, dy, ngy) & exists(c, dz, ngz)
        keep = keep & there
        if dz == 0:
            for j in range(4):
                v = got_halo[4 * i + j]
                v = pltpu.roll(v, turn, 1) if turn else v
                total[j] += jnp.where(keep, v, 0.0)
        else:
            v = got_halo[thin + i - len(FLAT)]
            v = pltpu.roll(v, turn, 1) if turn else v
            keep = keep & (at_z == (1 if dz == 1 else 0))
            j = 0 if dz == 1 else 3
            total[j] += jnp.where(keep, v, 0.0)

    phase("p12_leaf")
    gathered_cells = jnp.concatenate(total, axis=1)
    partial = times(gathered_cells, lead_pair)
    for g in range(groups1):
        send1[g] = partial[:, 128 * g : 128 * g + 128]
    steps = sorted(range(1, ngz), key=lambda k: -min(k, ngz - k))
    for k in steps:
        send(send1.at[quarter(k)], got1.at[k], at(0, 0, k), FIRST_G)
    own1 = send1[quarter(0)]
    word = pl.semaphore_wait
    word(word1, 2)
    tell(word2)
    e_pair = (e_h[...], e_l[...])
    s = times(gathered_cells, e_pair)
    s_leaf, s12, s3 = s[:, 0:128], s[:, 128:256], s[:, 256:384]
    w1_pair = (w1_h[...], w1_l[...])

    phase("p15_w2")
    arrived(SI_G, si_low)
    w2[...] = jnp.zeros(w2.shape, F32)
    mine = si[:, 0, :]
    lower = jnp.where(b > 0, si_low[:, 0, :], 0.0)
    for g in range(groups2):
        wide = min(4, plane - 4 * g) * n2
        cut = slice(4 * g * n2, 4 * g * n2 + wide)
        w2[0:n2, 128 * g : 128 * g + wide] = mine[:, cut]
        w2[n2 : 2 * n2, 128 * g : 128 * g + wide] = lower[:, cut]
    hi, lo = split(w2[...])
    w2_h[0:64, :] = hi
    w2_l[0:64, :] = lo
    back_rows = times(fsx[:, 0:64], (hi, lo))
    rall[c] = back_rows
    rows_h, rows_l = split(back_rows)
    r_hi[...] = dot(put1, rows_h).astype(BF16)
    r_lo[...] = dot(put1, rows_l).astype(BF16)
    partial = times(s12[:, 0:64], (hi, lo))

    phase("p16_wait_first")
    arrived(FIRST_G, got1.at[1:ngz])
    for k in steps:
        own1 += got1[k]
    phase("p17_second_product")
    own1 = jnp.where((lane >= place1) & (lane < place1 + n1), own1, 0.0)
    partial = partial + times(own1, (r_hi[...], r_lo[...]))
    for g in range(groups2):
        send2[g] = partial[:, 128 * g : 128 * g + 128]
    offsets = [(dy, dz) for dy in range(ngy) for dz in range(ngz) if dy or dz]
    offsets = sorted(offsets, key=lambda d: far_first((0,) + d))

    def group_of(dy, dz):
        if ngz % 4:
            return lax.div(step_along("y", b, dy, ngy) * ngz + step_along("z", c, dz, ngz), 4)
        return step_along("y", b, dy, ngy) * (ngz // 4) + quarter(dz)

    for dy, dz in offsets:
        there = at(-1, dy, dz)
        send(send2.at[group_of(dy, dz)], got2.at[plane + dy * ngz + dz], there, SECOND_G)
    for dy, dz in offsets:
        there = at(0, dy, dz)
        send(send2.at[group_of(dy, dz)], got2.at[dy * ngz + dz], there, SECOND_G)
    send(send2.at[me // 4], got2.at[plane], at(-1, 0, 0), SECOND_G)
    word(word2, 2)
    tell(word3)
    own2 = send2[me // 4]

    fs_top = (fs_hi[:, 128:256], fs_lo[:, 128:256])
    s3 = s3 + times(own1, fs_top)
    up_send[...] = s3
    send(up_send, up_got, at(-1, 0, 0), UP_G)

    phase("p18_wait_second")
    stu[...] = jnp.zeros(stu.shape, F32)
    ftu[...] = jnp.zeros(ftu.shape, F32)
    arrived(ST_G, st_high)
    arrived(FT_G, ft_high)
    stu[0:n2, 0:n3] = -st_high[:, n3 : 2 * n3]
    ftu[0:n1, 0:n3] = -ft_high[:, n3 : 2 * n3]
    for ref, put, row in ((stu, put2, 128), (ftu, put1, 384)):
        hi, lo = split(jnp.where(a < ngx - 1, ref[...], 0.0))
        back_hi[row : row + 128, :] = dot(put, hi).astype(BF16)
        back_lo[row : row + 128, :] = dot(put, lo).astype(BF16)
    column = iota((128, 128), 1)
    for got, src in ((back_hi, (st_hi[0:128, :], fs_top[0])), (back_lo, (st_lo[0:128, :], fs_top[1]))):
        for row, rows in zip((0, 256), src):
            got[row : row + 128, :] = jnp.where(column < n3, rows.astype(F32), 0.0).astype(BF16)
    st_hi[128:256, :] = back_hi[128:256, :]
    st_lo[128:256, :] = back_lo[128:256, :]
    send(rall.at[c], rall.at[c], other, ROWS_G)
    if chips > 1:
        after, before = at(0, 0, 2), at(0, 0, -2)
        send(rall.at[c], rall.at[c], after, ROWS_G)
        send(rall.at[c], rall.at[c], before, ROWS_G)
    arrived(UP_G, up_got)
    target = s3 + jnp.where(a < ngx - 1, pltpu.roll(up_got[...], 128 - n3, 1), 0.0)
    arrived(SECOND_G, got2.at[1 : 2 * plane])
    above = got2[plane]
    for dy, dz in offsets:
        own2 += got2[dy * ngz + dz]
        above += got2[plane + dy * ngz + dz]
    phase("p21_target")
    mine = (lane >= place2) & (lane < place2 + n2)
    own2 = jnp.where(mine, own2, 0.0)
    above = jnp.where(mine, above, 0.0)
    target = target + times(jnp.concatenate([own2, above], axis=1), (st_hi[...], st_lo[...]))
    columns = jnp.transpose(jnp.concatenate([target, jnp.zeros((8 - rhs, 128), F32)], axis=0))
    spread = [jnp.broadcast_to(columns[0:n3, r : r + 1], (n3, 128)) for r in range(rhs)]

    phase("p22_top_product")
    width = 2 * (ntop // ngz)
    step = 128 if width % 128 == 0 else width
    chip_steps = sorted(range(chips), key=lambda j: -min(j, chips - j))
    rows = sorted(range(ngy), key=lambda i: -min(i, ngy - i))

    def term_to(i, j):
        there = step_along("y", b, i, ngy)
        spot = 2 * (i * chips + j) + core
        send(part.at[there, chip_at[j]], got5.at[spot], (a, there, 2 * chip_at[j] + 1), TERM_G)

    loads[-1].wait()
    for j in chip_steps:
        for p in range(0, width, step):
            start = chip_at[j] * width + p
            if step == 128:
                start = pl.multiple_of(start, 128)
            block = ti[:, pl.ds(start, step)]
            for r in range(rhs):
                scale = spread[r] if step == 128 else jnp.broadcast_to(spread[r][:, 0:1], (n3, step))
                part[r, chip_at[j], :, p : p + step] = jnp.sum(scale * block, axis=0, keepdims=True)
        for i in rows:
            if i or j:
                term_to(i, j)

    @pl.when(jnp.logical_not(keeper))
    def _():
        term_to(0, 0)

    phase("p23_wait_top1")
    along_x = sorted(range(1, ngx), key=lambda k: -min(k, ngx - k))

    @pl.when(keeper)
    def _():
        term = part[b, chip]
        arrived(TERM_G, got5.at[1:plane])
        for k in range(plane):
            if k != 1:
                term += got5[k]
        s6[...] = term
        pl.semaphore_signal(go, inc=1, device_id=other, device_id_type=MESH)
        pl.semaphore_wait(word3, 2)
        for k in along_x:
            send(s6, got6.at[k], at(k, 0, 0), LINE_G)

    @pl.when(jnp.logical_not(keeper))
    def _():
        pl.semaphore_wait(word3, 2)
        pl.semaphore_wait(go, 1)

    phase("p24_top2")
    arrived(ROWS_G, rall.at[0 : 3 if chips > 1 else 1])
    if chips > 1:
        send(rall.at[before[2], 0:16], rall.at[before[2], 0:16], after, ACROSS_G)
        send(rall.at[after[2], 16:32], rall.at[after[2], 16:32], before, ACROSS_G)
        for d in (after, before):
            send(rall.at[d[2]], rall.at[d[2]], other, CORE_G)

    @pl.when(keeper)
    def _():
        term = s6[...]
        arrived(LINE_G, got6.at[1:ngx])
        for k in along_x:
            term += got6[k]
        yall[b, chip] = term
        for dy, dz in offsets:
            send(yall.at[b, chip], yall.at[b, chip], at(0, dy, dz), SPREAD_G, SPREAD_G + (1 + dz) // 2 % chips)

    phase("p25_top3")
    if chips > 1:
        far = at(0, 0, 4)[2]
        arrived(ACROSS_G, rall.at[0])
        send(rall.at[far], rall.at[far], other, CORE_G)

    @pl.when(keeper)
    def _():
        arrived(SPREAD_G, got5.at[1:ngy])

    @pl.when(jnp.logical_not(keeper))
    def _():
        arrived(SPREAD_G, got5.at[0:ngy])

    phase("p26_top_back")
    total = [jnp.zeros((n3, step), F32) for _ in range(rhs)]
    for j in reversed(chip_steps):
        group = chip_at[(-j) % chips]
        if j:
            arrived(SPREAD_G + j, got5.at[0:ngy])
        for p in range(0, width, step):
            start = group * width + p
            if step == 128:
                start = pl.multiple_of(start, 128)
            block = ti[:, pl.ds(start, step)]
            for r in range(rhs):
                total[r] += block * yall[r, group, :, p : p + step]
    phase("p27_down")
    ones = jnp.ones((8, step), BF16)
    back = jnp.zeros((rhs, n3), F32)
    which = iota((rhs, n3), 0)
    for r in range(rhs):
        hi, lo = split(total[r])
        both_sums = dot(ones, hi, BACK) + dot(ones, lo, BACK)
        back += jnp.where(which == r, both_sums[0:rhs], 0.0)
    down_send[...] = jnp.zeros((rhs, 128), F32)
    down_send[:, 0:n3] = back
    right_sides = times(down_send[...], (back_hi[...], back_lo[...]), BACK)
    gap2[me] = own2 + right_sides[:, 0:128]
    low2[...] = right_sides[:, 128:256]
    gap1[c] = own1 + right_sides[:, 256:384]
    low1[...] = right_sides[:, 384:512]
    for dy, dz in offsets:
        send(low2, gap2.at[plane + me], at(1, dy, dz), GAP_G)
    for dy, dz in offsets:
        send(gap2.at[me], gap2.at[me], at(0, dy, dz), GAP_G)
    send(low2, gap2.at[plane + me], at(1, 0, 0), GAP_G)
    for k in steps + [0]:
        send(low1, gap1.at[ngz + c], at(1, 0, k), FIRST_GAP_G)
    for k in steps:
        send(gap1.at[c], gap1.at[c], at(0, 0, k), FIRST_GAP_G)
    send(down_send, down_got, at(1, 0, 0), DOWN_G)

    phase("p29_rows")
    if chips > 1:
        arrived(CORE_G, rall.at[0:3])
    hi, lo = split(rall[...].reshape(32 * ngz, 128 * groups2))
    rows = dot(w1_h[64:128, 0 : 32 * ngz], hi) + dot(w1_l[64:128, 0 : 32 * ngz], hi) + dot(w1_h[64:128, 0 : 32 * ngz], lo)
    hi, lo = split(rows)
    w2_h[64:128, :] = hi
    w2_l[64:128, :] = lo

    def gathered(ref, members):
        blocks = []
        for g in range((members + 3) // 4):
            own_part, lower_part = ref[4 * g], ref[members + 4 * g]
            for i in range(4 * g + 1, min(4 * g + 4, members)):
                own_part += ref[i]
                lower_part += ref[members + i]
            blocks.append(own_part + jnp.where(a > 0, lower_part, 0.0))
        return jnp.concatenate(blocks, axis=1)

    for group, ref in ((HALO_G, got_halo), (FI_G, fi), (SI_G, si), (ST_G, st), (FT_G, ft), (FIRST_G, got1.at[1:ngz])):
        sent(group, ref)
    sent(SECOND_G, got2.at[1 : 2 * plane])
    sent(UP_G, up_send)
    sent(ROWS_G, rall.at[0 : 3 if chips > 1 else 1])
    if chips > 1:
        sent(ACROSS_G, rall.at[0])
        sent(CORE_G, rall.at[0:3])

    @pl.when(keeper)
    def _():
        sent(TERM_G, got5.at[1 : plane // 2])
        sent(LINE_G, got6.at[1:ngx])
        sent(SPREAD_G, got5.at[1:plane])

    @pl.when(jnp.logical_not(keeper))
    def _():
        sent(TERM_G, got5.at[0 : plane // 2])

    phase("p30_wait_gap")
    arrived(DOWN_G, down_got)
    z3 = down_send[...] + jnp.where(a > 0, pltpu.roll(down_got[...], n3, 1), 0.0)
    corr_part = times(jnp.concatenate([s_leaf, z3], axis=1), tuple(jnp.concatenate([e[:, 0:128], e[:, 256:384]], axis=1) for e in e_pair), BACK)
    arrived(FIRST_GAP_G, gap1.at[1 : 2 * ngz])
    z12 = times(gathered(gap1, ngz), w1_pair, BACK)
    arrived(GAP_G, gap2.at[1 : 2 * plane])
    phase("p31_z_leaf")
    z12 = z12 + times(gathered(gap2, plane), (w2_h[...], w2_l[...]), BACK)

    result = corr_part + times(z12, (e_h[:, 128:256], e_l[:, 128:256]), BACK)
    for j in range(4):
        corr[j] = result[:, 128 * j : 128 * j + 128]
    phase("p32_rim")
    rim = sorted(enumerate(RIM), key=lambda e: far_first(e[1]))
    spot = {i: sum(1 if d[2] else 4 for d in RIM[:i]) for i in range(len(RIM))}
    for i, (dx, dy, dz) in rim:
        there = at(-dx, -dy, -dz)
        if dz == 0:
            send(corr, got_corr.at[spot[i] : spot[i] + 4], there, RIM_G)
        else:
            send(corr.at[0], got_corr.at[spot[i]], there, RIM_G)

    total = [corr[j] for j in range(4)]
    arrived(RIM_G, got_corr)
    for i, (dx, dy, dz) in rim:
        turn = side * 8 * dx + side * dy
        keep = (at_x == side + 1) if dx else (at_x <= side)
        keep = keep & ((at_y == side + 1) if dy else (at_y <= side))
        if dx:
            keep = keep & (a < ngx - 1)
        if dy:
            keep = keep & (b < ngy - 1)
        if dz:
            keep = keep & (c < ngz - 1) & (at_z == 1)
        for j in range(4) if dz == 0 else (0,):
            v = got_corr[spot[i] + j]
            v = pltpu.roll(v, turn, 1) if turn else v
            total[j if dz == 0 else 3] += jnp.where(keep, v, 0.0)
    rows = []
    for j in range(4):
        rows += [total[j][:, 0:64], total[j][:, 64:128]]
    out_h[...] = jnp.concatenate(rows, axis=0)
    phase("p34_finish")
    sent(GAP_G, gap2.at[1 : 2 * plane])
    sent(FIRST_GAP_G, gap1.at[1 : 2 * ngz])
    sent(DOWN_G, down_send)
    sent(RIM_G, got_corr)
    stack.close()


def prolong(cfg, ct_h, out_h, ct, out_v, in_sem, out_sem):
    rhs, fine = cfg[3], cfg[4]
    load = pltpu.make_async_copy(ct_h, ct, in_sem)
    load.start()
    stack = contextlib.ExitStack()
    stack.enter_context(jax.named_scope("q0"))
    shape = (fine, 128)
    fx, col = floats(shape, 0), floats(shape, 1)
    rest = col - 64.0 * whole_part(col, 64)
    cx = whole_part(rest, 8)
    along_x = tent(cx - 1.0, fx) * 0.25
    along_y = tent(rest - 8.0 * cx - 1.0, fx) * 0.25
    spread_xy = (along_x[:, None, :] * along_y[None, :, :]).reshape(fine * fine, 128).astype(BF16)
    shape = (rhs * fine, 8 * rhs)
    row, col = floats(shape, 0), floats(shape, 1)
    fr = whole_part(row, fine)
    fz = row - fine * fr
    cz = whole_part(col, rhs)
    cr = col - rhs * cz
    same = jnp.maximum(1.0 - jnp.abs(cr - fr), 0.0)
    spread_z = (tent(cz - 1.0, fz) * same * 0.25).astype(BF16)

    stack.close()
    stack.enter_context(jax.named_scope("q1"))
    load.wait()
    stack.close()
    stack.enter_context(jax.named_scope("q2"))
    ct_h, ct_l = split(ct[...])
    ht = dot(spread_z, ct_h) + dot(spread_z, ct_l)
    ht_h = ht.astype(BF16).astype(F32)
    ht = jnp.concatenate([ht_h, ht - ht_h], axis=1)
    stack.close()
    stack.enter_context(jax.named_scope("q3"))
    stores = []
    for r in range(rhs):
        part_r = ht[r * fine : (r + 1) * fine].astype(BF16)
        out_v[r] = dot(spread_xy, part_r, BACK).reshape(fine, fine, fine)
        store = pltpu.make_async_copy(out_v.at[r], out_h.at[r], out_sem.at[r])
        store.start()
        stores.append(store)
    stack.close()
    stack.enter_context(jax.named_scope("q4"))
    for store in stores:
        store.wait()
    stack.close()


def per_device(mesh_sizes, *args):
    (rs, it, cf, od, li, lf, ls, lt, fi, fs, ft, si, st, ti) = args
    ngx, ngy, ngz = mesh_sizes
    od = od.reshape(1, -1)
    rhs, fine = rs.shape[0], rs.shape[1]
    side = fine // 4
    leaf, n1, n2, n3, ntop = li.shape[3], fs.shape[3], st.shape[3], ti.shape[0], ti.shape[1]
    li, fs, ft, st = (jnp.transpose(v, (0, 1, 3, 2, 4))[0, 0] for v in (li, fs, ft, st))
    fi, si = jnp.transpose(fi, (0, 2, 1, 3))[0], jnp.transpose(si, (1, 0, 2))
    lf, ls = (jnp.transpose(v, (0, 1, 4, 2, 3))[0, 0] for v in (lf, ls))
    lt = jnp.transpose(lt, (0, 1, 2, 4, 3))[0, 0, 0]
    cfg = (ngx, ngy, ngz, rhs, fine, side, leaf, n1, n2, n3, ntop)
    plane = ngy * ngz
    groups1, groups2 = (ngz + 3) // 4, (plane + 3) // 4
    cells = side**3
    inputs = [rs, it, cf, od, li, lf, ls, lt, fi, fs, ft, si, st, ti]
    v = pltpu.VMEM
    width = 2 * (ntop // ngz)
    narrow = [x.reshape(x.shape[0], -1) if any(x is y for y in (li, lf, ls, fs, ft, st)) else x for x in inputs]
    scratch = [v(x.shape, x.dtype) for x in narrow]
    scratch += [
        v((fine * fine, rhs * fine), F32), v((fine * fine, rhs * fine), F32), v((128, fine * fine), BF16),
        v((cells, 384), F32), v((512, 384), BF16), v((512, 384), BF16),
        v((32, 256), F32), v((128, 256), BF16), v((128, 256), BF16),
        v((32, 128), F32), v((256, 128), BF16), v((256, 128), BF16),
        v((32, 128), F32), v((32, 128), F32), v((512, 128), BF16), v((512, 128), BF16), v(st.shape[::2], F32), v(ft.shape[::2], F32),
        v((128, 128 * groups1), F32), v((128, 128 * groups1), BF16), v((128, 128 * groups1), BF16),
        v((64, 128 * groups2), F32), v((128, 128 * groups2), BF16), v((128, 128 * groups2), BF16),
        v(fi.shape, F32), v(si.shape, F32), v((ngz, 32, 128 * groups2), F32),
        v((128, 128 * groups2), BF16), v((128, 128 * groups2), BF16),
        v((4, rhs, 128), F32), v((len(HALO) + 3 * len(FLAT), rhs, 128), F32),
        v((groups1, rhs, 128), F32), v((ngz, rhs, 128), F32),
        v((groups2, rhs, 128), F32), v((2 * plane, rhs, 128), F32),
        v((rhs, 128), F32), v((rhs, 128), F32),
        v((rhs, ngz // 2, 1, width), F32), v((plane, 1, width), F32),
        v((1, width), F32), v((ngx, 1, width), F32),
        v((rhs, ngz // 2, 1, width), F32),
        v((rhs, 128), F32), v((rhs, 128), F32),
        v((2 * plane, rhs, 128), F32), v((2 * ngz, rhs, 128), F32), v((rhs, 128), F32), v((rhs, 128), F32),
        v((4, rhs, 128), F32), v((sum(1 if d[2] else 4 for d in RIM), rhs, 128), F32),
        pltpu.SemaphoreType.DMA((len(inputs) + rhs - 2,)),
        *[pltpu.SemaphoreType.REGULAR] * 4,
        pltpu.SemaphoreType.DMA((SPREAD_G + 1,)), pltpu.SemaphoreType.DMA((SPREAD_G + ngz // 2,)),
    ]
    coarse = pl.pallas_call(
        functools.partial(kernel, cfg),
        out_shape=jax.ShapeDtypeStruct((8 * rhs, 64), F32),
        in_specs=[pl.BlockSpec(memory_space=pl.ANY)] * len(inputs),
        out_specs=pl.BlockSpec(memory_space=pltpu.VMEM),
        scratch_shapes=scratch,
        compiler_params=pltpu.CompilerParams(
            collective_id=0, has_side_effects=True, vmem_limit_bytes=67043328
        ),
        name="coarse_correction",
    )(*inputs)
    return pl.pallas_call(
        functools.partial(prolong, cfg),
        out_shape=jax.ShapeDtypeStruct(rs.shape, F32),
        in_specs=[pl.BlockSpec(memory_space=pl.ANY)],
        out_specs=pl.BlockSpec(memory_space=pl.ANY),
        scratch_shapes=[v((8 * rhs, 64), F32), v(rs.shape, F32), pltpu.SemaphoreType.DMA, pltpu.SemaphoreType.DMA((rhs,))],
        compiler_params=pltpu.CompilerParams(vmem_limit_bytes=67043328),
        name="prolong",
    )(coarse)


def solution(mesh):
    sizes = tuple(mesh.shape[n] for n in AXES)
    cells = P("gx", "gy", "gz")
    lines = P("gx", "gy", "gz", None)
    blocks = P("gx", "gy", "gz", None, None)
    field = P(None, "gx", "gy", "gz")
    return jax.shard_map(
        functools.partial(per_device, sizes),
        mesh=mesh,
        in_specs=(
            field, field, cells, lines, blocks, blocks, blocks, blocks, lines, blocks, blocks,
            P("gx", ("gy", "gz"), None), blocks, P(("gx", "gy", "gz"), None),
        ),
        out_specs=field,
        check_vma=False,
    )
```

```python
import contextlib
import functools

import jax
import jax.numpy as jnp
from jax import lax
from jax.experimental import pallas as pl
from jax.experimental.pallas import tpu as pltpu
from jax.sharding import PartitionSpec as P

MESH = pl.DeviceIdType.MESH
F32 = jnp.float32
BF16 = jnp.bfloat16
AXES = ("gx", "gy", "gz")

FLAT = ((1, 0), (-1, 0), (0, 1), (0, -1), (1, 1), (1, -1), (-1, 1))
ABOVE = ((0, 0),) + FLAT
BELOW = ((0, 0), (1, 0), (0, 1), (1, 1))
HALO = [(x, y, 0) for x, y in FLAT] + [(x, y, 1) for x, y in ABOVE] + [(x, y, -1) for x, y in BELOW]
RIM = [(1, 0, 0), (0, 1, 0), (1, 1, 0), (0, 0, 1), (1, 0, 1), (0, 1, 1), (1, 1, 1)]

(
    HALO_G, FI_G, SI_G, ST_G, FT_G, FIRST_G, SECOND_G, UP_G, ROWS_G, ACROSS_G, CORE_G,
    TERM_G, LINE_G, GAP_G, FIRST_GAP_G, DOWN_G, RIM_G, SPREAD_G,
) = range(18)
SENT = {FI_G: 1, SI_G: 2, ST_G: 3, FT_G: 4, ROWS_G: 5, ACROSS_G: 5, CORE_G: 5, TERM_G: 6, LINE_G: 7, SPREAD_G: 8}


def split(value):
    high = value.astype(BF16)
    return high, (value - high.astype(F32)).astype(BF16)


def dot(left, right, dims=((1,), (0,))):
    return lax.dot_general(left, right, (dims, ((), ())), preferred_element_type=F32)


def times(value, factor, dims=((1,), (0,))):
    f_high, f_low = factor
    n = value.shape[0]
    if n > 4:
        high, low = split(value)
        return dot(high, f_high, dims) + dot(low, f_high, dims) + dot(high, f_low, dims)
    high = value.astype(BF16).astype(F32)
    both = jnp.concatenate([high, value - high], axis=0).astype(BF16)
    out = dot(both, f_high, dims) + dot(both, f_low, dims)
    return out[0:n] + out[n : 2 * n]


BACK = ((1,), (1,))


def iota(shape, dim):
    return lax.broadcasted_iota(jnp.int32, shape, dim)


def floats(shape, dim):
    return iota(shape, dim).astype(F32)


def whole_part(value, by):
    return jnp.floor((value + 0.5) * (1.0 / by))


def tent(coarse, fine):
    return jnp.maximum(4.0 - jnp.abs(fine - 4.0 * coarse), 0.0)


def inner(coarse, fine, first):
    below = 1.0 - first * jnp.maximum(1.0 - fine, 0.0)
    return (tent(coarse, fine + 1.0) + tent(coarse, fine - 1.0) * below) * 0.0625


def outer(coarse, fine):
    return tent(coarse, fine) * 0.0625


def kernel(cfg, *refs):
    ngx, ngy, ngz, rhs, fine, side, leaf, n1, n2, n3, ntop = cfg
    plane = ngy * ngz
    cells = side**3
    (rs_h, it_h, cf_h, od_h, li_h, lf_h, ls_h, lt_h, fi_h, fs_h, ft_h, si_h, st_h, ti_h) = refs[:14]
    out_h = refs[14]
    (
        rs, it, cf, od, li, lf, ls, lt, fi, fs, ft, si, st, ti,
        pack_it, pack_q, a21, bmat, e_h, e_l, fsx, fs_hi, fs_lo, stx, st_hi, st_lo,
        stu, ftu, back_hi, back_lo, st_high, ft_high,
        w1, w1_h, w1_l, w2, w2_h, w2_l, fi_low, si_low, rall, r_hi, r_lo,
        flat, got_halo, send1, got1, send2, got2, up_send, up_got,
        part, got5, s6, got6, yall, down_send, down_got, gap2, gap1, low2, low1, blocks, corr, got_corr,
        local_sem, word1, word2, word3, go, send_sem, recv_sem,
    ) = refs[15:]

    a, b, c = (lax.axis_index(n) for n in AXES)
    me = b * ngz + c
    stack = contextlib.ExitStack()

    def phase(name):
        stack.close()
        stack.enter_context(jax.named_scope(name))


    known = {}

    def step_along(name, here, by, n):
        by %= n
        if (name, by) not in known:
            known[name, by] = lax.rem(here + by, n) if by else here
        return known[name, by]

    def at(dx, dy, dz):
        return step_along("x", a, dx, ngx), step_along("y", b, dy, ngy), step_along("z", c, dz, ngz)

    def quarter(dz):
        if ("q", dz % ngz) not in known:
            known["q", dz % ngz] = lax.div(step_along("z", c, dz, ngz), 4)
        return known["q", dz % ngz]

    for n, here, size in (("x", a, ngx), ("y", b, ngy), ("z", c, ngz)):
        for by in range(size):
            step_along(n, here, by, size)
    for dz in range(ngz):
        quarter(dz)
    chips = ngz // 2
    chip, core = lax.div(c, 2), lax.rem(c, 2)
    chip_at = [lax.rem(chip + j, chips) if j else chip for j in range(chips)]
    keeper = core == 1
    other = (a, b, c + 1 - 2 * core)

    def far_first(d):
        return -sum(min(i % n, -i % n) * w for i, n, w in zip(d, (ngx, ngy, ngz), (2, 2, 1))), d

    def copy_of(src, dst, device, group, into=None):
        return pltpu.make_async_remote_copy(
            src_ref=src,
            dst_ref=dst,
            send_sem=send_sem.at[SENT.get(group, 0)],
            recv_sem=recv_sem.at[group if into is None else into],
            device_id=device,
            device_id_type=MESH,
        )

    def send(src, dst, device, group, into=None):
        copy_of(src, dst, device, group, into).start()

    def arrived(group, ref):
        copy_of(ref, ref, other, group).wait_recv()

    def sent(group, ref):
        copy_of(ref, ref, other, group).wait_send()

    phase("p00_loads")
    first = [(it_h, it), (cf_h, cf)] + [(rs_h.at[r], rs.at[r]) for r in range(rhs)]
    pairs = [
        (od_h, od), (li_h, li), (lf_h, lf), (ls_h, ls), (lt_h, lt),
        (fi_h, fi), (si_h, si), (fs_h, fs), (ft_h, ft), (st_h, st),
    ]
    pairs = first + [(s.at[:, 0, :] if len(s.shape) > len(d.shape) else s, d) for s, d in pairs] + [(ti_h, ti)]
    loads = [pltpu.make_async_copy(s, d, local_sem.at[i]) for i, (s, d) in enumerate(pairs)]
    for load in loads[:-1]:
        load.start()

    phase("p01_signal")
    partners = {(0, 0, dz) for dz in range(ngz)}
    for d in HALO + RIM:
        for s in (1, -1):
            partners.add((s * d[0] % ngx, s * d[1] % ngy, s * d[2] % ngz))
    partners.discard((0, 0, 0))
    barrier = pltpu.get_barrier_semaphore()
    for d in sorted(partners, key=far_first):
        pl.semaphore_signal(barrier, inc=1, device_id=at(*d), device_id_type=MESH)

    first_x = jnp.where(a == 0, 1.0, 0.0).astype(F32)
    first_y = jnp.where(b == 0, 1.0, 0.0).astype(F32)
    first_z = jnp.where(c == 0, 1.0, 0.0).astype(F32)

    phase("p02_weights")
    shape = (64, fine * fine)
    row, col = floats(shape, 0), floats(shape, 1)
    cx = whole_part(row, 8)
    cy = row - 8.0 * cx - 1.0
    cx = cx - 1.0
    fx = whole_part(col, fine)
    fy = col - fine * fx
    ox, oy = outer(cx, fx), outer(cy, fy)
    a21[0:64, :] = (inner(cx, fx, first_x) * oy + ox * inner(cy, fy, first_y)).astype(BF16)
    a21[64:128, :] = (ox * oy).astype(BF16)

    zshape = (8 * rhs, 2 * rhs * fine)
    row, col = floats(zshape, 0), floats(zshape, 1)
    cz = whole_part(row, rhs)
    cr = row - rhs * cz
    cz = cz - 1.0
    kind = whole_part(col, rhs * fine)
    rest = col - rhs * fine * kind
    fr = whole_part(rest, fine)
    fz = rest - fine * fr
    same = jnp.maximum(1.0 - jnp.abs(cr - fr), 0.0)
    wvz = ((1.0 - kind) * outer(cz, fz) + kind * inner(cz, fz, first_z)) * same
    wvz = wvz.astype(BF16)

    phase("p03_wait_residual")
    own = a21[64:128, :]
    both = a21[...]
    loads[0].wait()
    for r in range(rhs):
        pack_it[:, fine * r : fine * r + fine] = it[r].reshape(fine * fine, fine)
    i_h, i_l = split(pack_it[...])
    from_it = dot(both, i_h) + dot(both, i_l)
    loads[1].wait()
    diagonal = 6.0 + cf[...]
    for r in range(rhs):
        loads[2 + r].wait()
        pack_q[:, fine * r : fine * r + fine] = (rs[r] - diagonal * it[r]).reshape(fine * fine, fine)
    q_h, q_l = split(pack_q[...])
    g1 = from_it[0:64] + dot(own, q_h) + dot(own, q_l)
    g_h, g_l = split(jnp.concatenate([g1, from_it[64:128]], axis=1))
    ct = dot(wvz, g_h, BACK) + dot(wvz, g_l, BACK)
    for j in range(4):
        lo = ct[2 * rhs * j : 2 * rhs * j + rhs]
        hi = ct[2 * rhs * j + rhs : 2 * rhs * j + 2 * rhs]
        flat[j] = jnp.concatenate([lo, hi], axis=1)

    phase("p05_barrier")
    pl.semaphore_wait(barrier, len(partners))

    halo = sorted(enumerate(HALO), key=lambda e: far_first(e[1]))
    thin = 4 * len(FLAT)
    for i, (dx, dy, dz) in halo:
        if dz == 0:
            send(flat, got_halo.at[4 * i : 4 * i + 4], at(dx, dy, dz), HALO_G)
        else:
            src = flat.at[3 if dz == 1 else 0]
            send(src, got_halo.at[thin + i - len(FLAT)], at(dx, dy, dz), HALO_G)

    def tell(sem):
        for dx in (1, -1):
            pl.semaphore_signal(sem, inc=1, device_id=at(dx, 0, 0), device_id_type=MESH)

    tell(word1)
    loads[-1].start()
    for load in loads[2 + rhs : -1]:
        load.wait()
    send(fi, fi_low, at(0, 0, 1), FI_G)
    send(si, si_low, at(0, 1, 0), SI_G)
    send(st, st_high, at(-1, 0, 0), ST_G)
    send(ft, ft_high, at(-1, 0, 0), FT_G)

    phase("p07_factor")
    shape = (cells, 384)
    m, k = iota(shape, 0), iota(shape, 1)
    e1, e2 = leaf + n1, leaf + n1 + n2
    want = jnp.where(m < e1, m + (192 - leaf), jnp.where(m < e2, m + (128 - e1), m + (256 - e2)))
    bmat[...] = jnp.where((m >= leaf) & (k == want), 1.0, 0.0).astype(F32)
    li_v = li[...]
    li_pair = split(li_v)
    bmat[0:leaf, 0:leaf] = li_v
    bmat[0:leaf, 192 : 192 + 2 * n1] = -times(li_v, split(lf[...]), BACK)
    bmat[0:leaf, 128 : 128 + 2 * n2] = -times(li_v, split(ls[...]), BACK)
    bmat[0:leaf, 256 : 256 + 2 * n3] = -times(li_v, split(lt[...]), BACK)
    bh, bl = split(bmat[...])
    shape = (512, cells)
    k = iota(shape, 0)
    z, x, y = k >> 6, (k >> 3) & 7, k & 7
    inside = (z >= 1) & (z <= side) & (x >= 1) & (x <= side) & (y >= 1) & (y <= side)
    cell = jnp.where(inside, ((x - 1) * side + (y - 1)) * side + (z - 1), -1)
    chosen = jnp.where(cell == od[...], 1.0, 0.0).astype(BF16)
    e_h[...] = dot(chosen, bh).astype(BF16)
    e_l[...] = dot(chosen, bl).astype(BF16)

    phase("p08_place")
    fsx[...] = jnp.zeros(fsx.shape, F32)
    fsx[0:n1, 0 : 2 * n2] = -fs[...]
    fsx[0:n1, 128 : 128 + 2 * n3] = -ft[...]
    stx[...] = jnp.zeros(stx.shape, F32)
    stx[0:n2, 0 : 2 * n3] = -st[...]
    place1 = 32 * lax.rem(c, 4)
    place2 = n2 * lax.rem(me, 4)
    shift = (128, 32)
    put1 = jnp.where(iota(shift, 0) == iota(shift, 1) + place1, 1.0, 0.0).astype(BF16)
    put2 = jnp.where(iota(shift, 0) == iota(shift, 1) + place2, 1.0, 0.0).astype(BF16)
    hi, lo = split(fsx[...])
    fs_hi[...] = dot(put1, hi).astype(BF16)
    fs_lo[...] = dot(put1, lo).astype(BF16)
    hi, lo = split(stx[...])
    st_hi[0:128, :] = dot(put2, hi).astype(BF16)
    st_lo[0:128, :] = dot(put2, lo).astype(BF16)

    groups1 = (ngz + 3) // 4
    groups2 = (plane + 3) // 4

    phase("p09_w1")
    arrived(FI_G, fi_low)
    w1[...] = jnp.zeros(w1.shape, F32)
    mine = fi[:, 0, :]
    lower = jnp.where(c > 0, fi_low[:, 0, :], 0.0)
    for m in range(ngz):
        w1[64 : 64 + n1, 32 * m : 32 * m + n1] = mine[:, n1 * m : n1 * m + n1]
        w1[64 + n1 : 64 + 2 * n1, 32 * m : 32 * m + n1] = lower[:, n1 * m : n1 * m + n1]
    hi, lo = split(w1[...])
    w1_h[...] = hi
    w1_l[...] = lo
    e_mid = (e_h[:, 128:256], e_l[:, 128:256])
    lead = dot(e_mid[0], hi) + dot(e_mid[1], hi) + dot(e_mid[0], lo)
    lead_pair = split(lead)

    phase("p10_wait_halo")
    phase("p11_add_halo")
    lane = iota((rhs, 128), 1)
    at_z, at_x, at_y = lane >> 6, (lane >> 3) & 7, lane & 7

    def along(at_, d):
        if d == 0:
            return (at_ >= 1) & (at_ <= side)
        return at_ == (1 if d == 1 else side)

    def exists(i, d, n):
        return (i - d >= 0) & (i - d < n) if d else True

    total = [flat[j] for j in range(4)]
    arrived(HALO_G, got_halo)
    for i, (dx, dy, dz) in halo:
        turn = (-(side * 8) * dx - side * dy) % 128
        keep = along(at_x, dx) & along(at_y, dy)
        there = exists(a, dx, ngx) & exists(b, dy, ngy) & exists(c, dz, ngz)
        keep = keep & there
        if dz == 0:
            for j in range(4):
                v = got_halo[4 * i + j]
                v = pltpu.roll(v, turn, 1) if turn else v
                total[j] += jnp.where(keep, v, 0.0)
        else:
            v = got_halo[thin + i - len(FLAT)]
            v = pltpu.roll(v, turn, 1) if turn else v
            keep = keep & (at_z == (1 if dz == 1 else 0))
            j = 0 if dz == 1 else 3
            total[j] += jnp.where(keep, v, 0.0)

    phase("p12_leaf")
    gathered_cells = jnp.concatenate(total, axis=1)
    partial = times(gathered_cells, lead_pair)
    for g in range(groups1):
        send1[g] = partial[:, 128 * g : 128 * g + 128]
    steps = sorted(range(1, ngz), key=lambda k: -min(k, ngz - k))
    for k in steps:
        send(send1.at[quarter(k)], got1.at[k], at(0, 0, k), FIRST_G)
    own1 = send1[quarter(0)]
    word = pl.semaphore_wait
    word(word1, 2)
    tell(word2)
    e_pair = (e_h[...], e_l[...])
    s = times(gathered_cells, e_pair)
    s_leaf, s12, s3 = s[:, 0:128], s[:, 128:256], s[:, 256:384]
    w1_pair = (w1_h[...], w1_l[...])

    phase("p15_w2")
    arrived(SI_G, si_low)
    w2[...] = jnp.zeros(w2.shape, F32)
    mine = si[:, 0, :]
    lower = jnp.where(b > 0, si_low[:, 0, :], 0.0)
    for g in range(groups2):
        wide = min(4, plane - 4 * g) * n2
        cut = slice(4 * g * n2, 4 * g * n2 + wide)
        w2[0:n2, 128 * g : 128 * g + wide] = mine[:, cut]
        w2[n2 : 2 * n2, 128 * g : 128 * g + wide] = lower[:, cut]
    hi, lo = split(w2[...])
    w2_h[0:64, :] = hi
    w2_l[0:64, :] = lo
    back_rows = times(fsx[:, 0:64], (hi, lo))
    rall[c] = back_rows
    rows_h, rows_l = split(back_rows)
    r_hi[...] = dot(put1, rows_h).astype(BF16)
    r_lo[...] = dot(put1, rows_l).astype(BF16)
    partial = times(s12[:, 0:64], (hi, lo))

    phase("p16_wait_first")
    arrived(FIRST_G, got1.at[1:ngz])
    for k in steps:
        own1 += got1[k]
    phase("p17_second_product")
    own1 = jnp.where((lane >= place1) & (lane < place1 + n1), own1, 0.0)
    partial = partial + times(own1, (r_hi[...], r_lo[...]))
    for g in range(groups2):
        send2[g] = partial[:, 128 * g : 128 * g + 128]
    offsets = [(dy, dz) for dy in range(ngy) for dz in range(ngz) if dy or dz]
    offsets = sorted(offsets, key=lambda d: far_first((0,) + d))

    def group_of(dy, dz):
        if ngz % 4:
            return lax.div(step_along("y", b, dy, ngy) * ngz + step_along("z", c, dz, ngz), 4)
        return step_along("y", b, dy, ngy) * (ngz // 4) + quarter(dz)

    both_planes = [(0,) + d for d in offsets] + [(1,) + d for d in offsets] + [(1, 0, 0)]
    both_planes = sorted(both_planes, key=far_first)
    for dx, dy, dz in both_planes:
        send(send2.at[group_of(dy, dz)], got2.at[plane * dx + dy * ngz + dz], at(-dx, dy, dz), SECOND_G)
    word(word2, 2)
    tell(word3)
    own2 = send2[me // 4]

    fs_top = (fs_hi[:, 128:256], fs_lo[:, 128:256])
    s3 = s3 + times(own1, fs_top)
    up_send[...] = s3
    send(up_send, up_got, at(-1, 0, 0), UP_G)

    phase("p18_wait_second")
    stu[...] = jnp.zeros(stu.shape, F32)
    ftu[...] = jnp.zeros(ftu.shape, F32)
    arrived(ST_G, st_high)
    arrived(FT_G, ft_high)
    stu[0:n2, 0:n3] = -st_high[:, n3 : 2 * n3]
    ftu[0:n1, 0:n3] = -ft_high[:, n3 : 2 * n3]
    for ref, put, row in ((stu, put2, 128), (ftu, put1, 384)):
        hi, lo = split(jnp.where(a < ngx - 1, ref[...], 0.0))
        back_hi[row : row + 128, :] = dot(put, hi).astype(BF16)
        back_lo[row : row + 128, :] = dot(put, lo).astype(BF16)
    column = iota((128, 128), 1)
    for got, src in ((back_hi, (st_hi[0:128, :], fs_top[0])), (back_lo, (st_lo[0:128, :], fs_top[1]))):
        for row, rows in zip((0, 256), src):
            got[row : row + 128, :] = jnp.where(column < n3, rows.astype(F32), 0.0).astype(BF16)
    st_hi[128:256, :] = back_hi[128:256, :]
    st_lo[128:256, :] = back_lo[128:256, :]
    send(rall.at[c], rall.at[c], other, ROWS_G)
    if chips > 1:
        after, before = at(0, 0, 2), at(0, 0, -2)
        send(rall.at[c], rall.at[c], after, ROWS_G)
        send(rall.at[c], rall.at[c], before, ROWS_G)
    arrived(UP_G, up_got)
    target = s3 + jnp.where(a < ngx - 1, pltpu.roll(up_got[...], 128 - n3, 1), 0.0)
    arrived(SECOND_G, got2.at[1 : 2 * plane])
    above = got2[plane]
    for dy, dz in offsets:
        own2 += got2[dy * ngz + dz]
        above += got2[plane + dy * ngz + dz]
    phase("p21_target")
    mine = (lane >= place2) & (lane < place2 + n2)
    own2 = jnp.where(mine, own2, 0.0)
    above = jnp.where(mine, above, 0.0)
    target = target + times(jnp.concatenate([own2, above], axis=1), (st_hi[...], st_lo[...]))
    columns = jnp.transpose(jnp.concatenate([target, jnp.zeros((8 - rhs, 128), F32)], axis=0))
    spread = [jnp.broadcast_to(columns[0:n3, r : r + 1], (n3, 128)) for r in range(rhs)]

    phase("p22_top_product")
    width = 2 * (ntop // ngz)
    step = 128 if width % 128 == 0 else width
    chip_steps = sorted(range(chips), key=lambda j: -min(j, chips - j))
    rows = sorted(range(ngy), key=lambda i: -min(i, ngy - i))

    def term_to(i, j):
        there = step_along("y", b, i, ngy)
        spot = 2 * (i * chips + j) + core
        send(part.at[there, chip_at[j]], got5.at[spot], (a, there, 2 * chip_at[j] + 1), TERM_G)

    loads[-1].wait()
    for j in chip_steps:
        for p in range(0, width, step):
            start = chip_at[j] * width + p
            if step == 128:
                start = pl.multiple_of(start, 128)
            block = ti[:, pl.ds(start, step)]
            for r in range(rhs):
                scale = spread[r] if step == 128 else jnp.broadcast_to(spread[r][:, 0:1], (n3, step))
                part[r, chip_at[j], :, p : p + step] = jnp.sum(scale * block, axis=0, keepdims=True)
        for i in rows:
            if i or j:
                term_to(i, j)

    @pl.when(jnp.logical_not(keeper))
    def _():
        term_to(0, 0)

    phase("p23_wait_top1")
    along_x = sorted(range(1, ngx), key=lambda k: -min(k, ngx - k))

    @pl.when(keeper)
    def _():
        term = part[b, chip]
        arrived(TERM_G, got5.at[1:plane])
        for k in range(plane):
            if k != 1:
                term += got5[k]
        s6[...] = term
        pl.semaphore_signal(go, inc=1, device_id=other, device_id_type=MESH)
        pl.semaphore_wait(word3, 2)
        for k in along_x:
            send(s6, got6.at[k], at(k, 0, 0), LINE_G)

    @pl.when(jnp.logical_not(keeper))
    def _():
        pl.semaphore_wait(word3, 2)
        pl.semaphore_wait(go, 1)

    phase("p24_top2")
    arrived(ROWS_G, rall.at[0 : 3 if chips > 1 else 1])
    if chips > 1:
        send(rall.at[before[2], 0:16], rall.at[before[2], 0:16], after, ACROSS_G)
        send(rall.at[after[2], 16:32], rall.at[after[2], 16:32], before, ACROSS_G)
        for d in (after, before):
            send(rall.at[d[2]], rall.at[d[2]], other, CORE_G)

    @pl.when(keeper)
    def _():
        term = s6[...]
        arrived(LINE_G, got6.at[1:ngx])
        for k in along_x:
            term += got6[k]
        yall[b, chip] = term
        for dy, dz in offsets:
            send(yall.at[b, chip], yall.at[b, chip], at(0, dy, dz), SPREAD_G, SPREAD_G + (1 + dz) // 2 % chips)

    phase("p25_top3")
    if chips > 1:
        far = at(0, 0, 4)[2]
        arrived(ACROSS_G, rall.at[0])
        send(rall.at[far], rall.at[far], other, CORE_G)

    @pl.when(keeper)
    def _():
        arrived(SPREAD_G, got5.at[1:ngy])

    @pl.when(jnp.logical_not(keeper))
    def _():
        arrived(SPREAD_G, got5.at[0:ngy])

    phase("p26_top_back")
    total = [jnp.zeros((n3, step), F32) for _ in range(rhs)]
    for j in reversed(chip_steps):
        group = chip_at[(-j) % chips]
        if j:
            arrived(SPREAD_G + j, got5.at[0:ngy])
        for p in range(0, width, step):
            start = group * width + p
            if step == 128:
                start = pl.multiple_of(start, 128)
            block = ti[:, pl.ds(start, step)]
            for r in range(rhs):
                total[r] += block * yall[r, group, :, p : p + step]
    phase("p27_down")
    ones = jnp.ones((8, step), BF16)
    back = jnp.zeros((rhs, n3), F32)
    which = iota((rhs, n3), 0)
    for r in range(rhs):
        hi, lo = split(total[r])
        both_sums = dot(ones, hi, BACK) + dot(ones, lo, BACK)
        back += jnp.where(which == r, both_sums[0:rhs], 0.0)
    down_send[...] = jnp.zeros((rhs, 128), F32)
    down_send[:, 0:n3] = back
    right_sides = times(down_send[...], (back_hi[...], back_lo[...]), BACK)
    gap2[me] = own2 + right_sides[:, 0:128]
    low2[...] = right_sides[:, 128:256]
    gap1[c] = own1 + right_sides[:, 256:384]
    low1[...] = right_sides[:, 384:512]
    for dx, dy, dz in both_planes:
        src = low2 if dx else gap2.at[me]
        send(src, gap2.at[plane * dx + me], at(dx, dy, dz), GAP_G)
    for k in steps + [0]:
        send(low1, gap1.at[ngz + c], at(1, 0, k), FIRST_GAP_G)
    for k in steps:
        send(gap1.at[c], gap1.at[c], at(0, 0, k), FIRST_GAP_G)
    send(down_send, down_got, at(1, 0, 0), DOWN_G)

    phase("p29_rows")
    if chips > 1:
        arrived(CORE_G, rall.at[0:3])
    hi, lo = split(rall[...].reshape(32 * ngz, 128 * groups2))
    rows = dot(w1_h[64:128, 0 : 32 * ngz], hi) + dot(w1_l[64:128, 0 : 32 * ngz], hi) + dot(w1_h[64:128, 0 : 32 * ngz], lo)
    hi, lo = split(rows)
    w2_h[64:128, :] = hi
    w2_l[64:128, :] = lo

    def gathered(ref, members):
        blocks = []
        for g in range((members + 3) // 4):
            own_part, lower_part = ref[4 * g], ref[members + 4 * g]
            for i in range(4 * g + 1, min(4 * g + 4, members)):
                own_part += ref[i]
                lower_part += ref[members + i]
            blocks.append(own_part + jnp.where(a > 0, lower_part, 0.0))
        return jnp.concatenate(blocks, axis=1)

    for group, ref in ((FI_G, fi), (SI_G, si), (ST_G, st), (FT_G, ft)):
        sent(group, ref)
    sent(ROWS_G, rall.at[0 : 7 if chips > 1 else 1])

    @pl.when(keeper)
    def _():
        sent(TERM_G, got5.at[1 : plane // 2])
        sent(LINE_G, got6.at[1:ngx])
        sent(SPREAD_G, got5.at[1:plane])

    @pl.when(jnp.logical_not(keeper))
    def _():
        sent(TERM_G, got5.at[0 : plane // 2])

    phase("p30_wait_gap")
    arrived(DOWN_G, down_got)
    z3 = down_send[...] + jnp.where(a > 0, pltpu.roll(down_got[...], n3, 1), 0.0)
    corr_part = times(jnp.concatenate([s_leaf, z3], axis=1), tuple(jnp.concatenate([e[:, 0:128], e[:, 256:384]], axis=1) for e in e_pair), BACK)
    arrived(FIRST_GAP_G, gap1.at[1 : 2 * ngz])
    z12 = times(gathered(gap1, ngz), w1_pair, BACK)
    arrived(GAP_G, gap2.at[1 : 2 * plane])
    phase("p31_z_leaf")
    z12 = z12 + times(gathered(gap2, plane), (w2_h[...], w2_l[...]), BACK)

    result = corr_part + times(z12, (e_h[:, 128:256], e_l[:, 128:256]), BACK)
    for j in range(4):
        corr[j] = result[:, 128 * j : 128 * j + 128]
    phase("p32_rim")
    rim = sorted(enumerate(RIM), key=lambda e: far_first(e[1]))
    spot = {i: sum(1 if d[2] else 4 for d in RIM[:i]) for i in range(len(RIM))}
    for i, (dx, dy, dz) in rim:
        there = at(-dx, -dy, -dz)
        if dz == 0:
            send(corr, got_corr.at[spot[i] : spot[i] + 4], there, RIM_G)
        else:
            send(corr.at[0], got_corr.at[spot[i]], there, RIM_G)

    total = [corr[j] for j in range(4)]
    arrived(RIM_G, got_corr)
    for i, (dx, dy, dz) in rim:
        turn = side * 8 * dx + side * dy
        keep = (at_x == side + 1) if dx else (at_x <= side)
        keep = keep & ((at_y == side + 1) if dy else (at_y <= side))
        if dx:
            keep = keep & (a < ngx - 1)
        if dy:
            keep = keep & (b < ngy - 1)
        if dz:
            keep = keep & (c < ngz - 1) & (at_z == 1)
        for j in range(4) if dz == 0 else (0,):
            v = got_corr[spot[i] + j]
            v = pltpu.roll(v, turn, 1) if turn else v
            total[j if dz == 0 else 3] += jnp.where(keep, v, 0.0)
    rows = []
    for j in range(4):
        rows += [total[j][:, 0:64], total[j][:, 64:128]]
    out_h[...] = jnp.concatenate(rows, axis=0)
    phase("p34_finish")
    sent(HALO_G, blocks)
    stack.close()


def prolong(cfg, ct_h, out_h, ct, out_v, in_sem, out_sem):
    rhs, fine = cfg[3], cfg[4]
    load = pltpu.make_async_copy(ct_h, ct, in_sem)
    load.start()
    stack = contextlib.ExitStack()
    stack.enter_context(jax.named_scope("q0"))
    shape = (fine, 128)
    fx, col = floats(shape, 0), floats(shape, 1)
    rest = col - 64.0 * whole_part(col, 64)
    cx = whole_part(rest, 8)
    along_x = tent(cx - 1.0, fx) * 0.25
    along_y = tent(rest - 8.0 * cx - 1.0, fx) * 0.25
    spread_xy = (along_x[:, None, :] * along_y[None, :, :]).reshape(fine * fine, 128).astype(BF16)
    shape = (rhs * fine, 8 * rhs)
    row, col = floats(shape, 0), floats(shape, 1)
    fr = whole_part(row, fine)
    fz = row - fine * fr
    cz = whole_part(col, rhs)
    cr = col - rhs * cz
    same = jnp.maximum(1.0 - jnp.abs(cr - fr), 0.0)
    spread_z = (tent(cz - 1.0, fz) * same * 0.25).astype(BF16)

    stack.close()
    stack.enter_context(jax.named_scope("q1"))
    load.wait()
    stack.close()
    stack.enter_context(jax.named_scope("q2"))
    ct_h, ct_l = split(ct[...])
    ht = dot(spread_z, ct_h) + dot(spread_z, ct_l)
    ht_h = ht.astype(BF16).astype(F32)
    ht = jnp.concatenate([ht_h, ht - ht_h], axis=1)
    stack.close()
    stack.enter_context(jax.named_scope("q3"))
    stores = []
    for r in range(rhs):
        part_r = ht[r * fine : (r + 1) * fine].astype(BF16)
        out_v[r] = dot(spread_xy, part_r, BACK).reshape(fine, fine, fine)
        store = pltpu.make_async_copy(out_v.at[r], out_h.at[r], out_sem.at[r])
        store.start()
        stores.append(store)
    stack.close()
    stack.enter_context(jax.named_scope("q4"))
    for store in stores:
        store.wait()
    stack.close()


def per_device(mesh_sizes, *args):
    (rs, it, cf, od, li, lf, ls, lt, fi, fs, ft, si, st, ti) = args
    ngx, ngy, ngz = mesh_sizes
    od = od.reshape(1, -1)
    rhs, fine = rs.shape[0], rs.shape[1]
    side = fine // 4
    leaf, n1, n2, n3, ntop = li.shape[3], fs.shape[3], st.shape[3], ti.shape[0], ti.shape[1]
    li, fs, ft, st = (jnp.transpose(v, (0, 1, 3, 2, 4))[0, 0] for v in (li, fs, ft, st))
    fi, si = jnp.transpose(fi, (0, 2, 1, 3))[0], jnp.transpose(si, (1, 0, 2))
    lf, ls = (jnp.transpose(v, (0, 1, 4, 2, 3))[0, 0] for v in (lf, ls))
    lt = jnp.transpose(lt, (0, 1, 2, 4, 3))[0, 0, 0]
    cfg = (ngx, ngy, ngz, rhs, fine, side, leaf, n1, n2, n3, ntop)
    plane = ngy * ngz
    groups1, groups2 = (ngz + 3) // 4, (plane + 3) // 4
    cells = side**3
    inputs = [rs, it, cf, od, li, lf, ls, lt, fi, fs, ft, si, st, ti]
    v = pltpu.VMEM
    width = 2 * (ntop // ngz)
    narrow = [x.reshape(x.shape[0], -1) if any(x is y for y in (li, lf, ls, fs, ft, st)) else x for x in inputs]
    scratch = [v(x.shape, x.dtype) for x in narrow]
    small = len(HALO) + 3 * len(FLAT) + len(RIM) + 9 + 4 * plane + 3 * ngz - 2
    scratch += [
        v((fine * fine, rhs * fine), F32), v((fine * fine, rhs * fine), F32), v((128, fine * fine), BF16),
        v((cells, 384), F32), v((512, 384), BF16), v((512, 384), BF16),
        v((32, 256), F32), v((128, 256), BF16), v((128, 256), BF16),
        v((32, 128), F32), v((256, 128), BF16), v((256, 128), BF16),
        v((32, 128), F32), v((32, 128), F32), v((512, 128), BF16), v((512, 128), BF16), v(st.shape[::2], F32), v(ft.shape[::2], F32),
        v((128, 128 * groups1), F32), v((128, 128 * groups1), BF16), v((128, 128 * groups1), BF16),
        v((64, 128 * groups2), F32), v((128, 128 * groups2), BF16), v((128, 128 * groups2), BF16),
        v(fi.shape, F32), v(si.shape, F32), v((ngz, 32, 128 * groups2), F32),
        v((128, 128 * groups2), BF16), v((128, 128 * groups2), BF16),
        v((4, rhs, 128), F32), v((len(HALO) + 3 * len(FLAT), rhs, 128), F32),
        v((groups1, rhs, 128), F32), v((ngz, rhs, 128), F32),
        v((groups2, rhs, 128), F32), v((2 * plane, rhs, 128), F32),
        v((rhs, 128), F32), v((rhs, 128), F32),
        v((rhs, ngz // 2, 1, width), F32), v((plane, 1, width), F32),
        v((1, width), F32), v((ngx, 1, width), F32),
        v((rhs, ngz // 2, 1, width), F32),
        v((rhs, 128), F32), v((rhs, 128), F32),
        v((2 * plane, rhs, 128), F32), v((2 * ngz, rhs, 128), F32), v((rhs, 128), F32), v((rhs, 128), F32), v((small, rhs, 128), F32),
        v((4, rhs, 128), F32), v((sum(1 if d[2] else 4 for d in RIM), rhs, 128), F32),
        pltpu.SemaphoreType.DMA((len(inputs) + rhs - 1,)),
        *[pltpu.SemaphoreType.REGULAR] * 4,
        pltpu.SemaphoreType.DMA((9,)), pltpu.SemaphoreType.DMA((SPREAD_G + ngz // 2,)),
    ]
    coarse = pl.pallas_call(
        functools.partial(kernel, cfg),
        out_shape=jax.ShapeDtypeStruct((8 * rhs, 64), F32),
        in_specs=[pl.BlockSpec(memory_space=pl.ANY)] * len(inputs),
        out_specs=pl.BlockSpec(memory_space=pltpu.VMEM),
        scratch_shapes=scratch,
        compiler_params=pltpu.CompilerParams(
            collective_id=0, has_side_effects=True, vmem_limit_bytes=67043328
        ),
        name="coarse_correction",
    )(*inputs)
    return pl.pallas_call(
        functools.partial(prolong, cfg),
        out_shape=jax.ShapeDtypeStruct(rs.shape, F32),
        in_specs=[pl.BlockSpec(memory_space=pl.ANY)],
        out_specs=pl.BlockSpec(memory_space=pl.ANY),
        scratch_shapes=[v((8 * rhs, 64), F32), v(rs.shape, F32), pltpu.SemaphoreType.DMA, pltpu.SemaphoreType.DMA((rhs,))],
        compiler_params=pltpu.CompilerParams(vmem_limit_bytes=67043328),
        name="prolong",
    )(coarse)


def solution(mesh):
    sizes = tuple(mesh.shape[n] for n in AXES)
    cells = P("gx", "gy", "gz")
    lines = P("gx", "gy", "gz", None)
    blocks = P("gx", "gy", "gz", None, None)
    field = P(None, "gx", "gy", "gz")
    return jax.shard_map(
        functools.partial(per_device, sizes),
        mesh=mesh,
        in_specs=(
            field, field, cells, lines, blocks, blocks, blocks, blocks, lines, blocks, blocks,
            P("gx", ("gy", "gz"), None), blocks, P(("gx", "gy", "gz"), None),
        ),
        out_specs=field,
        check_vma=False,
    )
```
